32 devices in a mesh: dp: 4 (over y, z), tp: 8 (over x, core).
Axes of the slice: x: 4, y: 2, z: 2, core: 2. Of those that a mesh axis runs over, the one named last changes fastest.
The devices are a block of a 4x4x8 slice.
Arguments:
- out_y1: float32 [32, 128, 1024], P('dp'), parts along dimension 0
- out_y2: float32 [32, 128, 1024], P('dp'), parts along dimension 0
- cot_y1: float32 [32, 128, 1024], P('dp'), parts along dimension 0
- cot_y2: float32 [32, 128, 1024], P('dp'), parts along dimension 0
- w_qkv: bfloat16 [4, 1024, 8, 3, 128], P(None, None, 'tp')
- w_out: bfloat16 [4, 8, 128, 1024], P(None, 'tp')
- w_up: bfloat16 [4, 1024, 4096], P(None, None, 'tp')
- w_down: bfloat16 [4, 4096, 1024], P(None, 'tp')
Outputs:
- output 1: float32 [32, 128, 1024], P('dp'), parts along dimension 0
- output 2: float32 [32, 128, 1024], P('dp'), parts along dimension 0
- output 3: float32 [32, 128, 1024], P('dp'), parts along dimension 0
- output 4: float32 [32, 128, 1024], P('dp'), parts along dimension 0
- output 5: float32 [16, 1024, 8, 3, 128], P('dp', None, 'tp'), parts along dimension 0
- output 6: float32 [16, 8, 128, 1024], P('dp', 'tp'), parts along dimension 0
- output 7: float32 [16, 1024, 4096], P('dp', None, 'tp'), parts along dimension 0
- output 8: float32 [16, 4096, 1024], P('dp', 'tp'), parts along dimension 0
There are 4 independent parts. The reference program is written for one: setup_inputs(seed, part) draws one part's arguments, and reference() takes and returns one part's arrays. A program takes and returns all parts, laid end to end along the dimension named above; an argument that names none is the same for every part.
All inputs are finite; a program needn't handle non-finite values.
Results may differ from the reference program's by a relative error of at most 0.02.
Values are sent between devices in bfloat16 or wider.
A program may use at most 768 MiB of HBM per device.

```python
import math
import jax
import jax.numpy as jnp
from jax import lax

D = 1024
HEADS = 8
FF = 4096
SEQ = 128
SEQS_DEV = 1
LAYERS = 4
TP = 8

BATCH = SEQS_DEV * TP
HEAD = D // HEADS
TOKENS = BATCH * SEQ
SCORE_SCALE = 1.0 / math.sqrt(HEAD)
NORM_EPS = 1e-6


def setup_inputs(seed: int = 0, part: int = 0) -> dict:
    weight_keys = jax.random.split(jax.random.key(seed), 4)
    act_keys = jax.random.split(jax.random.fold_in(jax.random.key(seed + 1), part), 4)
    act_shape = (BATCH, SEQ, D)
    in_scale = 1.0 / math.sqrt(D)
    hid_scale = 1.0 / math.sqrt(FF)
    attn_gain = max(1.0, math.sqrt(SEQ / 55.0))
    qkv_gain = jnp.array([1.4142, 1.4142, 1.0], jnp.float32).reshape(1, 1, 1, 3, 1)
    w_qkv = jax.random.normal(weight_keys[0], (LAYERS, D, HEADS, 3, HEAD), jnp.float32) * qkv_gain * in_scale
    w_out = jax.random.normal(weight_keys[1], (LAYERS, HEADS, HEAD, D), jnp.float32) * (0.4 * attn_gain * in_scale)
    w_up = jax.random.normal(weight_keys[2], (LAYERS, D, FF), jnp.float32) * in_scale
    w_down = jax.random.normal(weight_keys[3], (LAYERS, FF, D), jnp.float32) * (0.6 * hid_scale)
    return {
        "out_y1": jax.random.normal(act_keys[0], act_shape, jnp.float32),
        "out_y2": jax.random.normal(act_keys[1], act_shape, jnp.float32),
        "cot_y1": jax.random.normal(act_keys[2], act_shape, jnp.float32),
        "cot_y2": jax.random.normal(act_keys[3], act_shape, jnp.float32),
        "w_qkv": w_qkv.astype(jnp.bfloat16),
        "w_out": w_out.astype(jnp.bfloat16),
        "w_up": w_up.astype(jnp.bfloat16),
        "w_down": w_down.astype(jnp.bfloat16),
    }


def rms_fwd(x_in):
    inv_rms = lax.rsqrt(jnp.mean(x_in * x_in, axis=-1, keepdims=True) + NORM_EPS)
    return inv_rms, x_in * inv_rms


def rms_back(inv_rms, normed, grad_n):
    return inv_rms * (grad_n - normed * jnp.mean(normed * grad_n, axis=-1, keepdims=True))


def mlp_block(x_in, cot_out, w_up, w_down):
    inv_rms, normed = rms_fwd(x_in)
    n_bf = normed.astype(jnp.bfloat16)
    hidden = jnp.dot(n_bf, w_up, preferred_element_type=jnp.float32)
    act_f, gelu_back = jax.vjp(jax.nn.gelu, hidden)
    act_bf = act_f.astype(jnp.bfloat16)
    branch = jnp.dot(act_bf, w_down, preferred_element_type=jnp.float32)
    cot_bf = cot_out.astype(jnp.bfloat16)
    g_down = jnp.dot(act_bf.T, cot_bf, preferred_element_type=jnp.float32)
    grad_act = jnp.dot(cot_bf, w_down.T, preferred_element_type=jnp.float32)
    grad_hid = gelu_back(grad_act)[0].astype(jnp.bfloat16)
    g_up = jnp.dot(n_bf.T, grad_hid, preferred_element_type=jnp.float32)
    grad_n = jnp.dot(grad_hid, w_up.T, preferred_element_type=jnp.float32)
    return branch, rms_back(inv_rms, normed, grad_n), g_up, g_down


def attn_probs(qkv_seq):
    q_rows = qkv_seq[:, :, 0].astype(jnp.float32)
    k_rows = qkv_seq[:, :, 1].astype(jnp.float32)
    scores = jnp.einsum("qhe,khe->hqk", q_rows, k_rows) * SCORE_SCALE
    return jax.nn.softmax(scores, axis=-1)


def attn_seq_fwd(qkv_seq):
    prob_f = attn_probs(qkv_seq).astype(jnp.bfloat16).astype(jnp.float32)
    v_rows = qkv_seq[:, :, 2].astype(jnp.float32)
    return jnp.einsum("hqk,khe->qhe", prob_f, v_rows).astype(jnp.bfloat16)


def attn_seq_back(seq_args):
    qkv_seq, grad_o = seq_args
    attn_prob = attn_probs(qkv_seq)
    prob_f = attn_prob.astype(jnp.bfloat16).astype(jnp.float32)
    q_rows = qkv_seq[:, :, 0].astype(jnp.float32)
    k_rows = qkv_seq[:, :, 1].astype(jnp.float32)
    v_rows = qkv_seq[:, :, 2].astype(jnp.float32)
    grad_of = grad_o.astype(jnp.float32)
    grad_p = jnp.einsum("qhe,khe->hqk", grad_of, v_rows)
    grad_v = jnp.einsum("hqk,qhe->khe", prob_f, grad_of)
    grad_s = attn_prob * (grad_p - jnp.sum(grad_p * attn_prob, axis=-1, keepdims=True)) * SCORE_SCALE
    grad_s = grad_s.astype(jnp.bfloat16).astype(jnp.float32)
    grad_q = jnp.einsum("hqk,khe->qhe", grad_s, k_rows)
    grad_k = jnp.einsum("hqk,qhe->khe", grad_s, q_rows)
    return jnp.stack([grad_q, grad_k, grad_v], axis=2).astype(jnp.bfloat16)


def attn_block(x_in, cot_out, w_qkv, w_out):
    inv_rms, normed = rms_fwd(x_in)
    n_bf = normed.astype(jnp.bfloat16)
    qkv_mat = w_qkv.reshape(D, 3 * D)
    out_mat = w_out.reshape(D, D)
    qkv = jnp.dot(n_bf, qkv_mat, preferred_element_type=jnp.float32).astype(jnp.bfloat16)
    qkv = qkv.reshape(BATCH, SEQ, HEADS, 3, HEAD)
    attn_out = lax.map(attn_seq_fwd, qkv).reshape(TOKENS, D)
    branch = jnp.dot(attn_out, out_mat, preferred_element_type=jnp.float32)
    cot_bf = cot_out.astype(jnp.bfloat16)
    g_out = jnp.dot(attn_out.T, cot_bf, preferred_element_type=jnp.float32).reshape(HEADS, HEAD, D)
    grad_o = jnp.dot(cot_bf, out_mat.T, preferred_element_type=jnp.float32).astype(jnp.bfloat16)
    grad_o = grad_o.reshape(BATCH, SEQ, HEADS, HEAD)
    grad_qkv = lax.map(attn_seq_back, (qkv, grad_o)).reshape(TOKENS, 3 * D)
    g_qkv = jnp.dot(n_bf.T, grad_qkv, preferred_element_type=jnp.float32).reshape(D, HEADS, 3, HEAD)
    grad_n = jnp.dot(grad_qkv, qkv_mat.T, preferred_element_type=jnp.float32)
    return branch, rms_back(inv_rms, normed, grad_n), g_qkv, g_out


def reference(out_y1, out_y2, cot_y1, cot_y2, w_qkv, w_out, w_up, w_down):
    def layer_step(carry, weights):
        run_y1, run_y2, run_c1, run_c2 = carry
        layer_qkv, layer_out, layer_up, layer_down = weights
        g_branch, g_grad, g_up, g_down = mlp_block(run_y1, run_c2, layer_up, layer_down)
        low_x2 = run_y2 - g_branch
        run_c1 = run_c1 + g_grad
        f_branch, f_grad, g_qkv, g_out = attn_block(low_x2, run_c1, layer_qkv, layer_out)
        low_x1 = run_y1 - f_branch
        run_c2 = run_c2 + f_grad
        return (low_x1, low_x2, run_c1, run_c2), (g_qkv, g_out, g_up, g_down)

    init = (out_y1.reshape(TOKENS, D), out_y2.reshape(TOKENS, D), cot_y1.reshape(TOKENS, D), cot_y2.reshape(TOKENS, D))
    final, grads = lax.scan(layer_step, init, (w_qkv, w_out, w_up, w_down), reverse=True)
    return (final[0].reshape(BATCH, SEQ, D), final[1].reshape(BATCH, SEQ, D), final[2].reshape(BATCH, SEQ, D), final[3].reshape(BATCH, SEQ, D), grads[0], grads[1], grads[2], grads[3])
```

```python
import functools
import math
import jax
import jax.numpy as jnp
from jax import lax
from jax.experimental import pallas as pl
from jax.experimental.pallas import tpu as pltpu
from jax.sharding import PartitionSpec as P

NORM_EPS = 1e-6
F32, BF16 = jnp.float32, jnp.bfloat16
GELU_C = math.sqrt(2.0 / math.pi)
GELU_A = 0.044715
NCHIP = 4


def mm(a, b):
    return lax.dot_general(a, b, (((1,), (0,)), ((), ())), preferred_element_type=F32)


def mm_t(a, b):
    return lax.dot_general(a, b, (((1,), (1,)), ((), ())), preferred_element_type=F32)


def tmm(a, b):
    return lax.dot_general(a, b, (((0,), (0,)), ((), ())), preferred_element_type=F32)


def kernel(y1_hbm, y2_hbm, c1_hbm, c2_hbm, wqkv_hbm, wo_hbm, wu_hbm, wd_hbm,
           x1_out, x2_out, g1_out, g2_out, gqkv_out, gout_out, gup_out, gdown_out,
           N1, N2, D1, D2, Wqkv, Wo, Wu, Wd, Gqkv, Go, Gu, Gd, H, ACT, GH, QKV, PROB, O, GQ,
           Y1, Y2, C1, C2, PF, PB, XF, XB, RF, RB,
           ag_send, ag_recv, rs_send, rs_recv, fg_send, fg_recv, w_sem, g_sem, io_sem, own_sem):
    layers = wqkv_hbm.shape[0]
    rows = y1_hbm.shape[1]
    half = rows // 2
    width = y1_hbm.shape[2]
    head = wo_hbm.shape[1]
    scale = 1.0 / math.sqrt(head)
    ndev = 2 * NCHIP
    me = lax.axis_index("tp")
    c = me // 2
    k = lax.rem(me, 2)
    sib = me + 1 - 2 * k
    left = lax.rem(me + ndev - 2, ndev)
    right = lax.rem(me + 2, ndev)
    cl = lax.rem(c + NCHIP - 1, NCHIP)
    cr = lax.rem(c + 1, NCHIP)
    co = lax.rem(c + 2, NCHIP)
    mine = pl.ds(pl.multiple_of(k * rows, rows), rows)
    other = pl.ds(pl.multiple_of((1 - k) * rows, rows), rows)

    def my_half(h):
        return pl.ds(pl.multiple_of(k * rows + h * half, half), half)

    def order(j):
        off = (2 + j) * (1 - j // 2) + (3 - j) * (j // 2)
        return lax.rem(c + off, NCHIP)

    def remote(src, dst, ssem, rsem, dev):
        return pltpu.make_async_remote_copy(src_ref=src, dst_ref=dst, send_sem=ssem, recv_sem=rsem,
                                            device_id={"tp": dev}, device_id_type=pl.DeviceIdType.MESH)

    barrier = pltpu.get_barrier_semaphore()
    for dev in (sib, left, right):
        pl.semaphore_signal(barrier, inc=1, device_id={"tp": dev}, device_id_type=pl.DeviceIdType.MESH)
    pl.semaphore_wait(barrier, 3)

    class Gather:
        def __init__(self, view, ssem, rsem):
            def full(chip):
                return view(chip, mine)

            def sibrows(chip):
                return view(chip, other)

            def hf(chip, h):
                return view(chip, my_half(h))

            def ohf(chip, h):
                return view(chip, pl.ds(pl.multiple_of((1 - k) * rows + h * half, half), half))

            self.send = [
                remote(full(c), full(c), ssem.at[0], rsem.at[0], left),
                remote(full(c), full(c), ssem.at[1], rsem.at[1], right),
                remote(full(c), full(c), ssem.at[2], rsem.at[2], sib),
                remote(hf(cr, 0), hf(cr, 0), ssem.at[3], rsem.at[3], left),
                remote(full(cr), full(cr), ssem.at[4], rsem.at[4], sib),
                remote(hf(cl, 1), hf(cl, 1), ssem.at[5], rsem.at[5], right),
                remote(full(cl), full(cl), ssem.at[6], rsem.at[6], sib),
                remote(hf(co, 0), hf(co, 0), ssem.at[7], rsem.at[7], sib),
                remote(hf(co, 1), hf(co, 1), ssem.at[8], rsem.at[8], sib),
            ]
            land = [full(cr), full(cl), sibrows(c), hf(co, 0), sibrows(cr), hf(co, 1), sibrows(cl),
                    ohf(co, 0), ohf(co, 1)]
            self.recv = [remote(r, r, ssem.at[i], rsem.at[i], sib) for i, r in enumerate(land)]

        def start(self):
            for i in (0, 1, 2):
                self.send[i].start()

        def near(self):
            self.recv[0].wait_recv()
            self.send[3].start()
            self.send[4].start()
            self.recv[1].wait_recv()
            self.send[5].start()
            self.send[6].start()

        def far(self):
            self.recv[3].wait_recv()
            self.send[7].start()
            self.recv[5].wait_recv()
            self.send[8].start()

        def finish(self):
            for i in (2, 4, 6, 7, 8):
                self.recv[i].wait_recv()
            for cp in self.send:
                cp.wait_send()

    class Scatter:
        def __init__(self, part, from_sib, rec, ssem, rsem):
            self.part, self.from_sib = part, from_sib
            self.rel, self.dir, self.fin = rec.at[0], rec.at[1], rec.at[2]
            self.ssem, self.rsem = ssem, rsem

            def hp(chip, h):
                return part.at[chip, my_half(h)]

            def hr(buf, h):
                return buf.at[pl.ds(h * half, half)]

            def mk(i, src, dst, dev):
                return remote(src, dst, ssem.at[i], rsem.at[i], dev)

            self.opp = [mk(4, hp(co, 0), hr(self.rel, 0), left), mk(5, hp(co, 1), hr(self.rel, 1), right)]
            self.direct = [mk(6, hp(cl, 1), hr(self.dir, 1), left), mk(7, hp(cr, 0), hr(self.dir, 0), right)]
            self.relay = [mk(8, hp(cl, 0), hr(self.fin, 0), left), mk(9, hp(cr, 1), hr(self.fin, 1), right)]

        def pair(self, chip):
            return remote(self.part.at[chip, other], self.from_sib.at[chip], self.ssem.at[chip],
                          self.rsem.at[chip], sib)

        def add(self, chip):
            self.pair_recv(chip)
            got = self.part[chip, mine].astype(F32) + self.from_sib[chip].astype(F32)
            self.part[chip, mine] = got.astype(self.part.dtype)

        def pair_recv(self, chip):
            remote(self.from_sib.at[chip], self.from_sib.at[chip], self.ssem.at[chip], self.rsem.at[chip],
                   sib).wait_recv()

        def send_opp(self):
            self.add(co)
            for cp in self.opp:
                cp.start()

        def send_direct(self):
            self.add(cl)
            self.direct[0].start()
            self.add(cr)
            self.direct[1].start()

        def send_relay(self):
            for h, (chip, cp) in enumerate(((cl, self.relay[0]), (cr, self.relay[1]))):
                self.opp[h].wait_recv()
                got = self.part[chip, my_half(h)].astype(F32) + self.rel[h * half:(h + 1) * half].astype(F32)
                self.part[chip, my_half(h)] = got.astype(self.part.dtype)
                cp.start()

        def land(self):
            self.pair_recv(c)
            for cp in self.direct + self.relay:
                cp.wait_recv()

        def total(self, r):
            at = pl.ds(pl.multiple_of(k * rows + r * 16, 16), 16)
            loc = pl.ds(pl.multiple_of(r * 16, 16), 16)
            return (self.part[c, at].astype(F32) + self.from_sib[c, loc].astype(F32)
                    + self.fin[loc].astype(F32) + self.dir[loc].astype(F32))

        def drain(self):
            for chip in range(NCHIP):
                self.pair(chip).wait_send()
            for cp in self.opp + self.direct + self.relay:
                cp.wait_send()

    rs_f = Scatter(PF, XF, RF, rs_send.at[0], rs_recv.at[0])
    rs_b = Scatter(PB, XB, RB, rs_send.at[1], rs_recv.at[1])

    def gather_n(buf, par, i):
        return Gather(lambda chip, r: buf.at[par, chip, r], ag_send.at[i], ag_recv.at[i])

    def gather_d(buf, i):
        return Gather(lambda chip, r: buf.at[chip, r], ag_send.at[i], ag_recv.at[i])

    def gather_out(out, i):
        def view(chip, r):
            return out.at[pl.ds(pl.multiple_of(chip * 2 * rows, rows) + r.start, r.size)]
        return Gather(view, fg_send.at[i], fg_recv.at[i])

    def weight_copies(layer, slot):
        return [pltpu.make_async_copy(src.at[layer], dst.at[slot], w_sem.at[slot, i])
                for i, (src, dst) in enumerate(((wqkv_hbm, Wqkv), (wo_hbm, Wo), (wu_hbm, Wu), (wd_hbm, Wd)))]

    def grad_copy(layer, i):
        src, dst = ((Gqkv, gqkv_out), (Go, gout_out), (Gu, gup_out), (Gd, gdown_out))[i]
        return pltpu.make_async_copy(src, dst.at[layer], g_sem.at[i])

    def mlp_fwd(chip, par):
        hid = mm(N1[par, chip], Wu[par])
        H[chip] = hid
        act = hid * (0.5 * (1.0 + jnp.tanh(GELU_C * (hid + GELU_A * (hid * hid * hid)))))
        act = act.astype(BF16)
        ACT[chip] = act
        PF[chip] = mm(act, Wd[par])

    def mlp_bwd(chip, par):
        grad_act = mm_t(D2[chip], Wd[par])
        hid = H[chip]
        sq = hid * hid
        t = jnp.tanh(GELU_C * (hid + GELU_A * (sq * hid)))
        slope = 0.5 * (1.0 + t) + (0.5 * hid) * ((1.0 - t * t) * (GELU_C * (1.0 + (3.0 * GELU_A) * sq)))
        grad_hid = (grad_act * slope).astype(BF16)
        GH[chip] = grad_hid
        PB[chip] = mm_t(grad_hid, Wu[par]).astype(BF16)

    def attn_fwd(chip, par):
        QKV[chip] = mm(N2[par, chip], Wqkv[par]).astype(BF16)
        for s in range(2):
            at = slice(s * rows, (s + 1) * rows)
            q = QKV[chip, at, 0:head]
            kk = QKV[chip, at, head:2 * head]
            v = QKV[chip, at, 2 * head:3 * head]
            sc = mm_t(q, kk) * scale
            e = jnp.exp(sc - jnp.max(sc, axis=-1, keepdims=True))
            prob = e / jnp.sum(e, axis=-1, keepdims=True)
            PROB[chip, at] = prob
            O[chip, at] = mm(prob.astype(BF16), v).astype(BF16)
        PF[chip] = mm(O[chip], Wo[par])

    def attn_bwd(chip, par):
        grad_o2 = mm_t(D1[chip], Wo[par]).astype(BF16)
        for s in range(2):
            at = slice(s * rows, (s + 1) * rows)
            grad_o = grad_o2[at]
            q = QKV[chip, at, 0:head]
            kk = QKV[chip, at, head:2 * head]
            v = QKV[chip, at, 2 * head:3 * head]
            prob = PROB[chip, at]
            grad_p = mm_t(grad_o, v)
            grad_s = (prob * (grad_p - jnp.sum(grad_p * prob, axis=-1, keepdims=True)) * scale).astype(BF16)
            GQ[chip, at, 0:head] = mm(grad_s, kk).astype(BF16)
            GQ[chip, at, head:2 * head] = tmm(grad_s, q).astype(BF16)
            GQ[chip, at, 2 * head:3 * head] = tmm(prob.astype(BF16), grad_o).astype(BF16)
        PB[chip] = mm_t(GQ[chip], Wqkv[par]).astype(BF16)

    def flat(x):
        return x.reshape((x.shape[0] * x.shape[1],) + x.shape[2:])

    def mlp_wgrad(layer, par, not_first):
        @pl.when(not_first)
        def _():
            grad_copy(layer, 2).wait()
            grad_copy(layer, 3).wait()
        tile = width // 4

        def up(i, _):
            at = pl.ds(pl.multiple_of(i * tile, tile), tile)
            Gu[at] = tmm(flat(N1[par, :, :, at]), flat(GH[...]))
            return 0

        def down(i, _):
            at = pl.ds(pl.multiple_of(i * tile, tile), tile)
            Gd[:, at] = tmm(flat(ACT[...]), flat(D2[:, :, at]))
            return 0
        lax.fori_loop(0, 4, up, 0)
        grad_copy(layer, 2).start()
        lax.fori_loop(0, 4, down, 0)
        grad_copy(layer, 3).start()

    def attn_wgrad(layer, par, not_first):
        @pl.when(not_first)
        def _():
            grad_copy(layer, 0).wait()
            grad_copy(layer, 1).wait()
        tile = width // 4

        def qkv(i, _):
            at = pl.ds(pl.multiple_of(i * tile, tile), tile)
            Gqkv[at] = tmm(flat(N2[par, :, :, at]), flat(GQ[...]))
            return 0

        def out(i, _):
            at = pl.ds(pl.multiple_of(i * tile, tile), tile)
            Go[:, at] = tmm(flat(O[...]), flat(D1[:, :, at]))
            return 0
        lax.fori_loop(0, 4, qkv, 0)
        grad_copy(layer, 0).start()
        lax.fori_loop(0, 4, out, 0)
        grad_copy(layer, 1).start()

    def own_rows(step):
        def body(r, _):
            step(r, pl.ds(pl.multiple_of(r * 16, 16), 16), pl.ds(pl.multiple_of(k * rows + r * 16, 16), 16))
            return 0
        lax.fori_loop(0, rows // 16, body, 0)

    def inv_rms(x):
        return lax.rsqrt(jnp.mean(x * x, axis=-1, keepdims=True) + NORM_EPS)

    def finish_state(rs, old, new, norm_to):
        rs.land()

        def step(r, loc, at):
            x = old[loc] - rs.total(r)
            new[loc] = x
            if norm_to is not None:
                norm_to[c, at] = (x * inv_rms(x)).astype(BF16)
        own_rows(step)
        rs.drain()

    def finish_cot(rs, cot, x_ref, cast_to):
        rs.land()

        def step(r, loc, at):
            x = x_ref[loc]
            inv = inv_rms(x)
            normed = x * inv
            grad_n = rs.total(r)
            new = cot[loc] + inv * (grad_n - normed * jnp.mean(normed * grad_n, axis=-1, keepdims=True))
            cot[loc] = new
            if cast_to is not None:
                cast_to[c, at] = new.astype(BF16)
        own_rows(step)
        rs.drain()

    def when(cond, fn):
        if cond is True:
            fn()
        elif cond is not False:
            pl.when(cond)(fn)

    def partials(rs, compute, early):
        def body(j, _):
            chip = order(j)
            compute(chip)
            rs.pair(chip).start()
            if early:
                pl.when(j == 1)(rs.send_opp)
            return 0
        lax.fori_loop(0, NCHIP, body, 0)

    def half_step(ag_n, fin_n, ag_d, fin_d, fwd, bwd, wgrad, has_d):
        fin_n()
        ag_n.start()
        when(has_d, rs_b.send_relay)
        ag_n.near()

        def d_start():
            fin_d()
            ag_d.start()
        when(has_d, d_start)
        ag_n.far()
        ag_n.finish()
        partials(rs_f, fwd, True)
        when(has_d, ag_d.near)
        rs_f.send_direct()
        rs_f.send_relay()

        def d_end():
            ag_d.far()
            ag_d.finish()
        when(has_d, d_end)
        partials(rs_b, bwd, False)
        rs_b.send_opp()
        rs_b.send_direct()
        wgrad()

    def stage_attn(layer, par, not_first, last):
        q = 1 - par
        if not last:
            for cp in weight_copies(layer - 1, q):
                cp.start()
        half_step(
            gather_n(N2, par, 0), lambda: finish_state(rs_f, Y2.at[q], Y2.at[par], N2.at[par]),
            gather_d(D2, 1), lambda: finish_cot(rs_b, C2, Y2.at[q], D2),
            lambda chip: attn_fwd(chip, par), lambda chip: mlp_bwd(chip, par),
            lambda: mlp_wgrad(layer, par, not_first), not_first)

    def stage_mlp(layer, par, not_first):
        q = 1 - par

        def fin():
            finish_state(rs_f, Y1.at[par], Y1.at[q], N1.at[q])
            for cp in weight_copies(layer - 1, q):
                cp.wait()
        half_step(
            gather_n(N1, q, 2), fin,
            gather_d(D1, 3), lambda: finish_cot(rs_b, C1, Y1.at[par], D1),
            lambda chip: mlp_fwd(chip, q), lambda chip: attn_bwd(chip, par),
            lambda: attn_wgrad(layer, par, not_first), True)

    top = layers - 1
    tp = top % 2
    for cp in weight_copies(top, tp):
        cp.start()
    blk = pl.ds(pl.multiple_of(me * 1, 1), 1)
    loads = [pltpu.make_async_copy(src.at[me], dst, own_sem.at[i]) for i, (src, dst) in enumerate(
        ((y1_hbm, Y1.at[tp]), (y2_hbm, Y2.at[1 - tp]), (c1_hbm, C1), (c2_hbm, C2)))]
    for cp in loads:
        cp.start()

    def bulk(src, i, chip, s):
        return pltpu.make_async_copy(src.at[2 * chip + s], PF.at[chip, pl.ds(s * rows, rows)], io_sem.at[i, chip, s])

    for chip in range(NCHIP):
        for s in range(2):
            bulk(y1_hbm, 0, chip, s).start()
    for chip in range(NCHIP):
        for s in range(2):
            bulk(y1_hbm, 0, chip, s).wait()

    def norm_all(i, _):
        for chip in range(NCHIP):
            at = pl.ds(pl.multiple_of(i * 16, 16), 16)
            x = PF[chip, at]
            N1[tp, chip, at] = (x * inv_rms(x)).astype(BF16)
        return 0
    lax.fori_loop(0, 2 * rows // 16, norm_all, 0)
    for chip in range(NCHIP):
        for s in range(2):
            bulk(c2_hbm, 1, chip, s).start()
    for chip in range(NCHIP):
        for s in range(2):
            bulk(c2_hbm, 1, chip, s).wait()

    def cast_all(i, _):
        for chip in range(NCHIP):
            at = pl.ds(pl.multiple_of(i * 16, 16), 16)
            D2[chip, at] = PF[chip, at].astype(BF16)
        return 0
    lax.fori_loop(0, 2 * rows // 16, cast_all, 0)
    for cp in loads:
        cp.wait()
    for cp in weight_copies(top, tp):
        cp.wait()
    partials(rs_f, lambda chip: mlp_fwd(chip, tp), True)
    rs_f.send_direct()
    rs_f.send_relay()

    def layer_body(i, _):
        layer = top - i
        par = lax.rem(layer, 2)
        stage_attn(layer, par, layer < top, False)
        stage_mlp(layer, par, layer < top)
        return 0
    lax.fori_loop(0, top, layer_body, 0)

    stage_attn(0, 0, True, True)
    outs = [gather_out(o, i) for i, o in enumerate((x1_out, x2_out, g1_out, g2_out))]

    def put(i, src):
        out = (x1_out, x2_out, g1_out, g2_out)[i]
        at = pl.ds(pl.multiple_of(me * rows, rows), rows)
        pltpu.make_async_copy(src, out.at[at], own_sem.at[i]).start()
        for n, dev in enumerate((left, right, sib)):
            remote(src, out.at[at], fg_send.at[i, n], fg_recv.at[i, n], dev).start()

    def put_done(i, src):
        out = (x1_out, x2_out, g1_out, g2_out)[i]
        at = pl.ds(pl.multiple_of(me * rows, rows), rows)
        pltpu.make_async_copy(src, out.at[at], own_sem.at[i]).wait()

    ag_d1 = gather_d(D1, 3)
    finish_state(rs_f, Y1.at[0], Y1.at[1], None)
    rs_b.send_relay()
    put(1, Y2.at[0])
    finish_cot(rs_b, C1, Y1.at[0], D1)
    ag_d1.start()
    put(0, Y1.at[1])
    ag_d1.near()
    outs[1].near()
    ag_d1.far()
    ag_d1.finish()
    partials(rs_b, lambda chip: attn_bwd(chip, 0), False)
    rs_b.send_opp()
    rs_b.send_direct()
    put(2, C1)
    attn_wgrad(0, 0, True)
    outs[0].near()
    rs_b.send_relay()
    outs[1].far()
    finish_cot(rs_b, C2, Y2.at[0], None)
    put(3, C2)
    outs[0].far()
    outs[2].near()
    outs[3].near()
    outs[2].far()
    outs[3].far()
    for i, src in enumerate((Y1.at[1], Y2.at[0], C1, C2)):
        outs[i].finish()
        put_done(i, src)
    for i in range(4):
        grad_copy(0, i).wait()


def solution(mesh):
    act_spec = P("dp", None, None)
    weight_specs = (P(None, None, "tp", None, None), P(None, "tp", None, None), P(None, None, "tp"), P(None, "tp", None))
    grad_specs = (P("dp", None, "tp", None, None), P("dp", "tp", None, None), P("dp", None, "tp"), P("dp", "tp", None))

    def local_backward(out_y1, out_y2, cot_y1, cot_y2, w_qkv, w_out, w_up, w_down):
        seqs, rows, width = out_y1.shape
        layers, _, heads, three, head = w_qkv.shape
        hidden = w_up.shape[2]
        wq = w_qkv.reshape(layers, width, heads * three * head)
        wo = w_out.reshape(layers, heads * head, width)
        pair = 2 * rows
        qkv_w = three * head
        act = jax.ShapeDtypeStruct((seqs * rows, width), F32)
        dma = pltpu.SemaphoreType.DMA
        outs = pl.pallas_call(
            kernel,
            out_shape=(act, act, act, act,
                       jax.ShapeDtypeStruct((layers, width, qkv_w), F32),
                       jax.ShapeDtypeStruct((layers, head, width), F32),
                       jax.ShapeDtypeStruct((layers, width, hidden), F32),
                       jax.ShapeDtypeStruct((layers, hidden, width), F32)),
            in_specs=[pl.BlockSpec(memory_space=pl.ANY)] * 8,
            out_specs=[pl.BlockSpec(memory_space=pl.ANY)] * 8,
            scratch_shapes=[
                pltpu.VMEM((2, NCHIP, pair, width), BF16),
                pltpu.VMEM((2, NCHIP, pair, width), BF16),
                pltpu.VMEM((NCHIP, pair, width), BF16),
                pltpu.VMEM((NCHIP, pair, width), BF16),
                pltpu.VMEM((2, width, qkv_w), BF16),
                pltpu.VMEM((2, head, width), BF16),
                pltpu.VMEM((2, width, hidden), BF16),
                pltpu.VMEM((2, hidden, width), BF16),
                pltpu.VMEM((width, qkv_w), F32),
                pltpu.VMEM((head, width), F32),
                pltpu.VMEM((width, hidden), F32),
                pltpu.VMEM((hidden, width), F32),
                pltpu.VMEM((NCHIP, pair, hidden), F32),
                pltpu.VMEM((NCHIP, pair, hidden), BF16),
                pltpu.VMEM((NCHIP, pair, hidden), BF16),
                pltpu.VMEM((NCHIP, pair, qkv_w), BF16),
                pltpu.VMEM((NCHIP, pair, rows), F32),
                pltpu.VMEM((NCHIP, pair, head), BF16),
                pltpu.VMEM((NCHIP, pair, qkv_w), BF16),
                pltpu.VMEM((2, rows, width), F32),
                pltpu.VMEM((2, rows, width), F32),
                pltpu.VMEM((rows, width), F32),
                pltpu.VMEM((rows, width), F32),
                pltpu.VMEM((NCHIP, pair, width), F32),
                pltpu.VMEM((NCHIP, pair, width), BF16),
                pltpu.VMEM((NCHIP, rows, width), F32),
                pltpu.VMEM((NCHIP, rows, width), BF16),
                pltpu.VMEM((3, rows, width), F32),
                pltpu.VMEM((3, rows, width), BF16),
                dma((4, 9)), dma((4, 9)), dma((2, 10)), dma((2, 10)), dma((4, 9)), dma((4, 9)),
                dma((2, 4)), dma((4,)), dma((2, NCHIP, 2)), dma((4,)),
            ],
            compiler_params=pltpu.CompilerParams(collective_id=0, has_side_effects=True,
                                                 vmem_limit_bytes=60 * 1024 * 1024),
        )(out_y1, out_y2, cot_y1, cot_y2, wq, wo, w_up, w_down)
        x1, x2, g1, g2 = (o.reshape(seqs, rows, width) for o in outs[:4])
        return (x1, x2, g1, g2, outs[4].reshape(w_qkv.shape), outs[5].reshape(w_out.shape), outs[6], outs[7])

    return jax.shard_map(local_backward, mesh=mesh, in_specs=(act_spec, act_spec, act_spec, act_spec) + weight_specs, out_specs=(act_spec, act_spec, act_spec, act_spec) + grad_specs, check_vma=False)
```

```python
import functools
import math
import jax
import jax.numpy as jnp
from jax import lax
from jax.experimental import pallas as pl
from jax.experimental.pallas import tpu as pltpu
from jax.sharding import PartitionSpec as P

NORM_EPS = 1e-6
F32, BF16 = jnp.float32, jnp.bfloat16
GELU_C = math.sqrt(2.0 / math.pi)
GELU_A = 0.044715
NCHIP = 4


def mm(a, b):
    return lax.dot_general(a, b, (((1,), (0,)), ((), ())), preferred_element_type=F32)


def mm_t(a, b):
    return lax.dot_general(a, b, (((1,), (1,)), ((), ())), preferred_element_type=F32)


def tmm(a, b):
    return lax.dot_general(a, b, (((0,), (0,)), ((), ())), preferred_element_type=F32)


def kernel(y1_hbm, y2_hbm, c1_hbm, c2_hbm, wqkv_hbm, wo_hbm, wu_hbm, wd_hbm,
           x1_out, x2_out, g1_out, g2_out, gqkv_out, gout_out, gup_out, gdown_out,
           N1, N2, D1, D2, Wqkv, Wo, Wu, Wd, Gqkv, Go, Gu, Gd, H, ACT, GH, QKV, PROB, O, GQ,
           Y1, Y2, C1, C2, PF, PB, XF, XB, RF, RB,
           ag_send, ag_recv, rs_send, rs_recv, fg_send, fg_recv, w_sem, g_sem, io_sem, own_sem):
    layers = wqkv_hbm.shape[0]
    rows = y1_hbm.shape[1]
    half = rows // 2
    width = y1_hbm.shape[2]
    head = wo_hbm.shape[1]
    scale = 1.0 / math.sqrt(head)
    ndev = 2 * NCHIP
    me = lax.axis_index("tp")
    c = me // 2
    k = lax.rem(me, 2)
    sib = me + 1 - 2 * k
    left = lax.rem(me + ndev - 2, ndev)
    right = lax.rem(me + 2, ndev)
    cl = lax.rem(c + NCHIP - 1, NCHIP)
    cr = lax.rem(c + 1, NCHIP)
    co = lax.rem(c + 2, NCHIP)
    mine = pl.ds(pl.multiple_of(k * rows, rows), rows)
    other = pl.ds(pl.multiple_of((1 - k) * rows, rows), rows)

    def my_half(h):
        return pl.ds(pl.multiple_of(k * rows + h * half, half), half)

    def order(j):
        off = (2 + j) * (1 - j // 2) + (3 - j) * (j // 2)
        return lax.rem(c + off, NCHIP)

    def remote(src, dst, ssem, rsem, dev):
        return pltpu.make_async_remote_copy(src_ref=src, dst_ref=dst, send_sem=ssem, recv_sem=rsem,
                                            device_id={"tp": dev}, device_id_type=pl.DeviceIdType.MESH)

    barrier = pltpu.get_barrier_semaphore()
    for dev in (sib, left, right):
        pl.semaphore_signal(barrier, inc=1, device_id={"tp": dev}, device_id_type=pl.DeviceIdType.MESH)
    pl.semaphore_wait(barrier, 3)

    class Gather:
        def __init__(self, view, ssem, rsem):
            def full(chip):
                return view(chip, mine)

            def sibrows(chip):
                return view(chip, other)

            def hf(chip, h):
                return view(chip, my_half(h))

            def ohf(chip, h):
                return view(chip, pl.ds(pl.multiple_of((1 - k) * rows + h * half, half), half))

            self.send = [
                remote(full(c), full(c), ssem.at[0], rsem.at[0], left),
                remote(full(c), full(c), ssem.at[1], rsem.at[1], right),
                remote(full(c), full(c), ssem.at[2], rsem.at[2], sib),
                remote(hf(cr, 0), hf(cr, 0), ssem.at[3], rsem.at[3], left),
                remote(full(cr), full(cr), ssem.at[4], rsem.at[4], sib),
                remote(hf(cl, 1), hf(cl, 1), ssem.at[5], rsem.at[5], right),
                remote(full(cl), full(cl), ssem.at[6], rsem.at[6], sib),
                remote(hf(co, 0), hf(co, 0), ssem.at[7], rsem.at[7], sib),
                remote(hf(co, 1), hf(co, 1), ssem.at[8], rsem.at[8], sib),
            ]
            land = [full(cr), full(cl), sibrows(c), hf(co, 0), sibrows(cr), hf(co, 1), sibrows(cl),
                    ohf(co, 0), ohf(co, 1)]
            self.recv = [remote(r, r, ssem.at[i], rsem.at[i], sib) for i, r in enumerate(land)]

        def start(self):
            for i in (0, 1, 2):
                self.send[i].start()

        def near(self):
            self.recv[0].wait_recv()
            self.send[3].start()
            self.send[4].start()
            self.recv[1].wait_recv()
            self.send[5].start()
            self.send[6].start()

        def far(self):
            self.recv[3].wait_recv()
            self.send[7].start()
            self.recv[5].wait_recv()
            self.send[8].start()

        def finish(self):
            for i in (2, 4, 6, 7, 8):
                self.recv[i].wait_recv()
            for cp in self.send:
                cp.wait_send()

    class Scatter:
        def __init__(self, part, from_sib, rec, ssem, rsem):
            self.part, self.from_sib = part, from_sib
            self.rel, self.dir, self.fin = rec.at[0], rec.at[1], rec.at[2]
            self.ssem, self.rsem = ssem, rsem

            def hp(chip, h):
                return part.at[chip, my_half(h)]

            def hr(buf, h):
                return buf.at[pl.ds(h * half, half)]

            def mk(i, src, dst, dev):
                return remote(src, dst, ssem.at[i], rsem.at[i], dev)

            self.opp = [mk(4, hp(co, 0), hr(self.rel, 0), left), mk(5, hp(co, 1), hr(self.rel, 1), right)]
            self.direct = [mk(6, hp(cl, 1), hr(self.dir, 1), left), mk(7, hp(cr, 0), hr(self.dir, 0), right)]
            self.relay = [mk(8, hp(cl, 0), hr(self.fin, 0), left), mk(9, hp(cr, 1), hr(self.fin, 1), right)]

        def pair(self, chip):
            return remote(self.part.at[chip, other], self.from_sib.at[chip], self.ssem.at[chip],
                          self.rsem.at[chip], sib)

        def add(self, chip):
            self.pair_recv(chip)
            got = self.part[chip, mine].astype(F32) + self.from_sib[chip].astype(F32)
            self.part[chip, mine] = got.astype(self.part.dtype)

        def pair_recv(self, chip):
            remote(self.from_sib.at[chip], self.from_sib.at[chip], self.ssem.at[chip], self.rsem.at[chip],
                   sib).wait_recv()

        def send_opp(self):
            self.add(co)
            for cp in self.opp:
                cp.start()

        def send_direct(self):
            self.add(cl)
            self.direct[0].start()
            self.add(cr)
            self.direct[1].start()

        def send_relay(self):
            for h, (chip, cp) in enumerate(((cl, self.relay[0]), (cr, self.relay[1]))):
                self.opp[h].wait_recv()
                got = self.part[chip, my_half(h)].astype(F32) + self.rel[h * half:(h + 1) * half].astype(F32)
                self.part[chip, my_half(h)] = got.astype(self.part.dtype)
                cp.start()

        def land(self):
            self.pair_recv(c)
            for cp in self.direct + self.relay:
                cp.wait_recv()

        def total(self, r):
            at = pl.ds(pl.multiple_of(k * rows + r * 16, 16), 16)
            loc = pl.ds(pl.multiple_of(r * 16, 16), 16)
            return (self.part[c, at].astype(F32) + self.from_sib[c, loc].astype(F32)
                    + self.fin[loc].astype(F32) + self.dir[loc].astype(F32))

        def drain(self):
            for chip in range(NCHIP):
                self.pair(chip).wait_send()
            for cp in self.opp + self.direct + self.relay:
                cp.wait_send()

    rs_f = Scatter(PF, XF, RF, rs_send.at[0], rs_recv.at[0])
    rs_b = Scatter(PB, XB, RB, rs_send.at[1], rs_recv.at[1])

    def gather_n(buf, par, i):
        return Gather(lambda chip, r: buf.at[par, chip, r], ag_send.at[i], ag_recv.at[i])

    def gather_d(buf, i):
        return Gather(lambda chip, r: buf.at[chip, r], ag_send.at[i], ag_recv.at[i])

    def gather_out(out, i):
        def view(chip, r):
            return out.at[pl.ds(pl.multiple_of(chip * 2 * rows, rows) + r.start, r.size)]
        return Gather(view, fg_send.at[i], fg_recv.at[i])

    def weight_copies(layer, slot):
        pairs = [(src.at[layer], dst.at[slot]) for src, dst in ((wo_hbm, Wo), (wu_hbm, Wu), (wd_hbm, Wd))]
        pairs += [(wqkv_hbm.at[layer, j], Wqkv.at[slot, :, pl.ds(j * head, head)]) for j in range(3)]
        return [pltpu.make_async_copy(src, dst, w_sem.at[slot, i]) for i, (src, dst) in enumerate(pairs)]

    def grad_copy(layer, i):
        src, dst = ((Gqkv, gqkv_out), (Go, gout_out), (Gu, gup_out), (Gd, gdown_out))[i]
        if i == 0:
            size = src.shape[0]
            return pltpu.make_async_copy(src, dst.at[pl.ds(pl.multiple_of(layer * size, size), size)], g_sem.at[i])
        return pltpu.make_async_copy(src, dst.at[layer], g_sem.at[i])

    def mlp_fwd(chip, par):
        hid = mm(N1[par, chip], Wu[par])
        H[chip] = hid
        act = hid * (0.5 * (1.0 + jnp.tanh(GELU_C * (hid + GELU_A * (hid * hid * hid)))))
        act = act.astype(BF16)
        ACT[chip] = act
        PF[chip] = mm(act, Wd[par])

    def mlp_bwd(chip, par):
        grad_act = mm_t(D2[chip], Wd[par])
        hid = H[chip]
        sq = hid * hid
        t = jnp.tanh(GELU_C * (hid + GELU_A * (sq * hid)))
        slope = 0.5 * (1.0 + t) + (0.5 * hid) * ((1.0 - t * t) * (GELU_C * (1.0 + (3.0 * GELU_A) * sq)))
        grad_hid = (grad_act * slope).astype(BF16)
        GH[chip] = grad_hid
        PB[chip] = mm_t(grad_hid, Wu[par]).astype(BF16)

    def attn_fwd(chip, par):
        QKV[chip] = mm(N2[par, chip], Wqkv[par]).astype(BF16)
        for s in range(2):
            at = slice(s * rows, (s + 1) * rows)
            q = QKV[chip, at, 0:head]
            kk = QKV[chip, at, head:2 * head]
            v = QKV[chip, at, 2 * head:3 * head]
            sc = mm_t(q, kk) * scale
            e = jnp.exp(sc - jnp.max(sc, axis=-1, keepdims=True))
            prob = e / jnp.sum(e, axis=-1, keepdims=True)
            PROB[chip, at] = prob
            O[chip, at] = mm(prob.astype(BF16), v).astype(BF16)
        PF[chip] = mm(O[chip], Wo[par])

    def attn_bwd(chip, par):
        grad_o2 = mm_t(D1[chip], Wo[par]).astype(BF16)
        for s in range(2):
            at = slice(s * rows, (s + 1) * rows)
            grad_o = grad_o2[at]
            q = QKV[chip, at, 0:head]
            kk = QKV[chip, at, head:2 * head]
            v = QKV[chip, at, 2 * head:3 * head]
            prob = PROB[chip, at]
            grad_p = mm_t(grad_o, v)
            grad_s = (prob * (grad_p - jnp.sum(grad_p * prob, axis=-1, keepdims=True)) * scale).astype(BF16)
            GQ[chip, at, 0:head] = mm(grad_s, kk).astype(BF16)
            GQ[chip, at, head:2 * head] = tmm(grad_s, q).astype(BF16)
            GQ[chip, at, 2 * head:3 * head] = tmm(prob.astype(BF16), grad_o).astype(BF16)
        PB[chip] = mm_t(GQ[chip], Wqkv[par]).astype(BF16)

    def flat(x):
        return x.reshape((x.shape[0] * x.shape[1],) + x.shape[2:])

    def mlp_wgrad(layer, par, not_first):
        @pl.when(not_first)
        def _():
            grad_copy(layer, 2).wait()
            grad_copy(layer, 3).wait()
        tile = width // 4

        def up(i, _):
            at = pl.ds(pl.multiple_of(i * tile, tile), tile)
            Gu[at] = tmm(flat(N1[par, :, :, at]), flat(GH[...]))
            return 0

        def down(i, _):
            at = pl.ds(pl.multiple_of(i * tile, tile), tile)
            Gd[:, at] = tmm(flat(ACT[...]), flat(D2[:, :, at]))
            return 0
        lax.fori_loop(0, 4, up, 0)
        grad_copy(layer, 2).start()
        lax.fori_loop(0, 4, down, 0)
        grad_copy(layer, 3).start()

    def attn_wgrad(layer, par, not_first):
        @pl.when(not_first)
        def _():
            grad_copy(layer, 0).wait()
            grad_copy(layer, 1).wait()
        tile = width // 4

        def qkv(i, _):
            at = pl.ds(pl.multiple_of(i * tile, tile), tile)
            res = tmm(flat(N2[par, :, :, at]), flat(GQ[...]))
            for j in range(3):
                Gqkv[pl.ds(i * (3 * tile) + j, tile, stride=3), :] = res[:, j * head:(j + 1) * head]
            return 0

        def out(i, _):
            at = pl.ds(pl.multiple_of(i * tile, tile), tile)
            Go[:, at] = tmm(flat(O[...]), flat(D1[:, :, at]))
            return 0
        lax.fori_loop(0, 4, qkv, 0)
        grad_copy(layer, 0).start()
        lax.fori_loop(0, 4, out, 0)
        grad_copy(layer, 1).start()

    def own_rows(step):
        def body(r, _):
            step(r, pl.ds(pl.multiple_of(r * 16, 16), 16), pl.ds(pl.multiple_of(k * rows + r * 16, 16), 16))
            return 0
        lax.fori_loop(0, rows // 16, body, 0)

    def inv_rms(x):
        return lax.rsqrt(jnp.mean(x * x, axis=-1, keepdims=True) + NORM_EPS)

    def finish_state(rs, old, new, norm_to):
        rs.land()

        def step(r, loc, at):
            x = old[loc] - rs.total(r)
            new[loc] = x
            if norm_to is not None:
                norm_to[c, at] = (x * inv_rms(x)).astype(BF16)
        own_rows(step)
        rs.drain()

    def finish_cot(rs, cot, x_ref, cast_to):
        rs.land()

        def step(r, loc, at):
            x = x_ref[loc]
            inv = inv_rms(x)
            normed = x * inv
            grad_n = rs.total(r)
            new = cot[loc] + inv * (grad_n - normed * jnp.mean(normed * grad_n, axis=-1, keepdims=True))
            cot[loc] = new
            if cast_to is not None:
                cast_to[c, at] = new.astype(BF16)
        own_rows(step)
        rs.drain()

    def when(cond, fn):
        if cond is True:
            fn()
        elif cond is not False:
            pl.when(cond)(fn)

    def partials(rs, compute, early):
        def body(j, _):
            chip = order(j)
            compute(chip)
            rs.pair(chip).start()
            if early:
                pl.when(j == 1)(rs.send_opp)
            return 0
        lax.fori_loop(0, NCHIP, body, 0)

    def half_step(ag_n, fin_n, ag_d, fin_d, fwd, bwd, wgrad, has_d):
        fin_n()
        ag_n.start()
        when(has_d, rs_b.send_relay)
        ag_n.near()

        def d_start():
            fin_d()
            ag_d.start()
        when(has_d, d_start)
        ag_n.far()
        ag_n.finish()
        partials(rs_f, fwd, True)
        when(has_d, ag_d.near)
        rs_f.send_direct()
        rs_f.send_relay()

        def d_end():
            ag_d.far()
            ag_d.finish()
        when(has_d, d_end)
        partials(rs_b, bwd, False)
        rs_b.send_opp()
        rs_b.send_direct()
        wgrad()

    def stage_attn(layer, par, not_first, last):
        q = 1 - par
        if not last:
            for cp in weight_copies(layer - 1, q):
                cp.start()
        half_step(
            gather_n(N2, par, 0), lambda: finish_state(rs_f, Y2.at[q], Y2.at[par], N2.at[par]),
            gather_d(D2, 1), lambda: finish_cot(rs_b, C2, Y2.at[q], D2),
            lambda chip: attn_fwd(chip, par), lambda chip: mlp_bwd(chip, par),
            lambda: mlp_wgrad(layer, par, not_first), not_first)

    def stage_mlp(layer, par, not_first):
        q = 1 - par

        def fin():
            finish_state(rs_f, Y1.at[par], Y1.at[q], N1.at[q])
            for cp in weight_copies(layer - 1, q):
                cp.wait()
        half_step(
            gather_n(N1, q, 2), fin,
            gather_d(D1, 3), lambda: finish_cot(rs_b, C1, Y1.at[par], D1),
            lambda chip: mlp_fwd(chip, q), lambda chip: attn_bwd(chip, par),
            lambda: attn_wgrad(layer, par, not_first), True)

    top = layers - 1
    tp = top % 2
    for cp in weight_copies(top, tp):
        cp.start()
    loads = [pltpu.make_async_copy(src.at[me], dst, own_sem.at[i]) for i, (src, dst) in enumerate(
        ((y1_hbm, Y1.at[tp]), (y2_hbm, Y2.at[1 - tp]), (c1_hbm, C1), (c2_hbm, C2)))]
    for cp in loads:
        cp.start()

    def load_y1(chip, s):
        return pltpu.make_async_copy(y1_hbm.at[2 * chip + s], PF.at[chip, pl.ds(s * rows, rows)], io_sem.at[0, chip, s])

    batch = Gd.shape[0] // rows

    def load_c2(b, i):
        return pltpu.make_async_copy(c2_hbm.at[b * batch + i], Gd.at[pl.ds(i * rows, rows)],
                                     io_sem.at[1, i // 2, i % 2])

    def top_fwd(chip):
        for s in range(2):
            load_y1(chip, s).wait()

        def norm(i, _):
            at = pl.ds(pl.multiple_of(i * 16, 16), 16)
            x = PF[chip, at]
            N1[tp, chip, at] = (x * inv_rms(x)).astype(BF16)
            return 0
        lax.fori_loop(0, 2 * rows // 16, norm, 0)
        mlp_fwd(chip, tp)

    def cast_c2(b):
        for i in range(batch):
            load_c2(b, i).wait()

        def cast(i, _):
            for n in range(batch // 2):
                at = pl.ds(pl.multiple_of(i * 16, 16), 16)
                D2[b * (batch // 2) + n, at] = Gd[pl.ds(pl.multiple_of(n * 2 * rows + i * 16, 16), 16)].astype(BF16)
            return 0
        lax.fori_loop(0, 2 * rows // 16, cast, 0)
        if b + 1 < 2 * NCHIP // batch:
            for i in range(batch):
                load_c2(b + 1, i).start()

    def start_y1(j, _):
        for s in range(2):
            load_y1(order(j), s).start()
        return 0
    lax.fori_loop(0, NCHIP, start_y1, 0)
    for i in range(batch):
        load_c2(0, i).start()
    for cp in weight_copies(top, tp):
        cp.wait()
    partials(rs_f, top_fwd, True)
    rs_f.send_direct()
    cast_c2(0)
    rs_f.send_relay()
    for b in range(1, 2 * NCHIP // batch):
        cast_c2(b)
    for cp in loads:
        cp.wait()

    def layer_body(i, _):
        layer = top - i
        par = lax.rem(layer, 2)
        stage_attn(layer, par, layer < top, False)
        stage_mlp(layer, par, layer < top)
        return 0
    lax.fori_loop(0, top, layer_body, 0)

    stage_attn(0, 0, True, True)
    outs = [gather_out(o, i) for i, o in enumerate((x1_out, x2_out, g1_out, g2_out))]

    def put(i, src):
        out = (x1_out, x2_out, g1_out, g2_out)[i]
        at = pl.ds(pl.multiple_of(me * rows, rows), rows)
        pltpu.make_async_copy(src, out.at[at], own_sem.at[i]).start()
        for n, dev in enumerate((left, right, sib)):
            remote(src, out.at[at], fg_send.at[i, n], fg_recv.at[i, n], dev).start()

    def put_done(i, src):
        out = (x1_out, x2_out, g1_out, g2_out)[i]
        at = pl.ds(pl.multiple_of(me * rows, rows), rows)
        pltpu.make_async_copy(src, out.at[at], own_sem.at[i]).wait()

    ag_d1 = gather_d(D1, 3)
    finish_state(rs_f, Y1.at[0], Y1.at[1], None)
    rs_b.send_relay()
    put(1, Y2.at[0])
    finish_cot(rs_b, C1, Y1.at[0], D1)
    ag_d1.start()
    put(0, Y1.at[1])
    ag_d1.near()
    outs[1].near()
    ag_d1.far()
    ag_d1.finish()
    partials(rs_b, lambda chip: attn_bwd(chip, 0), False)
    rs_b.send_opp()
    rs_b.send_direct()
    put(2, C1)
    attn_wgrad(0, 0, True)
    outs[0].near()
    rs_b.send_relay()
    outs[1].far()
    finish_cot(rs_b, C2, Y2.at[0], None)
    put(3, C2)
    outs[0].far()
    outs[2].near()
    outs[3].near()
    outs[2].far()
    outs[3].far()
    for i, src in enumerate((Y1.at[1], Y2.at[0], C1, C2)):
        outs[i].finish()
        put_done(i, src)
    for i in range(4):
        grad_copy(0, i).wait()


def solution(mesh):
    act_spec = P("dp", None, None)
    weight_specs = (P(None, None, "tp", None, None), P(None, "tp", None, None), P(None, None, "tp"), P(None, "tp", None))
    grad_specs = (P("dp", None, "tp", None, None), P("dp", "tp", None, None), P("dp", None, "tp"), P("dp", "tp", None))

    def local_backward(out_y1, out_y2, cot_y1, cot_y2, w_qkv, w_out, w_up, w_down):
        seqs, rows, width = out_y1.shape
        layers, _, heads, three, head = w_qkv.shape
        hidden = w_up.shape[2]
        wq = jnp.transpose(w_qkv.reshape(layers, width, three, head), (0, 2, 1, 3))
        wo = w_out.reshape(layers, heads * head, width)
        pair = 2 * rows
        qkv_w = three * head
        act = jax.ShapeDtypeStruct((seqs * rows, width), F32)
        dma = pltpu.SemaphoreType.DMA
        outs = pl.pallas_call(
            kernel,
            out_shape=(act, act, act, act,
                       jax.ShapeDtypeStruct((layers * width * three, head), F32),
                       jax.ShapeDtypeStruct((layers, head, width), F32),
                       jax.ShapeDtypeStruct((layers, width, hidden), F32),
                       jax.ShapeDtypeStruct((layers, hidden, width), F32)),
            in_specs=[pl.BlockSpec(memory_space=pl.ANY)] * 8,
            out_specs=[pl.BlockSpec(memory_space=pl.ANY)] * 8,
            scratch_shapes=[
                pltpu.VMEM((2, NCHIP, pair, width), BF16),
                pltpu.VMEM((2, NCHIP, pair, width), BF16),
                pltpu.VMEM((NCHIP, pair, width), BF16),
                pltpu.VMEM((NCHIP, pair, width), BF16),
                pltpu.VMEM((2, width, qkv_w), BF16),
                pltpu.VMEM((2, head, width), BF16),
                pltpu.VMEM((2, width, hidden), BF16),
                pltpu.VMEM((2, hidden, width), BF16),
                pltpu.VMEM((width * three, head), F32),
                pltpu.VMEM((head, width), F32),
                pltpu.VMEM((width, hidden), F32),
                pltpu.VMEM((hidden, width), F32),
                pltpu.VMEM((NCHIP, pair, hidden), F32),
                pltpu.VMEM((NCHIP, pair, hidden), BF16),
                pltpu.VMEM((NCHIP, pair, hidden), BF16),
                pltpu.VMEM((NCHIP, pair, qkv_w), BF16),
                pltpu.VMEM((NCHIP, pair, rows), F32),
                pltpu.VMEM((NCHIP, pair, head), BF16),
                pltpu.VMEM((NCHIP, pair, qkv_w), BF16),
                pltpu.VMEM((2, rows, width), F32),
                pltpu.VMEM((2, rows, width), F32),
                pltpu.VMEM((rows, width), F32),
                pltpu.VMEM((rows, width), F32),
                pltpu.VMEM((NCHIP, pair, width), F32),
                pltpu.VMEM((NCHIP, pair, width), BF16),
                pltpu.VMEM((NCHIP, rows, width), F32),
                pltpu.VMEM((NCHIP, rows, width), BF16),
                pltpu.VMEM((3, rows, width), F32),
                pltpu.VMEM((3, rows, width), BF16),
                dma((4, 9)), dma((4, 9)), dma((2, 10)), dma((2, 10)), dma((4, 9)), dma((4, 9)),
                dma((2, 6)), dma((4,)), dma((2, NCHIP, 2)), dma((4,)),
            ],
            compiler_params=pltpu.CompilerParams(collective_id=0, has_side_effects=True,
                                                 vmem_limit_bytes=60 * 1024 * 1024),
        )(out_y1, out_y2, cot_y1, cot_y2, wq, wo, w_up, w_down)
        x1, x2, g1, g2 = (o.reshape(seqs, rows, width) for o in outs[:4])
        return (x1, x2, g1, g2, outs[4].reshape(w_qkv.shape), outs[5].reshape(w_out.shape), outs[6], outs[7])

    return jax.shard_map(local_backward, mesh=mesh, in_specs=(act_spec, act_spec, act_spec, act_spec) + weight_specs, out_specs=(act_spec, act_spec, act_spec, act_spec) + grad_specs, check_vma=False)
```

```python
import functools
import math
import jax
import jax.numpy as jnp
from jax import lax
from jax.experimental import pallas as pl
from jax.experimental.pallas import tpu as pltpu
from jax.sharding import PartitionSpec as P

NORM_EPS = 1e-6
F32, BF16 = jnp.float32, jnp.bfloat16
GELU_C = math.sqrt(2.0 / math.pi)
GELU_A = 0.044715
NCHIP = 4


def mm(a, b):
    return lax.dot_general(a, b, (((1,), (0,)), ((), ())), preferred_element_type=F32)


def mm_t(a, b):
    return lax.dot_general(a, b, (((1,), (1,)), ((), ())), preferred_element_type=F32)


def tmm(a, b):
    return lax.dot_general(a, b, (((0,), (0,)), ((), ())), preferred_element_type=F32)


def kernel(groups, y1_hbm, y2_hbm, c1_hbm, c2_hbm, wqkv_hbm, wo_hbm, wu_hbm, wd_hbm,
           x1_out, x2_out, g1_out, g2_out, gqkv_out, gout_out, gup_out, gdown_out, wof_hbm,
           N1, N2, D1, D2, Wqkv, Wo, Wu, Wd, Gqkv, Go, Gu, Gd, H, ACT, GH, QKV, PROB, O, GQ,
           Y1, Y2, C1, C2, PF, PB, XF, XB, RF, RB, VG, WoV, OF, FT,
           ag_send, ag_recv, rs_send, rs_recv, fg_send, fg_recv, w_sem, g_sem, io_sem, own_sem,
           wg_send, wg_recv, wx_send, wx_recv, wl_sem, o_send, o_recv):
    layers = wqkv_hbm.shape[0]
    rows = y1_hbm.shape[1]
    half = rows // 2
    width = y1_hbm.shape[2]
    head = wo_hbm.shape[1]
    scale = 1.0 / math.sqrt(head)
    ndev = 2 * NCHIP
    me = lax.axis_index("tp")
    c = me // 2
    k = lax.rem(me, 2)
    sib = me + 1 - 2 * k
    left = lax.rem(me + ndev - 2, ndev)
    right = lax.rem(me + 2, ndev)
    cl = lax.rem(c + NCHIP - 1, NCHIP)
    cr = lax.rem(c + 1, NCHIP)
    co = lax.rem(c + 2, NCHIP)
    mine = pl.ds(pl.multiple_of(k * rows, rows), rows)
    other = pl.ds(pl.multiple_of((1 - k) * rows, rows), rows)

    def my_half(h):
        return pl.ds(pl.multiple_of(k * rows + h * half, half), half)

    def order(j):
        off = (2 + j) * (1 - j // 2) + (3 - j) * (j // 2)
        return lax.rem(c + off, NCHIP)

    def remote(src, dst, ssem, rsem, dev):
        return pltpu.make_async_remote_copy(src_ref=src, dst_ref=dst, send_sem=ssem, recv_sem=rsem,
                                            device_id={"tp": dev}, device_id_type=pl.DeviceIdType.MESH)

    grp = lax.axis_index("dp")
    barrier = pltpu.get_barrier_semaphore()

    def hello(axis, at, n):
        def one(i, _):
            pl.semaphore_signal(barrier, inc=1, device_id={axis: lax.rem(at + i, n)},
                                device_id_type=pl.DeviceIdType.MESH)
            return 0
        lax.fori_loop(1, n, one, 0)
    hello("tp", me, ndev)
    hello("dp", grp, groups)
    pl.semaphore_wait(barrier, ndev - 1 + groups - 1)

    class Gather:
        def __init__(self, view, ssem, rsem):
            def full(chip):
                return view(chip, (k, None))

            def sibrows(chip):
                return view(chip, (1 - k, None))

            def hf(chip, h):
                return view(chip, (k, h))

            def ohf(chip, h):
                return view(chip, (1 - k, h))

            self.send = [
                remote(full(c), full(c), ssem.at[0], rsem.at[0], left),
                remote(full(c), full(c), ssem.at[1], rsem.at[1], right),
                remote(full(c), full(c), ssem.at[2], rsem.at[2], sib),
                remote(hf(cr, 0), hf(cr, 0), ssem.at[3], rsem.at[3], left),
                remote(full(cr), full(cr), ssem.at[4], rsem.at[4], sib),
                remote(hf(cl, 1), hf(cl, 1), ssem.at[5], rsem.at[5], right),
                remote(full(cl), full(cl), ssem.at[6], rsem.at[6], sib),
                remote(hf(co, 0), hf(co, 0), ssem.at[7], rsem.at[7], sib),
                remote(hf(co, 1), hf(co, 1), ssem.at[8], rsem.at[8], sib),
            ]
            land = [full(cr), full(cl), sibrows(c), hf(co, 0), sibrows(cr), hf(co, 1), sibrows(cl),
                    ohf(co, 0), ohf(co, 1)]
            self.recv = [remote(r, r, ssem.at[i], rsem.at[i], sib) for i, r in enumerate(land)]

        def start(self):
            for i in (0, 1, 2):
                self.send[i].start()

        def near(self):
            self.recv[0].wait_recv()
            self.send[3].start()
            self.send[4].start()
            self.recv[1].wait_recv()
            self.send[5].start()
            self.send[6].start()

        def far(self):
            self.recv[3].wait_recv()
            self.send[7].start()
            self.recv[5].wait_recv()
            self.send[8].start()

        def finish(self):
            for i in (2, 4, 6, 7, 8):
                self.recv[i].wait_recv()
            for cp in self.send:
                cp.wait_send()

    class Scatter:
        def __init__(self, part, from_sib, rec, ssem, rsem):
            self.part, self.from_sib = part, from_sib
            self.rel, self.dir, self.fin = rec.at[0], rec.at[1], rec.at[2]
            self.ssem, self.rsem = ssem, rsem

            def hp(chip, h):
                return part.at[chip, my_half(h)]

            def hr(buf, h):
                return buf.at[pl.ds(h * half, half)]

            def mk(i, src, dst, dev):
                return remote(src, dst, ssem.at[i], rsem.at[i], dev)

            self.opp = [mk(4, hp(co, 0), hr(self.rel, 0), left), mk(5, hp(co, 1), hr(self.rel, 1), right)]
            self.direct = [mk(6, hp(cl, 1), hr(self.dir, 1), left), mk(7, hp(cr, 0), hr(self.dir, 0), right)]
            self.relay = [mk(8, hp(cl, 0), hr(self.fin, 0), left), mk(9, hp(cr, 1), hr(self.fin, 1), right)]

        def pair(self, chip):
            return remote(self.part.at[chip, other], self.from_sib.at[chip], self.ssem.at[chip],
                          self.rsem.at[chip], sib)

        def add(self, chip):
            self.pair_recv(chip)
            got = self.part[chip, mine].astype(F32) + self.from_sib[chip].astype(F32)
            self.part[chip, mine] = got.astype(self.part.dtype)

        def pair_recv(self, chip):
            remote(self.from_sib.at[chip], self.from_sib.at[chip], self.ssem.at[chip], self.rsem.at[chip],
                   sib).wait_recv()

        def send_opp(self):
            self.add(co)
            for cp in self.opp:
                cp.start()

        def send_direct(self):
            self.add(cl)
            self.direct[0].start()
            self.add(cr)
            self.direct[1].start()

        def send_relay(self):
            for h, (chip, cp) in enumerate(((cl, self.relay[0]), (cr, self.relay[1]))):
                self.opp[h].wait_recv()
                got = self.part[chip, my_half(h)].astype(F32) + self.rel[h * half:(h + 1) * half].astype(F32)
                self.part[chip, my_half(h)] = got.astype(self.part.dtype)
                cp.start()

        def land(self):
            self.pair_recv(c)
            for cp in self.direct + self.relay:
                cp.wait_recv()

        def total(self, r):
            at = pl.ds(pl.multiple_of(k * rows + r * 16, 16), 16)
            loc = pl.ds(pl.multiple_of(r * 16, 16), 16)
            return (self.part[c, at].astype(F32) + self.from_sib[c, loc].astype(F32)
                    + self.fin[loc].astype(F32) + self.dir[loc].astype(F32))

        def drain(self):
            for chip in range(NCHIP):
                self.pair(chip).wait_send()
            for cp in self.opp + self.direct + self.relay:
                cp.wait_send()

    rs_f = Scatter(PF, XF, RF, rs_send.at[0], rs_recv.at[0])
    rs_b = Scatter(PB, XB, RB, rs_send.at[1], rs_recv.at[1])

    def span(r):
        if r[1] is None:
            return pl.ds(pl.multiple_of(r[0] * rows, rows), rows)
        return pl.ds(pl.multiple_of(r[0] * rows + r[1] * half, half), half)

    def gather_n(buf, par, i):
        return Gather(lambda chip, r: buf.at[par, chip, span(r)], ag_send.at[i], ag_recv.at[i])

    def gather_d(buf, i):
        return Gather(lambda chip, r: buf.at[chip, span(r)], ag_send.at[i], ag_recv.at[i])

    def gather_out(out, i):
        def view(chip, r):
            at = span(r)
            return out.at[pl.ds(pl.multiple_of(chip * 2 * rows, rows) + at.start, at.size)]
        return Gather(view, fg_send.at[i], fg_recv.at[i])

    lanes = 128
    piece = width * head // (lanes * groups)

    def own_piece_copies(layer):
        if piece >= head:
            n = piece // head
            return [pltpu.make_async_copy(
                wo_hbm.at[layer, :, pl.ds(pl.multiple_of((grp * n + b) * lanes, lanes), lanes)],
                VG.at[me, pl.ds(layer * piece + b * head, head)], wl_sem.at[layer * n + b]) for b in range(n)]
        n = head // piece
        return [pltpu.make_async_copy(
            wo_hbm.at[layer, pl.ds(pl.multiple_of(lax.rem(grp, n) * piece, piece), piece),
                      pl.ds(pl.multiple_of((grp // n) * lanes, lanes), lanes)],
            VG.at[me, pl.ds(layer * piece, piece)], wl_sem.at[layer])]

    def vg_view(chip, r):
        dev = 2 * chip + r[0]
        n = layers * piece
        if r[1] is None:
            return VG.at[dev]
        return VG.at[dev, pl.ds(r[1] * (n // 2), n // 2)]

    def piece_send(layer, d):
        return pltpu.make_async_remote_copy(
            src_ref=VG.at[:, pl.ds(layer * piece, piece)], dst_ref=wof_hbm.at[layer, grp],
            send_sem=wx_send.at[layer, d], recv_sem=wx_recv.at[layer, d],
            device_id={"dp": lax.rem(grp + d, groups), "tp": me}, device_id_type=pl.DeviceIdType.MESH)

    def piece_keep(layer):
        return pltpu.make_async_copy(VG.at[:, pl.ds(layer * piece, piece)], wof_hbm.at[layer, grp],
                                     wx_send.at[layer, 0])

    def pieces_out():
        for layer in reversed(range(layers)):
            piece_keep(layer).start()

            def one(d, _):
                piece_send(layer, d).start()
                return 0
            lax.fori_loop(1, groups, one, 0)

    def pieces_sent():
        for layer in range(layers):
            def one(d, _):
                piece_send(layer, d).wait_send()
                return 0
            lax.fori_loop(1, groups, one, 0)

    def pieces_in(layer):
        def one(d, _):
            pltpu.make_async_remote_copy(
                src_ref=wof_hbm.at[layer, grp], dst_ref=wof_hbm.at[layer, lax.rem(grp + groups - d, groups)],
                send_sem=wx_send.at[layer, d], recv_sem=wx_recv.at[layer, d],
                device_id={"dp": grp, "tp": me}, device_id_type=pl.DeviceIdType.MESH).wait_recv()
            return 0
        piece_keep(layer).wait()
        lax.fori_loop(1, groups, one, 0)

    def wov_copies(layer):
        if piece >= head:
            n = piece // head
            return [pltpu.make_async_copy(wof_hbm.at[layer, g, :, pl.ds(b * head, head)],
                                          WoV.at[:, :, pl.ds((g * n + b) * lanes, lanes)], wl_sem.at[g * n + b])
                    for g in range(groups) for b in range(n)]
        n = head // piece
        return [pltpu.make_async_copy(wof_hbm.at[layer, g],
                                      WoV.at[:, pl.ds((g % n) * piece, piece), pl.ds((g // n) * lanes, lanes)],
                                      wl_sem.at[g]) for g in range(groups)]

    def o_copy(chip, s):
        return remote(O.at[chip, pl.ds(s * rows, rows)], OF.at[:, pl.ds(pl.multiple_of(me * head, head), head)],
                      o_send.at[2 * chip + s], o_recv.at[me], 2 * chip + s)

    def o_wait_recv():
        def one(i, _):
            src = lax.rem(me + i, ndev)
            at = OF.at[:, pl.ds(pl.multiple_of(src * head, head), head)]
            remote(at, at, o_send.at[src], o_recv.at[src], src).wait_recv()
            return 0
        lax.fori_loop(1, ndev, one, 0)

    def o_wait_send():
        def one(i, _):
            dst = lax.rem(me + i, ndev)
            at = O.at[dst // 2, pl.ds(pl.multiple_of(lax.rem(dst, 2) * rows, rows), rows)]
            remote(at, at, o_send.at[dst], o_recv.at[dst], dst).wait_send()
            return 0
        lax.fori_loop(1, ndev, one, 0)

    def weight_copies(layer, slot):
        pairs = [(src.at[layer], dst.at[slot]) for src, dst in ((wo_hbm, Wo), (wu_hbm, Wu), (wd_hbm, Wd))]
        pairs += [(wqkv_hbm.at[layer, j], Wqkv.at[slot, :, pl.ds(j * head, head)]) for j in range(3)]
        return [pltpu.make_async_copy(src, dst, w_sem.at[slot, i]) for i, (src, dst) in enumerate(pairs)]

    def grad_copy(layer, i):
        src, dst = ((Gqkv, gqkv_out), (Go, gout_out), (Gu, gup_out), (Gd, gdown_out))[i]
        if i == 0:
            size = src.shape[0]
            return pltpu.make_async_copy(src, dst.at[pl.ds(pl.multiple_of(layer * size, size), size)], g_sem.at[i])
        return pltpu.make_async_copy(src, dst.at[layer], g_sem.at[i])

    def mlp_fwd(chip, par):
        hid = mm(N1[par, chip], Wu[par])
        H[chip] = hid
        act = hid * (0.5 * (1.0 + jnp.tanh(GELU_C * (hid + GELU_A * (hid * hid * hid)))))
        act = act.astype(BF16)
        ACT[chip] = act
        PF[chip] = mm(act, Wd[par])

    def mlp_bwd(chip, par):
        grad_act = mm_t(D2[chip], Wd[par])
        hid = H[chip]
        sq = hid * hid
        t = jnp.tanh(GELU_C * (hid + GELU_A * (sq * hid)))
        slope = 0.5 * (1.0 + t) + (0.5 * hid) * ((1.0 - t * t) * (GELU_C * (1.0 + (3.0 * GELU_A) * sq)))
        grad_hid = (grad_act * slope).astype(BF16)
        GH[chip] = grad_hid
        PB[chip] = mm_t(grad_hid, Wu[par]).astype(BF16)

    def attn_fwd(chip, par):
        QKV[chip] = mm(N2[par, chip], Wqkv[par]).astype(BF16)
        for s in range(2):
            at = slice(s * rows, (s + 1) * rows)
            q = QKV[chip, at, 0:head]
            kk = QKV[chip, at, head:2 * head]
            v = QKV[chip, at, 2 * head:3 * head]
            sc = mm_t(q, kk) * scale
            e = jnp.exp(sc - jnp.max(sc, axis=-1, keepdims=True))
            prob = e / jnp.sum(e, axis=-1, keepdims=True)
            PROB[chip, at] = prob
            O[chip, at] = mm(prob.astype(BF16), v).astype(BF16)

            @pl.when(2 * chip + s != me)
            def _():
                o_copy(chip, s).start()

            @pl.when(2 * chip + s == me)
            def _():
                OF[:, pl.ds(pl.multiple_of(me * head, head), head)] = O[chip, at]

    def attn_bwd(chip, par):
        grad_o2 = mm_t(D1[chip], Wo[par]).astype(BF16)
        for s in range(2):
            at = slice(s * rows, (s + 1) * rows)
            grad_o = grad_o2[at]
            q = QKV[chip, at, 0:head]
            kk = QKV[chip, at, head:2 * head]
            v = QKV[chip, at, 2 * head:3 * head]
            prob = PROB[chip, at]
            grad_p = mm_t(grad_o, v)
            grad_s = (prob * (grad_p - jnp.sum(grad_p * prob, axis=-1, keepdims=True)) * scale).astype(BF16)
            GQ[chip, at, 0:head] = mm(grad_s, kk).astype(BF16)
            GQ[chip, at, head:2 * head] = tmm(grad_s, q).astype(BF16)
            GQ[chip, at, 2 * head:3 * head] = tmm(prob.astype(BF16), grad_o).astype(BF16)
        PB[chip] = mm_t(GQ[chip], Wqkv[par]).astype(BF16)

    def flat(x):
        return x.reshape((x.shape[0] * x.shape[1],) + x.shape[2:])

    def mlp_wgrad(layer, par, not_first):
        @pl.when(not_first)
        def _():
            grad_copy(layer, 2).wait()
            grad_copy(layer, 3).wait()
        tile = width // 4

        def up(i, _):
            at = pl.ds(pl.multiple_of(i * tile, tile), tile)
            Gu[at] = tmm(flat(N1[par, :, :, at]), flat(GH[...]))
            return 0

        def down(i, _):
            at = pl.ds(pl.multiple_of(i * tile, tile), tile)
            Gd[:, at] = tmm(flat(ACT[...]), flat(D2[:, :, at]))
            return 0
        lax.fori_loop(0, 4, up, 0)
        grad_copy(layer, 2).start()
        lax.fori_loop(0, 4, down, 0)
        grad_copy(layer, 3).start()

    def attn_wgrad(layer, par, not_first):
        @pl.when(not_first)
        def _():
            grad_copy(layer, 0).wait()
            grad_copy(layer, 1).wait()
        tile = width // 4

        def qkv(i, _):
            at = pl.ds(pl.multiple_of(i * tile, tile), tile)
            res = tmm(flat(N2[par, :, :, at]), flat(GQ[...]))
            for j in range(3):
                Gqkv[pl.ds(i * (3 * tile) + j, tile, stride=3), :] = res[:, j * head:(j + 1) * head]
            return 0

        def out(i, _):
            at = pl.ds(pl.multiple_of(i * tile, tile), tile)
            Go[:, at] = tmm(flat(O[...]), flat(D1[:, :, at]))
            return 0
        lax.fori_loop(0, 4, qkv, 0)
        grad_copy(layer, 0).start()
        lax.fori_loop(0, 4, out, 0)
        grad_copy(layer, 1).start()

    def own_rows(step):
        def body(r, _):
            step(r, pl.ds(pl.multiple_of(r * 16, 16), 16), pl.ds(pl.multiple_of(k * rows + r * 16, 16), 16))
            return 0
        lax.fori_loop(0, rows // 16, body, 0)

    def inv_rms(x):
        return lax.rsqrt(jnp.mean(x * x, axis=-1, keepdims=True) + NORM_EPS)

    def finish_state(rs, old, new, norm_to):
        rs.land()

        def step(r, loc, at):
            x = old[loc] - rs.total(r)
            new[loc] = x
            if norm_to is not None:
                norm_to[c, at] = (x * inv_rms(x)).astype(BF16)
        own_rows(step)
        rs.drain()

    def finish_cot(rs, cot, x_ref, cast_to):
        rs.land()

        def step(r, loc, at):
            x = x_ref[loc]
            inv = inv_rms(x)
            normed = x * inv
            grad_n = rs.total(r)
            new = cot[loc] + inv * (grad_n - normed * jnp.mean(normed * grad_n, axis=-1, keepdims=True))
            cot[loc] = new
            if cast_to is not None:
                cast_to[c, at] = new.astype(BF16)
        own_rows(step)
        rs.drain()

    def when(cond, fn):
        if cond is True:
            fn()
        elif cond is not False:
            pl.when(cond)(fn)

    def partials(rs, compute, early):
        def body(j, _):
            chip = order(j)
            compute(chip)
            rs.pair(chip).start()
            if early:
                pl.when(j == 1)(rs.send_opp)
            return 0
        lax.fori_loop(0, NCHIP, body, 0)

    def attn_apply(old, new, norm_to):
        o_wait_recv()
        tile = width // 4

        def tiles(i, _):
            at = pl.ds(pl.multiple_of(i * tile, tile), tile)
            FT[:, at] = mm(OF[...], flat(WoV[:, :, at]))
            return 0
        lax.fori_loop(0, 4, tiles, 0)

        def step(r, loc, at):
            x = old[loc] - FT[loc]
            new[loc] = x
            if norm_to is not None:
                norm_to[c, at] = (x * inv_rms(x)).astype(BF16)
        own_rows(step)
        o_wait_send()

    def top_half(layer, par, not_first, last):
        q = 1 - par
        ag_n = gather_n(N2, par, 0)
        ag_d = gather_d(D2, 1)
        ag_next = gather_n(N1, q, 2)
        finish_state(rs_f, Y2.at[q], Y2.at[par], N2.at[par])
        ag_n.start()
        if not last:
            for cp in weight_copies(layer - 1, q):
                cp.start()
        when(not_first, rs_b.send_relay)
        ag_n.near()

        def d_start():
            finish_cot(rs_b, C2, Y2.at[q], D2)
            ag_d.start()
        when(not_first, d_start)
        pieces_in(layer)
        for cp in wov_copies(layer):
            cp.start()
        ag_n.far()
        ag_n.finish()

        def fwd(j, _):
            attn_fwd(order(j), par)
            return 0
        lax.fori_loop(0, NCHIP, fwd, 0)
        when(not_first, ag_d.near)
        for cp in wov_copies(layer):
            cp.wait()
        if last:
            attn_apply(Y1.at[par], Y1.at[q], None)
        else:
            attn_apply(Y1.at[par], Y1.at[q], N1.at[q])
            ag_next.start()

        def d_end():
            ag_d.far()
            ag_d.finish()
        when(not_first, d_end)
        partials(rs_b, lambda chip: mlp_bwd(chip, par), False)
        rs_b.send_opp()
        rs_b.send_direct()

    def low_half(layer, par, not_first):
        q = 1 - par
        ag_n = gather_n(N1, q, 2)
        ag_d = gather_d(D1, 3)
        ag_n.near()
        mlp_wgrad(layer, par, not_first)
        rs_b.send_relay()
        ag_n.far()
        ag_n.finish()
        finish_cot(rs_b, C1, Y1.at[par], D1)
        ag_d.start()
        for cp in weight_copies(layer - 1, q):
            cp.wait()
        partials(rs_f, lambda chip: mlp_fwd(chip, q), True)
        ag_d.near()
        rs_f.send_direct()
        rs_f.send_relay()
        ag_d.far()
        ag_d.finish()
        partials(rs_b, lambda chip: attn_bwd(chip, par), False)
        rs_b.send_opp()
        rs_b.send_direct()
        attn_wgrad(layer, par, not_first)

    top = layers - 1
    tp = top % 2
    for layer in range(layers):
        for cp in own_piece_copies(layer):
            cp.start()
    for cp in weight_copies(top, tp):
        cp.start()
    loads = [pltpu.make_async_copy(src.at[me], dst, own_sem.at[i]) for i, (src, dst) in enumerate(
        ((y1_hbm, Y1.at[tp]), (y2_hbm, Y2.at[1 - tp]), (c1_hbm, C1), (c2_hbm, C2)))]
    for cp in loads:
        cp.start()

    def load_y1(chip, s):
        return pltpu.make_async_copy(y1_hbm.at[2 * chip + s], PF.at[chip, pl.ds(s * rows, rows)], io_sem.at[0, chip, s])

    batch = Gd.shape[0] // rows

    def load_c2(b, i):
        return pltpu.make_async_copy(c2_hbm.at[b * batch + i], Gd.at[pl.ds(i * rows, rows)],
                                     io_sem.at[1, i // 2, i % 2])

    def top_fwd(chip):
        for s in range(2):
            load_y1(chip, s).wait()

        def norm(i, _):
            at = pl.ds(pl.multiple_of(i * 16, 16), 16)
            x = PF[chip, at]
            N1[tp, chip, at] = (x * inv_rms(x)).astype(BF16)
            return 0
        lax.fori_loop(0, 2 * rows // 16, norm, 0)
        mlp_fwd(chip, tp)

    def cast_c2(b):
        for i in range(batch):
            load_c2(b, i).wait()

        def cast(i, _):
            for n in range(batch // 2):
                at = pl.ds(pl.multiple_of(i * 16, 16), 16)
                D2[b * (batch // 2) + n, at] = Gd[pl.ds(pl.multiple_of(n * 2 * rows + i * 16, 16), 16)].astype(BF16)
            return 0
        lax.fori_loop(0, 2 * rows // 16, cast, 0)
        if b + 1 < 2 * NCHIP // batch:
            for i in range(batch):
                load_c2(b + 1, i).start()

    def start_y1(j, _):
        for s in range(2):
            load_y1(order(j), s).start()
        return 0
    lax.fori_loop(0, NCHIP, start_y1, 0)
    for i in range(batch):
        load_c2(0, i).start()
    ag_w = Gather(vg_view, wg_send, wg_recv)
    for layer in range(layers):
        for cp in own_piece_copies(layer):
            cp.wait()
    ag_w.start()
    for cp in weight_copies(top, tp):
        cp.wait()
    partials(rs_f, top_fwd, True)
    ag_w.near()
    rs_f.send_direct()
    ag_w.far()
    ag_w.finish()
    pieces_out()
    cast_c2(0)
    rs_f.send_relay()
    for b in range(1, 2 * NCHIP // batch):
        cast_c2(b)
    for cp in loads:
        cp.wait()

    def layer_body(i, _):
        layer = top - i
        par = lax.rem(layer, 2)
        top_half(layer, par, layer < top, False)
        low_half(layer, par, layer < top)
        return 0
    lax.fori_loop(0, top, layer_body, 0)

    top_half(0, 0, True, True)
    outs = [gather_out(o, i) for i, o in enumerate((x1_out, x2_out, g1_out, g2_out))]

    def put(i, src):
        out = (x1_out, x2_out, g1_out, g2_out)[i]
        at = pl.ds(pl.multiple_of(me * rows, rows), rows)
        pltpu.make_async_copy(src, out.at[at], own_sem.at[i]).start()
        for n, dev in enumerate((left, right, sib)):
            remote(src, out.at[at], fg_send.at[i, n], fg_recv.at[i, n], dev).start()

    def put_done(i, src):
        out = (x1_out, x2_out, g1_out, g2_out)[i]
        at = pl.ds(pl.multiple_of(me * rows, rows), rows)
        pltpu.make_async_copy(src, out.at[at], own_sem.at[i]).wait()

    ag_d1 = gather_d(D1, 3)
    put(0, Y1.at[1])
    mlp_wgrad(0, 0, True)
    rs_b.send_relay()
    finish_cot(rs_b, C1, Y1.at[0], D1)
    ag_d1.start()
    outs[0].near()
    put(1, Y2.at[0])
    ag_d1.near()
    ag_d1.far()
    ag_d1.finish()
    partials(rs_b, lambda chip: attn_bwd(chip, 0), False)
    rs_b.send_opp()
    rs_b.send_direct()
    outs[1].near()
    put(2, C1)
    attn_wgrad(0, 0, True)
    outs[0].far()
    rs_b.send_relay()
    outs[1].far()
    finish_cot(rs_b, C2, Y2.at[0], None)
    put(3, C2)
    outs[2].near()
    outs[3].near()
    outs[2].far()
    outs[3].far()
    pieces_sent()
    for i, src in enumerate((Y1.at[1], Y2.at[0], C1, C2)):
        outs[i].finish()
        put_done(i, src)
    for i in range(4):
        grad_copy(0, i).wait()


def solution(mesh):
    act_spec = P("dp", None, None)
    weight_specs = (P(None, None, "tp", None, None), P(None, "tp", None, None), P(None, None, "tp"), P(None, "tp", None))
    grad_specs = (P("dp", None, "tp", None, None), P("dp", "tp", None, None), P("dp", None, "tp"), P("dp", "tp", None))

    groups = mesh.shape["dp"]

    def local_backward(out_y1, out_y2, cot_y1, cot_y2, w_qkv, w_out, w_up, w_down):
        seqs, rows, width = out_y1.shape
        layers, _, heads, three, head = w_qkv.shape
        hidden = w_up.shape[2]
        wq = jnp.transpose(w_qkv.reshape(layers, width, three, head), (0, 2, 1, 3))
        wo = w_out.reshape(layers, heads * head, width)
        pair = 2 * rows
        qkv_w = three * head
        piece = width * head // (128 * groups)
        act = jax.ShapeDtypeStruct((seqs * rows, width), F32)
        dma = pltpu.SemaphoreType.DMA
        outs = pl.pallas_call(
            functools.partial(kernel, groups),
            out_shape=(act, act, act, act,
                       jax.ShapeDtypeStruct((layers * width * three, head), F32),
                       jax.ShapeDtypeStruct((layers, head, width), F32),
                       jax.ShapeDtypeStruct((layers, width, hidden), F32),
                       jax.ShapeDtypeStruct((layers, hidden, width), F32),
                       jax.ShapeDtypeStruct((layers, groups, seqs, piece, 128), BF16)),
            in_specs=[pl.BlockSpec(memory_space=pl.ANY)] * 8,
            out_specs=[pl.BlockSpec(memory_space=pl.ANY)] * 9,
            scratch_shapes=[
                pltpu.VMEM((2, NCHIP, pair, width), BF16),
                pltpu.VMEM((2, NCHIP, pair, width), BF16),
                pltpu.VMEM((NCHIP, pair, width), BF16),
                pltpu.VMEM((NCHIP, pair, width), BF16),
                pltpu.VMEM((2, width, qkv_w), BF16),
                pltpu.VMEM((2, head, width), BF16),
                pltpu.VMEM((2, width, hidden), BF16),
                pltpu.VMEM((2, hidden, width), BF16),
                pltpu.VMEM((width * three, head), F32),
                pltpu.VMEM((head, width), F32),
                pltpu.VMEM((width, hidden), F32),
                pltpu.VMEM((hidden, width), F32),
                pltpu.VMEM((NCHIP, pair, hidden), F32),
                pltpu.VMEM((NCHIP, pair, hidden), BF16),
                pltpu.VMEM((NCHIP, pair, hidden), BF16),
                pltpu.VMEM((NCHIP, pair, qkv_w), BF16),
                pltpu.VMEM((NCHIP, pair, rows), F32),
                pltpu.VMEM((NCHIP, pair, head), BF16),
                pltpu.VMEM((NCHIP, pair, qkv_w), BF16),
                pltpu.VMEM((2, rows, width), F32),
                pltpu.VMEM((2, rows, width), F32),
                pltpu.VMEM((rows, width), F32),
                pltpu.VMEM((rows, width), F32),
                pltpu.VMEM((NCHIP, pair, width), F32),
                pltpu.VMEM((NCHIP, pair, width), BF16),
                pltpu.VMEM((NCHIP, rows, width), F32),
                pltpu.VMEM((NCHIP, rows, width), BF16),
                pltpu.VMEM((3, rows, width), F32),
                pltpu.VMEM((3, rows, width), BF16),
                pltpu.VMEM((seqs, layers * piece, 128), BF16),
                pltpu.VMEM((seqs, head, width), BF16),
                pltpu.VMEM((rows, seqs * head), BF16),
                pltpu.VMEM((rows, width), F32),
                dma((4, 9)), dma((4, 9)), dma((2, 10)), dma((2, 10)), dma((4, 9)), dma((4, 9)),
                dma((2, 6)), dma((4,)), dma((2, NCHIP, 2)), dma((4,)),
                dma((9,)), dma((9,)), dma((layers, groups)), dma((layers, groups)),
                dma((max(layers * max(1, piece // head), groups, width // 128),)), dma((seqs,)), dma((seqs,)),
            ],
            compiler_params=pltpu.CompilerParams(collective_id=0, has_side_effects=True,
                                                 vmem_limit_bytes=60 * 1024 * 1024),
        )(out_y1, out_y2, cot_y1, cot_y2, wq, wo, w_up, w_down)
        x1, x2, g1, g2 = (o.reshape(seqs, rows, width) for o in outs[:4])
        return (x1, x2, g1, g2, outs[4].reshape(w_qkv.shape), outs[5].reshape(w_out.shape), outs[6], outs[7])

    return jax.shard_map(local_backward, mesh=mesh, in_specs=(act_spec, act_spec, act_spec, act_spec) + weight_specs, out_specs=(act_spec, act_spec, act_spec, act_spec) + grad_specs, check_vma=False)
```

```python
import functools
import math
import jax
import jax.numpy as jnp
from jax import lax
from jax.experimental import pallas as pl
from jax.experimental.pallas import tpu as pltpu
from jax.sharding import PartitionSpec as P

NORM_EPS = 1e-6
F32, BF16 = jnp.float32, jnp.bfloat16
GELU_C = math.sqrt(2.0 / math.pi)
GELU_A = 0.044715
NCHIP = 4


def mm(a, b):
    return lax.dot_general(a, b, (((1,), (0,)), ((), ())), preferred_element_type=F32)


def mm_t(a, b):
    return lax.dot_general(a, b, (((1,), (1,)), ((), ())), preferred_element_type=F32)


def tmm(a, b):
    return lax.dot_general(a, b, (((0,), (0,)), ((), ())), preferred_element_type=F32)


def kernel(groups, y1_hbm, y2_hbm, c1_hbm, c2_hbm, wqkv_hbm, wo_hbm, wu_hbm, wd_hbm,
           x1_out, x2_out, g1_out, g2_out, gqkv_out, gout_out, gup_out, gdown_out, wof_hbm,
           N1, N2, D1, D2, Wqkv, Wo, Wu, Wd, SQ, SO, SU, SD, H, ACT, GH, QKV, PROB, OG, GQ,
           Y1, Y2, C1, C2, PF, PB, XF, XB, RF, RB, VG, WoV,
           ag_send, ag_recv, rs_send, rs_recv, fg_send, fg_recv, w_sem, g_sem, io_sem, own_sem,
           wg_send, wg_recv, wx_send, wx_recv, wl_sem):
    layers = wqkv_hbm.shape[0]
    rows = y1_hbm.shape[1]
    half = rows // 2
    width = y1_hbm.shape[2]
    head = wo_hbm.shape[1]
    scale = 1.0 / math.sqrt(head)
    ndev = 2 * NCHIP
    me = lax.axis_index("tp")
    c = me // 2
    k = lax.rem(me, 2)
    sib = me + 1 - 2 * k
    left = lax.rem(me + ndev - 2, ndev)
    right = lax.rem(me + 2, ndev)
    cl = lax.rem(c + NCHIP - 1, NCHIP)
    cr = lax.rem(c + 1, NCHIP)
    co = lax.rem(c + 2, NCHIP)
    mine = pl.ds(pl.multiple_of(k * rows, rows), rows)
    other = pl.ds(pl.multiple_of((1 - k) * rows, rows), rows)

    def my_half(h):
        return pl.ds(pl.multiple_of(k * rows + h * half, half), half)

    def order(j):
        off = (2 + j) * (1 - j // 2) + (3 - j) * (j // 2)
        return lax.rem(c + off, NCHIP)

    def remote(src, dst, ssem, rsem, dev):
        return pltpu.make_async_remote_copy(src_ref=src, dst_ref=dst, send_sem=ssem, recv_sem=rsem,
                                            device_id={"tp": dev}, device_id_type=pl.DeviceIdType.MESH)

    grp = lax.axis_index("dp")
    barrier = pltpu.get_barrier_semaphore()

    def hello(axis, at, n):
        def one(i, _):
            pl.semaphore_signal(barrier, inc=1, device_id={axis: lax.rem(at + i, n)},
                                device_id_type=pl.DeviceIdType.MESH)
            return 0
        lax.fori_loop(1, n, one, 0)
    hello("tp", me, ndev)
    hello("dp", grp, groups)
    pl.semaphore_wait(barrier, ndev - 1 + groups - 1)

    class Gather:
        def __init__(self, view, ssem, rsem, own=None):
            src = (lambda h: view(c, k, h)) if own is None else own
            moves = [(src(h), view(c, k, h), dev) for h in (0, 1) for dev in (left, right, sib)]
            moves += [(view(chip, k, h), view(chip, k, h), dev) for chip, h, dev in (
                (cr, 0, left), (cl, 1, right), (cr, 0, sib), (cl, 0, sib), (cr, 1, sib), (cl, 1, sib),
                (co, 0, sib), (co, 1, sib))]
            self.send = [remote(a, b, ssem.at[i], rsem.at[i], dev) for i, (a, b, dev) in enumerate(moves)]
            o = 1 - k
            land = [(cr, k, 0), (cl, k, 0), (c, o, 0), (cr, k, 1), (cl, k, 1), (c, o, 1), (co, k, 0), (co, k, 1),
                    (cr, o, 0), (cl, o, 0), (cr, o, 1), (cl, o, 1), (co, o, 0), (co, o, 1)]
            self.recv = [remote(view(*at), view(*at), ssem.at[i], rsem.at[i], sib) for i, at in enumerate(land)]

        def pass_on(self, got, *sends):
            self.recv[got].wait_recv()
            for i in sends:
                self.send[i].start()

        def start_half(self, h):
            for i in range(3 * h, 3 * h + 3):
                self.send[i].start()

        def start(self):
            self.start_half(0)
            self.start_half(1)

        def near0(self):
            self.pass_on(0, 6, 8)
            self.pass_on(1, 9)

        def near1(self):
            self.pass_on(4, 7, 11)
            self.pass_on(3, 10)

        def near(self):
            self.near0()
            self.near1()

        def far(self):
            self.pass_on(6, 12)
            self.pass_on(7, 13)

        def finish(self):
            for i in (2, 5, 8, 9, 10, 11, 12, 13):
                self.recv[i].wait_recv()
            for cp in self.send:
                cp.wait_send()

    class Scatter:
        def __init__(self, part, from_sib, rec, ssem, rsem):
            self.part, self.from_sib = part, from_sib
            self.rel, self.dir, self.fin = rec.at[0], rec.at[1], rec.at[2]
            self.ssem, self.rsem = ssem, rsem

            def hp(chip, h):
                return part.at[chip, my_half(h)]

            def hr(buf, h):
                return buf.at[pl.ds(h * half, half)]

            def mk(i, src, dst, dev):
                return remote(src, dst, ssem.at[i], rsem.at[i], dev)

            self.opp = [mk(4, hp(co, 0), hr(self.rel, 0), left), mk(5, hp(co, 1), hr(self.rel, 1), right)]
            self.direct = [mk(6, hp(cl, 1), hr(self.dir, 1), left), mk(7, hp(cr, 0), hr(self.dir, 0), right)]
            self.relay = [mk(8, hp(cl, 0), hr(self.fin, 0), left), mk(9, hp(cr, 1), hr(self.fin, 1), right)]

        def pair(self, chip):
            return remote(self.part.at[chip, other], self.from_sib.at[chip], self.ssem.at[chip],
                          self.rsem.at[chip], sib)

        def add(self, chip):
            self.pair_recv(chip)
            got = self.part[chip, mine].astype(F32) + self.from_sib[chip].astype(F32)
            self.part[chip, mine] = got.astype(self.part.dtype)

        def pair_recv(self, chip):
            remote(self.from_sib.at[chip], self.from_sib.at[chip], self.ssem.at[chip], self.rsem.at[chip],
                   sib).wait_recv()

        def send_opp(self):
            self.add(co)
            for cp in self.opp:
                cp.start()

        def send_direct(self):
            self.add(cl)
            self.direct[0].start()
            self.add(cr)
            self.direct[1].start()

        def send_relay(self):
            for h, (chip, cp) in enumerate(((cl, self.relay[0]), (cr, self.relay[1]))):
                self.opp[h].wait_recv()
                got = self.part[chip, my_half(h)].astype(F32) + self.rel[h * half:(h + 1) * half].astype(F32)
                self.part[chip, my_half(h)] = got.astype(self.part.dtype)
                cp.start()

        def land(self):
            self.pair_recv(c)
            for cp in self.direct + self.relay:
                cp.wait_recv()

        def total(self, r):
            at = pl.ds(pl.multiple_of(k * rows + r * 16, 16), 16)
            loc = pl.ds(pl.multiple_of(r * 16, 16), 16)
            return (self.part[c, at].astype(F32) + self.from_sib[c, loc].astype(F32)
                    + self.fin[loc].astype(F32) + self.dir[loc].astype(F32))

        def drain(self):
            for chip in range(NCHIP):
                self.pair(chip).wait_send()
            for cp in self.opp + self.direct + self.relay:
                cp.wait_send()

    rs_f = Scatter(PF, XF, RF, rs_send.at[0], rs_recv.at[0])
    rs_b = Scatter(PB, XB, RB, rs_send.at[1], rs_recv.at[1])

    def span(core, h):
        return pl.ds(pl.multiple_of(core * rows + h * half, half), half)

    def gather_rows(buf, i):
        return Gather(lambda chip, core, h: buf.at[chip, span(core, h)], ag_send.at[i], ag_recv.at[i])

    def heads_of(chip, core):
        return pl.ds(pl.multiple_of((2 * chip + core) * head, head), head)

    def gather_o():
        n = NCHIP // 2
        return Gather(lambda chip, core, h: OG.at[pl.ds(h * n, n), :, heads_of(chip, core)],
                      ag_send.at[3], ag_recv.at[3])

    def gather_out(out, i, src):
        def view(chip, core, h):
            return out.at[pl.ds(pl.multiple_of((2 * chip + core) * rows + h * half, half), half)]
        return Gather(view, fg_send.at[i], fg_recv.at[i], lambda h: src.at[pl.ds(h * half, half)])

    def keep_out(out, i, src):
        return pltpu.make_async_copy(src, out.at[pl.ds(pl.multiple_of(me * rows, rows), rows)], own_sem.at[i])

    lanes = 128
    piece = width * head // (lanes * groups)

    def own_piece_copies(layer):
        if piece >= head:
            n = piece // head
            return [pltpu.make_async_copy(
                wo_hbm.at[layer, :, pl.ds(pl.multiple_of((grp * n + b) * lanes, lanes), lanes)],
                VG.at[me, pl.ds(layer * piece + b * head, head)], wl_sem.at[layer * n + b]) for b in range(n)]
        n = head // piece
        return [pltpu.make_async_copy(
            wo_hbm.at[layer, pl.ds(pl.multiple_of(lax.rem(grp, n) * piece, piece), piece),
                      pl.ds(pl.multiple_of((grp // n) * lanes, lanes), lanes)],
            VG.at[me, pl.ds(layer * piece, piece)], wl_sem.at[layer])]

    def vg_view(chip, core, h):
        n = layers * piece // 2
        return VG.at[2 * chip + core, pl.ds(h * n, n)]

    def piece_send(layer, d):
        return pltpu.make_async_remote_copy(
            src_ref=VG.at[:, pl.ds(layer * piece, piece)], dst_ref=wof_hbm.at[layer, grp],
            send_sem=wx_send.at[layer, d], recv_sem=wx_recv.at[layer, d],
            device_id={"dp": lax.rem(grp + d, groups), "tp": me}, device_id_type=pl.DeviceIdType.MESH)

    def piece_keep(layer):
        return pltpu.make_async_copy(VG.at[:, pl.ds(layer * piece, piece)], wof_hbm.at[layer, grp],
                                     wx_send.at[layer, 0])

    def pieces_out():
        for layer in reversed(range(layers)):
            piece_keep(layer).start()

            def one(d, _):
                piece_send(layer, d).start()
                return 0
            lax.fori_loop(1, groups, one, 0)

    def pieces_sent():
        for layer in range(layers):
            def one(d, _):
                piece_send(layer, d).wait_send()
                return 0
            lax.fori_loop(1, groups, one, 0)

    def pieces_in(layer):
        def one(d, _):
            pltpu.make_async_remote_copy(
                src_ref=wof_hbm.at[layer, grp], dst_ref=wof_hbm.at[layer, lax.rem(grp + groups - d, groups)],
                send_sem=wx_send.at[layer, d], recv_sem=wx_recv.at[layer, d],
                device_id={"dp": grp, "tp": me}, device_id_type=pl.DeviceIdType.MESH).wait_recv()
            return 0
        piece_keep(layer).wait()
        lax.fori_loop(1, groups, one, 0)

    def wov_copies(layer):
        if piece >= head:
            n = piece // head
            return [pltpu.make_async_copy(wof_hbm.at[layer, g, :, pl.ds(b * head, head)],
                                          WoV.at[:, :, pl.ds((g * n + b) * lanes, lanes)], wl_sem.at[g * n + b])
                    for g in range(groups) for b in range(n)]
        n = head // piece
        return [pltpu.make_async_copy(wof_hbm.at[layer, g],
                                      WoV.at[:, pl.ds((g % n) * piece, piece), pl.ds((g // n) * lanes, lanes)],
                                      wl_sem.at[g]) for g in range(groups)]

    def weight_copies(layer, slot):
        pairs = [(src.at[layer], dst.at[slot]) for src, dst in ((wo_hbm, Wo), (wu_hbm, Wu), (wd_hbm, Wd))]
        pairs += [(wqkv_hbm.at[layer, j], Wqkv.at[slot, :, pl.ds(j * head, head)]) for j in range(3)]
        return [pltpu.make_async_copy(src, dst, w_sem.at[slot, i]) for i, (src, dst) in enumerate(pairs)]

    tile = width // 4

    def grad_copy(layer, i, t):
        at = pl.ds(pl.multiple_of(t * tile, tile), tile)
        if i == 0:
            size = 3 * width
            dst = gqkv_out.at[pl.ds(pl.multiple_of(layer * size + t * 3 * tile, 3 * tile), 3 * tile)]
        else:
            dst = (gout_out.at[layer, :, at], gup_out.at[layer, at], gdown_out.at[layer, :, at])[i - 1]
        return pltpu.make_async_copy((SQ, SO, SU, SD)[i].at[lax.rem(t, 2)], dst, g_sem.at[i, lax.rem(t, 2)])

    def wgrad_tiles(layer, i, fill):
        def body(t, _):
            pl.when(t >= 2)(lambda: grad_copy(layer, i, t - 2).wait())
            fill(t, lax.rem(t, 2), pl.ds(pl.multiple_of(t * tile, tile), tile))
            grad_copy(layer, i, t).start()
            return 0
        lax.fori_loop(0, 4, body, 0)

    def wgrad_wait(layer, i):
        for t in (2, 3):
            grad_copy(layer, i, t).wait()

    def mlp_fwd(chip, par):
        hid = mm(N1[par, chip], Wu[par])
        H[chip] = hid
        act = hid * (0.5 * (1.0 + jnp.tanh(GELU_C * (hid + GELU_A * (hid * hid * hid)))))
        act = act.astype(BF16)
        ACT[par, chip] = act
        PF[chip] = mm(act, Wd[par])

    def mlp_bwd(chip, par):
        grad_act = mm_t(D2[chip], Wd[par])
        hid = H[chip]
        sq = hid * hid
        t = jnp.tanh(GELU_C * (hid + GELU_A * (sq * hid)))
        slope = 0.5 * (1.0 + t) + (0.5 * hid) * ((1.0 - t * t) * (GELU_C * (1.0 + (3.0 * GELU_A) * sq)))
        grad_hid = (grad_act * slope).astype(BF16)
        GH[chip] = grad_hid
        PB[chip] = mm_t(grad_hid, Wu[par]).astype(BF16)

    def attn_fwd(chip, par):
        QKV[chip] = mm(N2[par, chip], Wqkv[par]).astype(BF16)
        for s in range(2):
            at = slice(s * rows, (s + 1) * rows)
            q = QKV[chip, at, 0:head]
            kk = QKV[chip, at, head:2 * head]
            v = QKV[chip, at, 2 * head:3 * head]
            sc = mm_t(q, kk) * scale
            e = jnp.exp(sc - jnp.max(sc, axis=-1, keepdims=True))
            prob = e / jnp.sum(e, axis=-1, keepdims=True)
            PROB[chip, at] = prob
            OG[chip, at, heads_of(c, k)] = mm(prob.astype(BF16), v).astype(BF16)

    def attn_bwd(chip, par):
        grad_o2 = mm_t(D1[chip], Wo[par]).astype(BF16)
        for s in range(2):
            at = slice(s * rows, (s + 1) * rows)
            grad_o = grad_o2[at]
            q = QKV[chip, at, 0:head]
            kk = QKV[chip, at, head:2 * head]
            v = QKV[chip, at, 2 * head:3 * head]
            prob = PROB[chip, at]
            grad_p = mm_t(grad_o, v)
            grad_s = (prob * (grad_p - jnp.sum(grad_p * prob, axis=-1, keepdims=True)) * scale).astype(BF16)
            GQ[chip, at, 0:head] = mm(grad_s, kk).astype(BF16)
            GQ[chip, at, head:2 * head] = tmm(grad_s, q).astype(BF16)
            GQ[chip, at, 2 * head:3 * head] = tmm(prob.astype(BF16), grad_o).astype(BF16)
        PB[chip] = mm_t(GQ[chip], Wqkv[par]).astype(BF16)

    def flat(x):
        return x.reshape((x.shape[0] * x.shape[1],) + x.shape[2:])

    def mlp_wgrad(layer, par):
        def up(t, slot, at):
            SU[slot] = tmm(flat(N1[par, :, :, at]), flat(GH[...]))

        def down(t, slot, at):
            SD[slot] = tmm(flat(ACT[par]), flat(D2[:, :, at]))
        wgrad_tiles(layer, 2, up)
        wgrad_tiles(layer, 3, down)
        wgrad_wait(layer, 2)
        wgrad_wait(layer, 3)

    def attn_wgrad(layer, par):
        def qkv(t, slot, at):
            res = tmm(flat(N2[par, :, :, at]), flat(GQ[...]))
            for j in range(3):
                SQ[slot, pl.ds(j, tile, stride=3), :] = res[:, j * head:(j + 1) * head]

        def out(t, slot, at):
            SO[slot] = tmm(flat(OG[:, :, heads_of(c, k)]), flat(D1[:, :, at]))
        wgrad_tiles(layer, 0, qkv)
        wgrad_tiles(layer, 1, out)
        wgrad_wait(layer, 0)
        wgrad_wait(layer, 1)

    def own_rows(step):
        def body(r, _):
            step(r, pl.ds(pl.multiple_of(r * 16, 16), 16), pl.ds(pl.multiple_of(k * rows + r * 16, 16), 16))
            return 0
        lax.fori_loop(0, rows // 16, body, 0)

    def inv_rms(x):
        return lax.rsqrt(jnp.mean(x * x, axis=-1, keepdims=True) + NORM_EPS)

    def finish_state(rs, old, new, norm_to):
        rs.land()

        def step(r, loc, at):
            x = old[loc] - rs.total(r)
            new[loc] = x
            if norm_to is not None:
                norm_to[c, at] = (x * inv_rms(x)).astype(BF16)
        own_rows(step)
        rs.drain()

    def finish_cot(rs, cot, x_ref, cast_to):
        rs.land()

        def step(r, loc, at):
            x = x_ref[loc]
            inv = inv_rms(x)
            normed = x * inv
            grad_n = rs.total(r)
            new = cot[loc] + inv * (grad_n - normed * jnp.mean(normed * grad_n, axis=-1, keepdims=True))
            cot[loc] = new
            if cast_to is not None:
                cast_to[c, at] = new.astype(BF16)
        own_rows(step)
        rs.drain()

    def finish_sum(rs, to):
        rs.land()

        def step(r, loc, at):
            to[c, at] = rs.total(r).astype(BF16)
        own_rows(step)
        rs.drain()

    def chip_rows(step):
        def body(i, _):
            step(pl.ds(pl.multiple_of(i * 16, 16), 16))
            return 0
        lax.fori_loop(0, 2 * rows // 16, body, 0)

    def attn_apply(chip, par):
        q = 1 - par
        PF[chip] = mm(OG[chip], flat(WoV[...]))

        def step(at):
            x = Y1[par, chip, at] - PF[chip, at]
            Y1[q, chip, at] = x
            N1[q, chip, at] = (x * inv_rms(x)).astype(BF16)
        chip_rows(step)

    def cot_apply(chip, par):
        def step(at):
            x = Y1[par, chip, at]
            inv = inv_rms(x)
            normed = x * inv
            grad_n = D1[chip, at].astype(F32)
            new = C1[chip, at] + inv * (grad_n - normed * jnp.mean(normed * grad_n, axis=-1, keepdims=True))
            C1[chip, at] = new
            D1[chip, at] = new.astype(BF16)
        chip_rows(step)

    def when(cond, fn):
        if cond is True:
            fn()
        elif cond is not False:
            pl.when(cond)(fn)

    def partials(rs, compute, extra=()):
        def body(j, _):
            chip = order(j)
            compute(chip)
            rs.pair(chip).start()
            for at, fn in extra:
                pl.when(j == at)(fn)
            return 0
        lax.fori_loop(0, NCHIP, body, 0)

    def top_half(layer, par, not_first, last):
        q = 1 - par
        ag_d = gather_rows(D2, 1)
        ag_o = gather_o()
        if last:
            ag_n = gather_out(x2_out, 0, Y2.at[par])
            finish_state(rs_f, Y2.at[q], Y2.at[par], None)
            ag_n.start()
            keep_out(x2_out, 0, Y2.at[par]).start()
        else:
            ag_n = gather_rows(N2.at[par], 0)
            finish_state(rs_f, Y2.at[q], Y2.at[par], N2.at[par])
            ag_n.start()
            for cp in weight_copies(layer - 1, q):
                cp.start()
        when(not_first, rs_b.send_relay)
        ag_n.near()

        def d_start():
            attn_wgrad(layer + 1, q)
            finish_cot(rs_b, C2, Y2.at[q], D2)
            ag_d.start()
        when(not_first, d_start)
        ag_n.far()
        ag_n.finish()
        if last:
            keep_out(x2_out, 0, Y2.at[par]).wait()
            loads = [pltpu.make_async_copy(x2_out.at[pl.ds(chip * 2 * rows, 2 * rows)], PF.at[chip],
                                           io_sem.at[0, chip, 0]) for chip in range(NCHIP)]
            for cp in loads:
                cp.start()
            for chip in range(NCHIP):
                loads[chip].wait()

                def step(at):
                    x = PF[chip, at]
                    N2[par, chip, at] = (x * inv_rms(x)).astype(BF16)
                chip_rows(step)
        pieces_in(layer)
        for cp in wov_copies(layer):
            cp.start()

        def fwd(chip, _):
            attn_fwd(chip, par)

            @pl.when(chip == NCHIP // 2 - 1)
            def _():
                ag_o.start_half(0)
                when(not_first, ag_d.near)
            return 0
        lax.fori_loop(0, NCHIP, fwd, 0)
        ag_o.start_half(1)
        ag_o.near0()

        def d_end():
            ag_d.far()
            ag_d.finish()
        when(not_first, d_end)
        partials(rs_b, lambda chip: mlp_bwd(chip, par), ((0, ag_o.near1), (1, rs_b.send_opp)))
        rs_b.send_direct()
        for cp in wov_copies(layer):
            cp.wait()
        ag_o.far()
        ag_o.finish()

    def low_half(layer, par):
        q = 1 - par
        ag_d = gather_rows(D1, 2)
        for cp in weight_copies(layer - 1, q):
            cp.wait()

        def fwd(chip):
            attn_apply(chip, par)
            mlp_fwd(chip, q)
        partials(rs_f, fwd, ((0, rs_b.send_relay), (1, rs_f.send_opp)))
        finish_sum(rs_b, D1)
        ag_d.start()
        rs_f.send_direct()
        mlp_wgrad(layer, par)
        ag_d.near()
        rs_f.send_relay()
        ag_d.far()
        ag_d.finish()
        attn_back(par)

    def attn_back(par):
        def bwd(chip):
            cot_apply(chip, par)
            attn_bwd(chip, par)
        partials(rs_b, bwd, ((1, rs_b.send_opp),))
        rs_b.send_direct()

    top = layers - 1
    tp = top % 2
    for layer in range(layers):
        for cp in own_piece_copies(layer):
            cp.start()
    for cp in weight_copies(top, tp):
        cp.start()
    loads = [pltpu.make_async_copy(src.at[me], dst, own_sem.at[i]) for i, (src, dst) in enumerate(
        ((y2_hbm, Y2.at[1 - tp]), (c2_hbm, C2)))]
    for cp in loads:
        cp.start()

    def load_rows(src, dst, i, chip, s):
        return pltpu.make_async_copy(src.at[2 * chip + s], dst.at[chip, pl.ds(s * rows, rows)], io_sem.at[i, chip, s])

    def each_pair(fn):
        def body(j, _):
            for s in range(2):
                fn(order(j), s)
            return 0
        lax.fori_loop(0, NCHIP, body, 0)

    def top_fwd(chip):
        for s in range(2):
            load_rows(y1_hbm, Y1.at[tp], 0, chip, s).wait()

        def step(at):
            x = Y1[tp, chip, at]
            N1[tp, chip, at] = (x * inv_rms(x)).astype(BF16)
        chip_rows(step)
        mlp_fwd(chip, tp)

    def cast_c2():
        each_pair(lambda chip, s: load_rows(c2_hbm, C1, 1, chip, s).wait())

        def body(chip, _):
            def step(at):
                D2[chip, at] = C1[chip, at].astype(BF16)
            chip_rows(step)
            return 0
        lax.fori_loop(0, NCHIP, body, 0)
        each_pair(lambda chip, s: load_rows(c1_hbm, C1, 1, chip, s).start())

    each_pair(lambda chip, s: load_rows(y1_hbm, Y1.at[tp], 0, chip, s).start())
    each_pair(lambda chip, s: load_rows(c2_hbm, C1, 1, chip, s).start())
    ag_w = Gather(vg_view, wg_send, wg_recv)
    for layer in range(layers):
        for cp in own_piece_copies(layer):
            cp.wait()
    ag_w.start()
    for cp in weight_copies(top, tp):
        cp.wait()
    partials(rs_f, top_fwd, ((1, rs_f.send_opp),))
    ag_w.near()
    rs_f.send_direct()
    ag_w.far()
    ag_w.finish()
    pieces_out()
    rs_f.send_relay()
    cast_c2()
    for cp in loads:
        cp.wait()
    each_pair(lambda chip, s: load_rows(c1_hbm, C1, 1, chip, s).wait())

    def layer_body(i, _):
        layer = top - i
        par = lax.rem(layer, 2)
        top_half(layer, par, layer < top, False)
        low_half(layer, par)
        return 0
    lax.fori_loop(0, top, layer_body, 0)

    top_half(0, 0, True, True)
    def put_x1(chip):
        return pltpu.make_async_copy(Y1.at[1, chip], x1_out.at[pl.ds(pl.multiple_of(chip * 2 * rows, rows), 2 * rows)],
                                     io_sem.at[0, chip, 0])

    def put_g1(chip):
        return pltpu.make_async_copy(C1.at[chip], g1_out.at[pl.ds(pl.multiple_of(chip * 2 * rows, rows), 2 * rows)],
                                     io_sem.at[0, chip, 1])

    def x1_rows(chip, _):
        attn_apply(chip, 0)
        put_x1(chip).start()
        return 0

    def each_chip(fn):
        def body(chip, _):
            fn(chip)
            return 0
        lax.fori_loop(0, NCHIP, body, 0)

    ag_d1 = gather_rows(D1, 2)
    rs_b.send_relay()
    finish_sum(rs_b, D1)
    ag_d1.start()
    lax.fori_loop(0, NCHIP, x1_rows, 0)
    ag_d1.near()
    mlp_wgrad(0, 0)
    ag_d1.far()
    ag_d1.finish()
    attn_back(0)
    each_chip(lambda chip: put_g1(chip).start())
    rs_b.send_relay()
    attn_wgrad(0, 0)
    finish_cot(rs_b, C2, Y2.at[0], None)
    last = gather_out(g2_out, 1, C2)
    last.start()
    keep_out(g2_out, 1, C2).start()
    last.near()
    last.far()
    each_chip(lambda chip: put_x1(chip).wait())
    each_chip(lambda chip: put_g1(chip).wait())
    pieces_sent()
    keep_out(g2_out, 1, C2).wait()
    last.finish()


def solution(mesh):
    act_spec = P("dp", None, None)
    weight_specs = (P(None, None, "tp", None, None), P(None, "tp", None, None), P(None, None, "tp"), P(None, "tp", None))
    grad_specs = (P("dp", None, "tp", None, None), P("dp", "tp", None, None), P("dp", None, "tp"), P("dp", "tp", None))

    groups = mesh.shape["dp"]

    def local_backward(out_y1, out_y2, cot_y1, cot_y2, w_qkv, w_out, w_up, w_down):
        seqs, rows, width = out_y1.shape
        layers, _, heads, three, head = w_qkv.shape
        hidden = w_up.shape[2]
        wq = jnp.transpose(w_qkv.reshape(layers, width, three, head), (0, 2, 1, 3))
        wo = w_out.reshape(layers, heads * head, width)
        pair = 2 * rows
        qkv_w = three * head
        piece = width * head // (128 * groups)
        act = jax.ShapeDtypeStruct((seqs * rows, width), F32)
        dma = pltpu.SemaphoreType.DMA
        outs = pl.pallas_call(
            functools.partial(kernel, groups),
            out_shape=(act, act, act, act,
                       jax.ShapeDtypeStruct((layers * width * three, head), F32),
                       jax.ShapeDtypeStruct((layers, head, width), F32),
                       jax.ShapeDtypeStruct((layers, width, hidden), F32),
                       jax.ShapeDtypeStruct((layers, hidden, width), F32),
                       jax.ShapeDtypeStruct((layers, groups, seqs, piece, 128), BF16)),
            in_specs=[pl.BlockSpec(memory_space=pl.ANY)] * 8,
            out_specs=[pl.BlockSpec(memory_space=pl.ANY)] * 9,
            scratch_shapes=[
                pltpu.VMEM((2, NCHIP, pair, width), BF16),
                pltpu.VMEM((2, NCHIP, pair, width), BF16),
                pltpu.VMEM((NCHIP, pair, width), BF16),
                pltpu.VMEM((NCHIP, pair, width), BF16),
                pltpu.VMEM((2, width, qkv_w), BF16),
                pltpu.VMEM((2, head, width), BF16),
                pltpu.VMEM((2, width, hidden), BF16),
                pltpu.VMEM((2, hidden, width), BF16),
                pltpu.VMEM((2, width // 4 * three, head), F32),
                pltpu.VMEM((2, head, width // 4), F32),
                pltpu.VMEM((2, width // 4, hidden), F32),
                pltpu.VMEM((2, hidden, width // 4), F32),
                pltpu.VMEM((NCHIP, pair, hidden), F32),
                pltpu.VMEM((2, NCHIP, pair, hidden), BF16),
                pltpu.VMEM((NCHIP, pair, hidden), BF16),
                pltpu.VMEM((NCHIP, pair, qkv_w), BF16),
                pltpu.VMEM((NCHIP, pair, rows), F32),
                pltpu.VMEM((NCHIP, pair, seqs * head), BF16),
                pltpu.VMEM((NCHIP, pair, qkv_w), BF16),
                pltpu.VMEM((2, NCHIP, pair, width), F32),
                pltpu.VMEM((2, rows, width), F32),
                pltpu.VMEM((NCHIP, pair, width), F32),
                pltpu.VMEM((rows, width), F32),
                pltpu.VMEM((NCHIP, pair, width), F32),
                pltpu.VMEM((NCHIP, pair, width), BF16),
                pltpu.VMEM((NCHIP, rows, width), F32),
                pltpu.VMEM((NCHIP, rows, width), BF16),
                pltpu.VMEM((3, rows, width), F32),
                pltpu.VMEM((3, rows, width), BF16),
                pltpu.VMEM((seqs, layers * piece, 128), BF16),
                pltpu.VMEM((seqs, head, width), BF16),
                dma((4, 14)), dma((4, 14)), dma((2, 10)), dma((2, 10)), dma((2, 14)), dma((2, 14)),
                dma((2, 6)), dma((4, 2)), dma((2, NCHIP, 2)), dma((2,)),
                dma((14,)), dma((14,)), dma((layers, groups)), dma((layers, groups)),
                dma((max(layers * max(1, piece // head), groups, width // 128),)),
            ],
            compiler_params=pltpu.CompilerParams(collective_id=0, has_side_effects=True,
                                                 vmem_limit_bytes=67043328),
        )(out_y1, out_y2, cot_y1, cot_y2, wq, wo, w_up, w_down)
        x1, x2, g1, g2 = (o.reshape(seqs, rows, width) for o in outs[:4])
        return (x1, x2, g1, g2, outs[4].reshape(w_qkv.shape), outs[5].reshape(w_out.shape), outs[6], outs[7])

    return jax.shard_map(local_backward, mesh=mesh, in_specs=(act_spec, act_spec, act_spec, act_spec) + weight_specs, out_specs=(act_spec, act_spec, act_spec, act_spec) + grad_specs, check_vma=False)
```

```python
import functools
import math
import jax
import jax.numpy as jnp
from jax import lax
from jax.experimental import pallas as pl
from jax.experimental.pallas import tpu as pltpu
from jax.sharding import PartitionSpec as P

NORM_EPS = 1e-6
F32, BF16 = jnp.float32, jnp.bfloat16
GELU_C = math.sqrt(2.0 / math.pi)
GELU_A = 0.044715
CHUNK = 64
NCHIP = 4


def mm(a, b):
    return lax.dot_general(a, b, (((1,), (0,)), ((), ())), preferred_element_type=F32)


def mm_t(a, b):
    return lax.dot_general(a, b, (((1,), (1,)), ((), ())), preferred_element_type=F32)


def tmm(a, b):
    return lax.dot_general(a, b, (((0,), (0,)), ((), ())), preferred_element_type=F32)


def kernel(groups, y1_hbm, y2_hbm, c1_hbm, c2_hbm, wqkv_hbm, wo_hbm, wu_hbm, wd_hbm,
           x1_out, x2_out, g1_out, g2_out, gqkv_out, gout_out, gup_out, gdown_out, wof_hbm,
           N1, N2, D1, D2, Wqkv, Wo, Wu, Wd, SQ, SO, SU, SD, H, ACT, GH, QKV, PROB, OG, GQ,
           Y1, Y2, C1, C2, PF, PB, XF, XB, RF, RB, VG, WoV,
           ag_send, ag_recv, rs_send, rs_recv, fg_send, fg_recv, w_sem, g_sem, io_sem, own_sem,
           wg_send, wg_recv, wx_send, wx_recv, wl_sem):
    layers = wqkv_hbm.shape[0]
    rows = y1_hbm.shape[1]
    half = rows // 2
    width = y1_hbm.shape[2]
    head = wo_hbm.shape[1]
    scale = 1.0 / math.sqrt(head)
    ndev = 2 * NCHIP
    me = lax.axis_index("tp")
    c = me // 2
    k = lax.rem(me, 2)
    sib = me + 1 - 2 * k
    left = lax.rem(me + ndev - 2, ndev)
    right = lax.rem(me + 2, ndev)
    cl = lax.rem(c + NCHIP - 1, NCHIP)
    cr = lax.rem(c + 1, NCHIP)
    co = lax.rem(c + 2, NCHIP)
    mine = pl.ds(pl.multiple_of(k * rows, rows), rows)
    other = pl.ds(pl.multiple_of((1 - k) * rows, rows), rows)

    def my_half(h):
        return pl.ds(pl.multiple_of(k * rows + h * half, half), half)

    def order(j):
        off = (2 + j) * (1 - j // 2) + (3 - j) * (j // 2)
        return lax.rem(c + off, NCHIP)

    def remote(src, dst, ssem, rsem, dev):
        return pltpu.make_async_remote_copy(src_ref=src, dst_ref=dst, send_sem=ssem, recv_sem=rsem,
                                            device_id={"tp": dev}, device_id_type=pl.DeviceIdType.MESH)

    grp = lax.axis_index("dp")
    barrier = pltpu.get_barrier_semaphore()

    def hello(axis, at, n):
        def one(i, _):
            pl.semaphore_signal(barrier, inc=1, device_id={axis: lax.rem(at + i, n)},
                                device_id_type=pl.DeviceIdType.MESH)
            return 0
        lax.fori_loop(1, n, one, 0)
    hello("tp", me, ndev)
    hello("dp", grp, groups)
    pl.semaphore_wait(barrier, ndev - 1 + groups - 1)

    class Gather:
        def __init__(self, view, ssem, rsem, own=None):
            src = (lambda h: view(c, k, h)) if own is None else own
            moves = [(src(h), view(c, k, h), dev) for h in (0, 1) for dev in (left, right, sib)]
            moves += [(view(chip, k, h), view(chip, k, h), dev) for chip, h, dev in (
                (cr, 0, left), (cl, 1, right), (cr, 0, sib), (cl, 0, sib), (cr, 1, sib), (cl, 1, sib),
                (co, 0, sib), (co, 1, sib))]
            self.send = [remote(a, b, ssem.at[i], rsem.at[i], dev) for i, (a, b, dev) in enumerate(moves)]
            o = 1 - k
            land = [(cr, k, 0), (cl, k, 0), (c, o, 0), (cr, k, 1), (cl, k, 1), (c, o, 1), (co, k, 0), (co, k, 1),
                    (cr, o, 0), (cl, o, 0), (cr, o, 1), (cl, o, 1), (co, o, 0), (co, o, 1)]
            self.recv = [remote(view(*at), view(*at), ssem.at[i], rsem.at[i], sib) for i, at in enumerate(land)]

        def pass_on(self, got, *sends):
            self.recv[got].wait_recv()
            for i in sends:
                self.send[i].start()

        def start_half(self, h):
            for i in range(3 * h, 3 * h + 3):
                self.send[i].start()

        def start(self):
            self.start_half(0)
            self.start_half(1)

        def near0(self):
            self.pass_on(0, 6, 8)
            self.pass_on(1, 9)

        def near1(self):
            self.pass_on(4, 7, 11)
            self.pass_on(3, 10)

        def near(self):
            self.near0()
            self.near1()

        def far(self):
            self.pass_on(6, 12)
            self.pass_on(7, 13)

        def finish(self):
            for i in (2, 5, 8, 9, 10, 11, 12, 13):
                self.recv[i].wait_recv()
            for cp in self.send:
                cp.wait_send()

    class Scatter:
        def __init__(self, part, from_sib, rec, ssem, rsem):
            self.part, self.from_sib = part, from_sib
            self.rel, self.dir, self.fin = rec.at[0], rec.at[1], rec.at[2]
            self.ssem, self.rsem = ssem, rsem

            def hp(chip, h):
                return part.at[chip, my_half(h)]

            def hr(buf, h):
                return buf.at[pl.ds(h * half, half)]

            def mk(i, src, dst, dev):
                return remote(src, dst, ssem.at[i], rsem.at[i], dev)

            self.opp = [mk(4, hp(co, 0), hr(self.rel, 0), left), mk(5, hp(co, 1), hr(self.rel, 1), right)]
            self.direct = [mk(6, hp(cl, 1), hr(self.dir, 1), left), mk(7, hp(cr, 0), hr(self.dir, 0), right)]
            self.relay = [mk(8, hp(cl, 0), hr(self.fin, 0), left), mk(9, hp(cr, 1), hr(self.fin, 1), right)]

        def pair(self, chip):
            return remote(self.part.at[chip, other], self.from_sib.at[chip], self.ssem.at[chip],
                          self.rsem.at[chip], sib)

        def add(self, chip):
            self.pair_recv(chip)
            got = self.part[chip, mine].astype(F32) + self.from_sib[chip].astype(F32)
            self.part[chip, mine] = got.astype(self.part.dtype)

        def pair_recv(self, chip):
            remote(self.from_sib.at[chip], self.from_sib.at[chip], self.ssem.at[chip], self.rsem.at[chip],
                   sib).wait_recv()

        def send_opp(self):
            self.add(co)
            for cp in self.opp:
                cp.start()

        def send_direct(self):
            self.add(cl)
            self.direct[0].start()
            self.add(cr)
            self.direct[1].start()

        def send_relay(self):
            for h, (chip, cp) in enumerate(((cl, self.relay[0]), (cr, self.relay[1]))):
                self.opp[h].wait_recv()
                got = self.part[chip, my_half(h)].astype(F32) + self.rel[h * half:(h + 1) * half].astype(F32)
                self.part[chip, my_half(h)] = got.astype(self.part.dtype)
                cp.start()

        def land(self):
            self.pair_recv(c)
            for cp in self.direct + self.relay:
                cp.wait_recv()

        def total(self, r):
            at = pl.ds(pl.multiple_of(k * rows + r * CHUNK, CHUNK), CHUNK)
            loc = pl.ds(pl.multiple_of(r * CHUNK, CHUNK), CHUNK)
            return (self.part[c, at].astype(F32) + self.from_sib[c, loc].astype(F32)
                    + self.fin[loc].astype(F32) + self.dir[loc].astype(F32))

        def drain(self):
            for chip in range(NCHIP):
                self.pair(chip).wait_send()
            for cp in self.opp + self.direct + self.relay:
                cp.wait_send()

    rs_f = Scatter(PF, XF, RF, rs_send.at[0], rs_recv.at[0])
    rs_b = Scatter(PB, XB, RB, rs_send.at[1], rs_recv.at[1])

    def span(core, h):
        return pl.ds(pl.multiple_of(core * rows + h * half, half), half)

    def gather_rows(buf, i):
        return Gather(lambda chip, core, h: buf.at[chip, span(core, h)], ag_send.at[i], ag_recv.at[i])

    def heads_of(chip, core):
        return pl.ds(pl.multiple_of((2 * chip + core) * head, head), head)

    def gather_o():
        n = NCHIP // 2
        return Gather(lambda chip, core, h: OG.at[pl.ds(h * n, n), :, heads_of(chip, core)],
                      ag_send.at[3], ag_recv.at[3])

    def gather_out(out, i, src):
        def view(chip, core, h):
            return out.at[pl.ds(pl.multiple_of((2 * chip + core) * rows + h * half, half), half)]
        return Gather(view, fg_send.at[i], fg_recv.at[i], lambda h: src.at[pl.ds(h * half, half)])

    def keep_out(out, i, src):
        return pltpu.make_async_copy(src, out.at[pl.ds(pl.multiple_of(me * rows, rows), rows)], own_sem.at[i])

    lanes = 128
    piece = width * head // (lanes * groups)

    def own_piece_copies(layer):
        if piece >= head:
            n = piece // head
            return [pltpu.make_async_copy(
                wo_hbm.at[layer, :, pl.ds(pl.multiple_of((grp * n + b) * lanes, lanes), lanes)],
                VG.at[me, pl.ds(layer * piece + b * head, head)], wl_sem.at[layer * n + b]) for b in range(n)]
        n = head // piece
        return [pltpu.make_async_copy(
            wo_hbm.at[layer, pl.ds(pl.multiple_of(lax.rem(grp, n) * piece, piece), piece),
                      pl.ds(pl.multiple_of((grp // n) * lanes, lanes), lanes)],
            VG.at[me, pl.ds(layer * piece, piece)], wl_sem.at[layer])]

    def vg_view(chip, core, h):
        n = layers * piece // 2
        return VG.at[2 * chip + core, pl.ds(h * n, n)]

    def piece_send(layer, d):
        return pltpu.make_async_remote_copy(
            src_ref=VG.at[:, pl.ds(layer * piece, piece)], dst_ref=wof_hbm.at[layer, grp],
            send_sem=wx_send.at[layer, d], recv_sem=wx_recv.at[layer, d],
            device_id={"dp": lax.rem(grp + d, groups), "tp": me}, device_id_type=pl.DeviceIdType.MESH)

    def piece_keep(layer):
        return pltpu.make_async_copy(VG.at[:, pl.ds(layer * piece, piece)], wof_hbm.at[layer, grp],
                                     wx_send.at[layer, 0])

    def pieces_out():
        for layer in reversed(range(layers)):
            piece_keep(layer).start()

            def one(d, _):
                piece_send(layer, d).start()
                return 0
            lax.fori_loop(1, groups, one, 0)

    def pieces_sent():
        for layer in range(layers):
            def one(d, _):
                piece_send(layer, d).wait_send()
                return 0
            lax.fori_loop(1, groups, one, 0)

    def pieces_in(layer):
        def one(d, _):
            pltpu.make_async_remote_copy(
                src_ref=wof_hbm.at[layer, grp], dst_ref=wof_hbm.at[layer, lax.rem(grp + groups - d, groups)],
                send_sem=wx_send.at[layer, d], recv_sem=wx_recv.at[layer, d],
                device_id={"dp": grp, "tp": me}, device_id_type=pl.DeviceIdType.MESH).wait_recv()
            return 0
        piece_keep(layer).wait()
        lax.fori_loop(1, groups, one, 0)

    def wov_copies(layer):
        if piece >= head:
            n = piece // head
            return [pltpu.make_async_copy(wof_hbm.at[layer, g, :, pl.ds(b * head, head)],
                                          WoV.at[:, :, pl.ds((g * n + b) * lanes, lanes)], wl_sem.at[g * n + b])
                    for g in range(groups) for b in range(n)]
        n = head // piece
        return [pltpu.make_async_copy(wof_hbm.at[layer, g],
                                      WoV.at[:, pl.ds((g % n) * piece, piece), pl.ds((g // n) * lanes, lanes)],
                                      wl_sem.at[g]) for g in range(groups)]

    def weight_copies(layer, slot):
        pairs = [(src.at[layer], dst.at[slot]) for src, dst in ((wo_hbm, Wo), (wu_hbm, Wu), (wd_hbm, Wd))]
        pairs += [(wqkv_hbm.at[layer, j], Wqkv.at[slot, :, pl.ds(j * head, head)]) for j in range(3)]
        return [pltpu.make_async_copy(src, dst, w_sem.at[slot, i]) for i, (src, dst) in enumerate(pairs)]

    tile = width // 4

    def grad_copy(layer, i, t):
        at = pl.ds(pl.multiple_of(t * tile, tile), tile)
        if i == 0:
            size = 3 * width
            dst = gqkv_out.at[pl.ds(pl.multiple_of(layer * size + t * 3 * tile, 3 * tile), 3 * tile)]
        else:
            dst = (gout_out.at[layer, :, at], gup_out.at[layer, at], gdown_out.at[layer, :, at])[i - 1]
        return pltpu.make_async_copy((SQ, SO, SU, SD)[i].at[lax.rem(t, 2)], dst, g_sem.at[i, lax.rem(t, 2)])

    def wgrad_tiles(layer, i, fill):
        def body(t, _):
            pl.when(t >= 2)(lambda: grad_copy(layer, i, t - 2).wait())
            fill(t, lax.rem(t, 2), pl.ds(pl.multiple_of(t * tile, tile), tile))
            grad_copy(layer, i, t).start()
            return 0
        lax.fori_loop(0, 4, body, 0)

    def wgrad_wait(layer, i):
        for t in (2, 3):
            grad_copy(layer, i, t).wait()

    def mlp_fwd(chip, par):
        hid = mm(N1[par, chip], Wu[par])
        H[chip] = hid
        act = hid * (0.5 * (1.0 + jnp.tanh(GELU_C * (hid + GELU_A * (hid * hid * hid)))))
        act = act.astype(BF16)
        ACT[par, chip] = act
        PF[chip] = mm(act, Wd[par])

    def mlp_bwd(chip, par):
        grad_act = mm_t(D2[chip], Wd[par])
        hid = H[chip]
        sq = hid * hid
        t = jnp.tanh(GELU_C * (hid + GELU_A * (sq * hid)))
        slope = 0.5 * (1.0 + t) + (0.5 * hid) * ((1.0 - t * t) * (GELU_C * (1.0 + (3.0 * GELU_A) * sq)))
        grad_hid = (grad_act * slope).astype(BF16)
        GH[chip] = grad_hid
        PB[chip] = mm_t(grad_hid, Wu[par]).astype(BF16)

    def attn_fwd(chip, par):
        qkv = mm(N2[par, chip], Wqkv[par]).astype(BF16)
        QKV[chip] = qkv
        parts = [[qkv[s * rows:(s + 1) * rows, j * head:(j + 1) * head] for j in range(3)] for s in range(2)]
        scores = [mm_t(q, kk) * scale for q, kk, _ in parts]
        exps = [jnp.exp(sc - jnp.max(sc, axis=-1, keepdims=True)) for sc in scores]
        probs = [e / jnp.sum(e, axis=-1, keepdims=True) for e in exps]
        for s in range(2):
            PROB[chip, s * rows:(s + 1) * rows] = probs[s]
        outs = [mm(probs[s].astype(BF16), parts[s][2]).astype(BF16) for s in range(2)]
        for s in range(2):
            OG[chip, s * rows:(s + 1) * rows, heads_of(c, k)] = outs[s]

    def attn_bwd(chip, par):
        go = mm_t(D1[chip], Wo[par]).astype(BF16)
        grad_o = [go[s * rows:(s + 1) * rows] for s in range(2)]
        parts = [[QKV[chip, s * rows:(s + 1) * rows, j * head:(j + 1) * head] for j in range(3)] for s in range(2)]
        probs = [PROB[chip, s * rows:(s + 1) * rows] for s in range(2)]
        grad_p = [mm_t(grad_o[s], parts[s][2]) for s in range(2)]
        dots = [jnp.sum(grad_p[s] * probs[s], axis=-1, keepdims=True) for s in range(2)]
        grad_s = [(probs[s] * (grad_p[s] - dots[s]) * scale).astype(BF16) for s in range(2)]
        grads = [[mm(grad_s[s], parts[s][1]), tmm(grad_s[s], parts[s][0]), tmm(probs[s].astype(BF16), grad_o[s])]
                 for s in range(2)]
        for s in range(2):
            for j in range(3):
                GQ[chip, s * rows:(s + 1) * rows, j * head:(j + 1) * head] = grads[s][j].astype(BF16)
        PB[chip] = mm_t(GQ[chip], Wqkv[par]).astype(BF16)

    def flat(x):
        return x.reshape((x.shape[0] * x.shape[1],) + x.shape[2:])

    def mlp_wgrad(layer, par):
        def up(t, slot, at):
            SU[slot] = tmm(flat(N1[par, :, :, at]), flat(GH[...]))

        def down(t, slot, at):
            SD[slot] = tmm(flat(ACT[par]), flat(D2[:, :, at]))
        wgrad_tiles(layer, 2, up)
        wgrad_tiles(layer, 3, down)
        wgrad_wait(layer, 2)
        wgrad_wait(layer, 3)

    def attn_wgrad(layer, par):
        def qkv(t, slot, at):
            res = tmm(flat(N2[par, :, :, at]), flat(GQ[...]))
            for j in range(3):
                SQ[slot, pl.ds(j, tile, stride=3), :] = res[:, j * head:(j + 1) * head]

        def out(t, slot, at):
            SO[slot] = tmm(flat(OG[:, :, heads_of(c, k)]), flat(D1[:, :, at]))
        wgrad_tiles(layer, 0, qkv)
        wgrad_tiles(layer, 1, out)
        wgrad_wait(layer, 0)
        wgrad_wait(layer, 1)

    def own_rows(step):
        def body(r, _):
            step(r, pl.ds(pl.multiple_of(r * CHUNK, CHUNK), CHUNK),
                 pl.ds(pl.multiple_of(k * rows + r * CHUNK, CHUNK), CHUNK))
            return 0
        lax.fori_loop(0, rows // CHUNK, body, 0)

    def inv_rms(x):
        return lax.rsqrt(jnp.mean(x * x, axis=-1, keepdims=True) + NORM_EPS)

    def finish_state(rs, old, new, norm_to):
        rs.land()

        def step(r, loc, at):
            x = old[loc] - rs.total(r)
            new[loc] = x
            if norm_to is not None:
                norm_to[c, at] = (x * inv_rms(x)).astype(BF16)
        own_rows(step)
        rs.drain()

    def finish_cot(rs, cot, x_ref, cast_to):
        rs.land()

        def step(r, loc, at):
            x = x_ref[loc]
            inv = inv_rms(x)
            normed = x * inv
            grad_n = rs.total(r)
            new = cot[loc] + inv * (grad_n - normed * jnp.mean(normed * grad_n, axis=-1, keepdims=True))
            cot[loc] = new
            if cast_to is not None:
                cast_to[c, at] = new.astype(BF16)
        own_rows(step)
        rs.drain()

    def finish_sum(rs, to):
        rs.land()

        def step(r, loc, at):
            to[c, at] = rs.total(r).astype(BF16)
        own_rows(step)
        rs.drain()

    def chip_rows(step):
        def body(i, _):
            step(pl.ds(pl.multiple_of(i * CHUNK, CHUNK), CHUNK))
            return 0
        lax.fori_loop(0, 2 * rows // CHUNK, body, 0)

    def attn_apply(chip, par):
        q = 1 - par
        PF[chip] = mm(OG[chip], flat(WoV[...]))

        def step(at):
            x = Y1[par, chip, at] - PF[chip, at]
            Y1[q, chip, at] = x
            N1[q, chip, at] = (x * inv_rms(x)).astype(BF16)
        chip_rows(step)

    def cot_apply(chip, par):
        def step(at):
            x = Y1[par, chip, at]
            inv = inv_rms(x)
            normed = x * inv
            grad_n = D1[chip, at].astype(F32)
            new = C1[chip, at] + inv * (grad_n - normed * jnp.mean(normed * grad_n, axis=-1, keepdims=True))
            C1[chip, at] = new
            D1[chip, at] = new.astype(BF16)
        chip_rows(step)

    def when(cond, fn):
        if cond is True:
            fn()
        elif cond is not False:
            pl.when(cond)(fn)

    def partials(rs, compute, extra=()):
        def body(j, _):
            chip = order(j)
            compute(chip)
            rs.pair(chip).start()
            for at, fn in extra:
                pl.when(j == at)(fn)
            return 0
        lax.fori_loop(0, NCHIP, body, 0)

    def top_half(layer, par, not_first, last):
        q = 1 - par
        ag_d = gather_rows(D2, 1)
        ag_o = gather_o()
        if last:
            ag_n = gather_out(x2_out, 0, Y2.at[par])
            finish_state(rs_f, Y2.at[q], Y2.at[par], None)
            ag_n.start()
            keep_out(x2_out, 0, Y2.at[par]).start()
        else:
            ag_n = gather_rows(N2.at[par], 0)
            finish_state(rs_f, Y2.at[q], Y2.at[par], N2.at[par])
            ag_n.start()
            for cp in weight_copies(layer - 1, q):
                cp.start()
        when(not_first, rs_b.send_relay)
        ag_n.near()

        def d_start():
            attn_wgrad(layer + 1, q)
            finish_cot(rs_b, C2, Y2.at[q], D2)
            ag_d.start()
        when(not_first, d_start)
        ag_n.far()
        ag_n.finish()
        if last:
            keep_out(x2_out, 0, Y2.at[par]).wait()
            loads = [pltpu.make_async_copy(x2_out.at[pl.ds(chip * 2 * rows, 2 * rows)], PF.at[chip],
                                           io_sem.at[0, chip, 0]) for chip in range(NCHIP)]
            for cp in loads:
                cp.start()
            for chip in range(NCHIP):
                loads[chip].wait()

                def step(at):
                    x = PF[chip, at]
                    N2[par, chip, at] = (x * inv_rms(x)).astype(BF16)
                chip_rows(step)
        pieces_in(layer)
        for cp in wov_copies(layer):
            cp.start()

        def fwd(chip, _):
            attn_fwd(chip, par)

            @pl.when(chip == NCHIP // 2 - 1)
            def _():
                ag_o.start_half(0)
                when(not_first, ag_d.near)
            return 0
        lax.fori_loop(0, NCHIP, fwd, 0)
        ag_o.start_half(1)
        ag_o.near0()

        def d_end():
            ag_d.far()
            ag_d.finish()
        when(not_first, d_end)
        partials(rs_b, lambda chip: mlp_bwd(chip, par), ((0, ag_o.near1), (1, rs_b.send_opp)))
        rs_b.send_direct()
        for cp in wov_copies(layer):
            cp.wait()
        ag_o.far()
        ag_o.finish()

    def low_half(layer, par):
        q = 1 - par
        ag_d = gather_rows(D1, 2)
        for cp in weight_copies(layer - 1, q):
            cp.wait()

        def fwd(chip):
            attn_apply(chip, par)
            mlp_fwd(chip, q)
        partials(rs_f, fwd, ((0, rs_b.send_relay), (1, rs_f.send_opp)))
        finish_sum(rs_b, D1)
        ag_d.start()
        rs_f.send_direct()
        mlp_wgrad(layer, par)
        ag_d.near()
        rs_f.send_relay()
        ag_d.far()
        ag_d.finish()
        attn_back(par)

    def attn_back(par):
        def bwd(chip):
            cot_apply(chip, par)
            attn_bwd(chip, par)
        partials(rs_b, bwd, ((1, rs_b.send_opp),))
        rs_b.send_direct()

    top = layers - 1
    tp = top % 2
    for layer in range(layers):
        for cp in own_piece_copies(layer):
            cp.start()
    for cp in weight_copies(top, tp):
        cp.start()
    loads = [pltpu.make_async_copy(src.at[me], dst, own_sem.at[i]) for i, (src, dst) in enumerate(
        ((y2_hbm, Y2.at[1 - tp]), (c2_hbm, C2)))]
    for cp in loads:
        cp.start()

    def load_rows(src, dst, i, chip, s):
        return pltpu.make_async_copy(src.at[2 * chip + s], dst.at[chip, pl.ds(s * rows, rows)], io_sem.at[i, chip, s])

    def each_pair(fn):
        def body(j, _):
            for s in range(2):
                fn(order(j), s)
            return 0
        lax.fori_loop(0, NCHIP, body, 0)

    def top_fwd(chip):
        for s in range(2):
            load_rows(y1_hbm, Y1.at[tp], 0, chip, s).wait()

        def step(at):
            x = Y1[tp, chip, at]
            N1[tp, chip, at] = (x * inv_rms(x)).astype(BF16)
        chip_rows(step)
        mlp_fwd(chip, tp)

    def cast_c2():
        each_pair(lambda chip, s: load_rows(c2_hbm, C1, 1, chip, s).wait())

        def body(chip, _):
            def step(at):
                D2[chip, at] = C1[chip, at].astype(BF16)
            chip_rows(step)
            return 0
        lax.fori_loop(0, NCHIP, body, 0)
        each_pair(lambda chip, s: load_rows(c1_hbm, C1, 1, chip, s).start())

    each_pair(lambda chip, s: load_rows(y1_hbm, Y1.at[tp], 0, chip, s).start())
    each_pair(lambda chip, s: load_rows(c2_hbm, C1, 1, chip, s).start())
    ag_w = Gather(vg_view, wg_send, wg_recv)
    for layer in range(layers):
        for cp in own_piece_copies(layer):
            cp.wait()
    ag_w.start()
    for cp in weight_copies(top, tp):
        cp.wait()
    partials(rs_f, top_fwd, ((1, rs_f.send_opp),))
    ag_w.near()
    rs_f.send_direct()
    ag_w.far()
    ag_w.finish()
    pieces_out()
    rs_f.send_relay()
    cast_c2()
    for cp in loads:
        cp.wait()
    each_pair(lambda chip, s: load_rows(c1_hbm, C1, 1, chip, s).wait())

    def layer_body(i, _):
        layer = top - i
        par = lax.rem(layer, 2)
        top_half(layer, par, layer < top, False)
        low_half(layer, par)
        return 0
    lax.fori_loop(0, top, layer_body, 0)

    top_half(0, 0, True, True)
    def put_x1(chip):
        return pltpu.make_async_copy(Y1.at[1, chip], x1_out.at[pl.ds(pl.multiple_of(chip * 2 * rows, rows), 2 * rows)],
                                     io_sem.at[0, chip, 0])

    def put_g1(chip):
        return pltpu.make_async_copy(C1.at[chip], g1_out.at[pl.ds(pl.multiple_of(chip * 2 * rows, rows), 2 * rows)],
                                     io_sem.at[0, chip, 1])

    def x1_rows(chip, _):
        attn_apply(chip, 0)
        put_x1(chip).start()
        return 0

    def each_chip(fn):
        def body(chip, _):
            fn(chip)
            return 0
        lax.fori_loop(0, NCHIP, body, 0)

    ag_d1 = gather_rows(D1, 2)
    rs_b.send_relay()
    finish_sum(rs_b, D1)
    ag_d1.start()
    lax.fori_loop(0, NCHIP, x1_rows, 0)
    ag_d1.near()
    mlp_wgrad(0, 0)
    ag_d1.far()
    ag_d1.finish()
    attn_back(0)
    each_chip(lambda chip: put_g1(chip).start())
    rs_b.send_relay()
    attn_wgrad(0, 0)
    finish_cot(rs_b, C2, Y2.at[0], None)
    last = gather_out(g2_out, 1, C2)
    last.start()
    keep_out(g2_out, 1, C2).start()
    last.near()
    last.far()
    each_chip(lambda chip: put_x1(chip).wait())
    each_chip(lambda chip: put_g1(chip).wait())
    pieces_sent()
    keep_out(g2_out, 1, C2).wait()
    last.finish()


def solution(mesh):
    act_spec = P("dp", None, None)
    weight_specs = (P(None, None, "tp", None, None), P(None, "tp", None, None), P(None, None, "tp"), P(None, "tp", None))
    grad_specs = (P("dp", None, "tp", None, None), P("dp", "tp", None, None), P("dp", None, "tp"), P("dp", "tp", None))

    groups = mesh.shape["dp"]

    def local_backward(out_y1, out_y2, cot_y1, cot_y2, w_qkv, w_out, w_up, w_down):
        seqs, rows, width = out_y1.shape
        layers, _, heads, three, head = w_qkv.shape
        hidden = w_up.shape[2]
        wq = jnp.transpose(w_qkv.reshape(layers, width, three, head), (0, 2, 1, 3))
        wo = w_out.reshape(layers, heads * head, width)
        pair = 2 * rows
        qkv_w = three * head
        piece = width * head // (128 * groups)
        act = jax.ShapeDtypeStruct((seqs * rows, width), F32)
        dma = pltpu.SemaphoreType.DMA
        outs = pl.pallas_call(
            functools.partial(kernel, groups),
            out_shape=(act, act, act, act,
                       jax.ShapeDtypeStruct((layers * width * three, head), F32),
                       jax.ShapeDtypeStruct((layers, head, width), F32),
                       jax.ShapeDtypeStruct((layers, width, hidden), F32),
                       jax.ShapeDtypeStruct((layers, hidden, width), F32),
                       jax.ShapeDtypeStruct((layers, groups, seqs, piece, 128), BF16)),
            in_specs=[pl.BlockSpec(memory_space=pl.ANY)] * 8,
            out_specs=[pl.BlockSpec(memory_space=pl.ANY)] * 9,
            scratch_shapes=[
                pltpu.VMEM((2, NCHIP, pair, width), BF16),
                pltpu.VMEM((2, NCHIP, pair, width), BF16),
                pltpu.VMEM((NCHIP, pair, width), BF16),
                pltpu.VMEM((NCHIP, pair, width), BF16),
                pltpu.VMEM((2, width, qkv_w), BF16),
                pltpu.VMEM((2, head, width), BF16),
                pltpu.VMEM((2, width, hidden), BF16),
                pltpu.VMEM((2, hidden, width), BF16),
                pltpu.VMEM((2, width // 4 * three, head), F32),
                pltpu.VMEM((2, head, width // 4), F32),
                pltpu.VMEM((2, width // 4, hidden), F32),
                pltpu.VMEM((2, hidden, width // 4), F32),
                pltpu.VMEM((NCHIP, pair, hidden), F32),
                pltpu.VMEM((2, NCHIP, pair, hidden), BF16),
                pltpu.VMEM((NCHIP, pair, hidden), BF16),
                pltpu.VMEM((NCHIP, pair, qkv_w), BF16),
                pltpu.VMEM((NCHIP, pair, rows), F32),
                pltpu.VMEM((NCHIP, pair, seqs * head), BF16),
                pltpu.VMEM((NCHIP, pair, qkv_w), BF16),
                pltpu.VMEM((2, NCHIP, pair, width), F32),
                pltpu.VMEM((2, rows, width), F32),
                pltpu.VMEM((NCHIP, pair, width), F32),
                pltpu.VMEM((rows, width), F32),
                pltpu.VMEM((NCHIP, pair, width), F32),
                pltpu.VMEM((NCHIP, pair, width), BF16),
                pltpu.VMEM((NCHIP, rows, width), F32),
                pltpu.VMEM((NCHIP, rows, width), BF16),
                pltpu.VMEM((3, rows, width), F32),
                pltpu.VMEM((3, rows, width), BF16),
                pltpu.VMEM((seqs, layers * piece, 128), BF16),
                pltpu.VMEM((seqs, head, width), BF16),
                dma((4, 14)), dma((4, 14)), dma((2, 10)), dma((2, 10)), dma((2, 14)), dma((2, 14)),
                dma((2, 6)), dma((4, 2)), dma((2, NCHIP, 2)), dma((2,)),
                dma((14,)), dma((14,)), dma((layers, groups)), dma((layers, groups)),
                dma((max(layers * max(1, piece // head), groups, width // 128),)),
            ],
            compiler_params=pltpu.CompilerParams(collective_id=0, has_side_effects=True,
                                                 vmem_limit_bytes=67043328),
        )(out_y1, out_y2, cot_y1, cot_y2, wq, wo, w_up, w_down)
        x1, x2, g1, g2 = (o.reshape(seqs, rows, width) for o in outs[:4])
        return (x1, x2, g1, g2, outs[4].reshape(w_qkv.shape), outs[5].reshape(w_out.shape), outs[6], outs[7])

    return jax.shard_map(local_backward, mesh=mesh, in_specs=(act_spec, act_spec, act_spec, act_spec) + weight_specs, out_specs=(act_spec, act_spec, act_spec, act_spec) + grad_specs, check_vma=False)
```

```python
import functools
import math
import jax
import jax.numpy as jnp
from jax import lax
from jax.experimental import pallas as pl
from jax.experimental.pallas import tpu as pltpu
from jax.sharding import PartitionSpec as P

NORM_EPS = 1e-6
F32, BF16 = jnp.float32, jnp.bfloat16
GELU_C = math.sqrt(2.0 / math.pi)
GELU_A = 0.044715
CHUNK = 64
NCHIP = 4


def mm(a, b):
    return lax.dot_general(a, b, (((1,), (0,)), ((), ())), preferred_element_type=F32)


def mm_t(a, b):
    return lax.dot_general(a, b, (((1,), (1,)), ((), ())), preferred_element_type=F32)


def tmm(a, b):
    return lax.dot_general(a, b, (((0,), (0,)), ((), ())), preferred_element_type=F32)


def kernel(groups, y1_hbm, y2_hbm, c1_hbm, c2_hbm, wqkv_hbm, wo_hbm, wu_hbm, wd_hbm,
           x1_out, x2_out, g1_out, g2_out, gqkv_out, gout_out, gup_out, gdown_out, wof_hbm,
           N1, N2, D1, D2, Wqkv, Wo, Wu, Wd, SQ, SO, SU, SD, H, ACT, GH, QKV, PROB, OG, GQ,
           Y1, Y2, C1, C2, PF, PB, XF, XB, RF, RB, VG, WoV,
           ag_send, ag_recv, rs_send, rs_recv, fg_send, fg_recv, w_sem, g_sem, io_sem, own_sem,
           wg_send, wg_recv, wx_send, wx_recv, wl_sem):
    layers = wqkv_hbm.shape[0]
    rows = y1_hbm.shape[1]
    half = rows // 2
    width = y1_hbm.shape[2]
    head = wo_hbm.shape[1]
    scale = 1.0 / math.sqrt(head)
    ndev = 2 * NCHIP
    me = lax.axis_index("tp")
    c = me // 2
    k = lax.rem(me, 2)
    sib = me + 1 - 2 * k
    left = lax.rem(me + ndev - 2, ndev)
    right = lax.rem(me + 2, ndev)
    cl = lax.rem(c + NCHIP - 1, NCHIP)
    cr = lax.rem(c + 1, NCHIP)
    co = lax.rem(c + 2, NCHIP)
    mine = pl.ds(pl.multiple_of(k * rows, rows), rows)
    other = pl.ds(pl.multiple_of((1 - k) * rows, rows), rows)

    def my_half(h):
        return pl.ds(pl.multiple_of(k * rows + h * half, half), half)

    def order(j):
        off = (2 + j) * (1 - j // 2) + (3 - j) * (j // 2)
        return lax.rem(c + off, NCHIP)

    def remote(src, dst, ssem, rsem, dev):
        return pltpu.make_async_remote_copy(src_ref=src, dst_ref=dst, send_sem=ssem, recv_sem=rsem,
                                            device_id={"tp": dev}, device_id_type=pl.DeviceIdType.MESH)

    grp = lax.axis_index("dp")
    barrier = pltpu.get_barrier_semaphore()

    def hello(axis, at, n):
        def one(i, _):
            pl.semaphore_signal(barrier, inc=1, device_id={axis: lax.rem(at + i, n)},
                                device_id_type=pl.DeviceIdType.MESH)
            return 0
        lax.fori_loop(1, n, one, 0)
    hello("tp", me, ndev)
    hello("dp", grp, groups)
    pl.semaphore_wait(barrier, ndev - 1 + groups - 1)

    class Gather:
        def __init__(self, view, ssem, rsem, own=None):
            src = (lambda h: view(c, k, h)) if own is None else own
            moves = [(src(h), view(c, k, h), dev) for h in (0, 1) for dev in (left, right, sib)]
            moves += [(view(chip, k, h), view(chip, k, h), dev) for chip, h, dev in (
                (cr, 0, left), (cl, 1, right), (cr, 0, sib), (cl, 0, sib), (cr, 1, sib), (cl, 1, sib),
                (co, 0, sib), (co, 1, sib))]
            self.send = [remote(a, b, ssem.at[i], rsem.at[i], dev) for i, (a, b, dev) in enumerate(moves)]
            o = 1 - k
            land = [(cr, k, 0), (cl, k, 0), (c, o, 0), (cr, k, 1), (cl, k, 1), (c, o, 1), (co, k, 0), (co, k, 1),
                    (cr, o, 0), (cl, o, 0), (cr, o, 1), (cl, o, 1), (co, o, 0), (co, o, 1)]
            self.recv = [remote(view(*at), view(*at), ssem.at[i], rsem.at[i], sib) for i, at in enumerate(land)]

        def pass_on(self, got, *sends):
            self.recv[got].wait_recv()
            for i in sends:
                self.send[i].start()

        def start_half(self, h):
            for i in range(3 * h, 3 * h + 3):
                self.send[i].start()

        def start(self):
            self.start_half(0)
            self.start_half(1)

        def near0(self):
            self.pass_on(0, 6, 8)
            self.pass_on(1, 9)

        def near1(self):
            self.pass_on(4, 7, 11)
            self.pass_on(3, 10)

        def near(self):
            self.near0()
            self.near1()

        def far(self):
            self.pass_on(6, 12)
            self.pass_on(7, 13)

        def finish(self):
            for i in (2, 5, 8, 9, 10, 11, 12, 13):
                self.recv[i].wait_recv()
            for cp in self.send:
                cp.wait_send()

    class Scatter:
        def __init__(self, part, from_sib, rec, ssem, rsem):
            self.part, self.from_sib = part, from_sib
            self.rel, self.dir, self.fin = rec.at[0], rec.at[1], rec.at[2]
            self.ssem, self.rsem = ssem, rsem

            def hp(chip, h):
                return part.at[chip, my_half(h)]

            def hr(buf, h):
                return buf.at[pl.ds(h * half, half)]

            def mk(i, src, dst, dev):
                return remote(src, dst, ssem.at[i], rsem.at[i], dev)

            self.opp = [mk(4, hp(co, 0), hr(self.rel, 0), left), mk(5, hp(co, 1), hr(self.rel, 1), right)]
            self.direct = [mk(6, hp(cl, 1), hr(self.dir, 1), left), mk(7, hp(cr, 0), hr(self.dir, 0), right)]
            self.relay = [mk(8, hp(cl, 0), hr(self.fin, 0), left), mk(9, hp(cr, 1), hr(self.fin, 1), right)]

        def pair(self, chip):
            return remote(self.part.at[chip, other], self.from_sib.at[chip], self.ssem.at[chip],
                          self.rsem.at[chip], sib)

        def add(self, chip):
            self.pair_recv(chip)
            got = self.part[chip, mine].astype(F32) + self.from_sib[chip].astype(F32)
            self.part[chip, mine] = got.astype(self.part.dtype)

        def pair_recv(self, chip):
            remote(self.from_sib.at[chip], self.from_sib.at[chip], self.ssem.at[chip], self.rsem.at[chip],
                   sib).wait_recv()

        def send_opp(self):
            self.add(co)
            for cp in self.opp:
                cp.start()

        def send_left(self):
            self.add(cl)
            self.direct[0].start()

        def send_right(self):
            self.add(cr)
            self.direct[1].start()

        def send_direct(self):
            self.send_left()
            self.send_right()

        def send_relay(self):
            for h, (chip, cp) in enumerate(((cl, self.relay[0]), (cr, self.relay[1]))):
                self.opp[h].wait_recv()
                got = self.part[chip, my_half(h)].astype(F32) + self.rel[h * half:(h + 1) * half].astype(F32)
                self.part[chip, my_half(h)] = got.astype(self.part.dtype)
                cp.start()

        def land(self):
            self.pair_recv(c)
            for cp in self.direct + self.relay:
                cp.wait_recv()

        def total(self, r):
            at = pl.ds(pl.multiple_of(k * rows + r * CHUNK, CHUNK), CHUNK)
            loc = pl.ds(pl.multiple_of(r * CHUNK, CHUNK), CHUNK)
            return (self.part[c, at].astype(F32) + self.from_sib[c, loc].astype(F32)
                    + self.fin[loc].astype(F32) + self.dir[loc].astype(F32))

        def drain(self):
            for chip in range(NCHIP):
                self.pair(chip).wait_send()
            for cp in self.opp + self.direct + self.relay:
                cp.wait_send()

    rs_f = Scatter(PF, XF, RF, rs_send.at[0], rs_recv.at[0])
    rs_b = Scatter(PB, XB, RB, rs_send.at[1], rs_recv.at[1])

    def span(core, h):
        return pl.ds(pl.multiple_of(core * rows + h * half, half), half)

    def gather_rows(buf, i):
        return Gather(lambda chip, core, h: buf.at[chip, span(core, h)], ag_send.at[i], ag_recv.at[i])

    def heads_of(chip, core):
        return pl.ds(pl.multiple_of((2 * chip + core) * head, head), head)

    def gather_o():
        n = NCHIP // 2
        return Gather(lambda chip, core, h: OG.at[pl.ds(h * n, n), :, heads_of(chip, core)],
                      ag_send.at[3], ag_recv.at[3])

    def gather_out(out, i, src):
        def view(chip, core, h):
            return out.at[pl.ds(pl.multiple_of((2 * chip + core) * rows + h * half, half), half)]
        return Gather(view, fg_send.at[i], fg_recv.at[i], lambda h: src.at[pl.ds(h * half, half)])

    def keep_out(out, i, src):
        return pltpu.make_async_copy(src, out.at[pl.ds(pl.multiple_of(me * rows, rows), rows)], own_sem.at[i])

    lanes = 128
    piece = width * head // (lanes * groups)

    def own_piece_copies(layer):
        if piece >= head:
            n = piece // head
            return [pltpu.make_async_copy(
                wo_hbm.at[layer, :, pl.ds(pl.multiple_of((grp * n + b) * lanes, lanes), lanes)],
                VG.at[me, pl.ds(layer * piece + b * head, head)], wl_sem.at[layer * n + b]) for b in range(n)]
        n = head // piece
        return [pltpu.make_async_copy(
            wo_hbm.at[layer, pl.ds(pl.multiple_of(lax.rem(grp, n) * piece, piece), piece),
                      pl.ds(pl.multiple_of((grp // n) * lanes, lanes), lanes)],
            VG.at[me, pl.ds(layer * piece, piece)], wl_sem.at[layer])]

    def gather_pieces(i, first, n):
        size = n * piece // 2
        return Gather(lambda chip, core, h: VG.at[2 * chip + core, pl.ds(first * piece + h * size, size)],
                      wg_send.at[i], wg_recv.at[i])

    def piece_send(layer, d):
        return pltpu.make_async_remote_copy(
            src_ref=VG.at[:, pl.ds(layer * piece, piece)], dst_ref=wof_hbm.at[layer, grp],
            send_sem=wx_send.at[layer, d], recv_sem=wx_recv.at[layer, d],
            device_id={"dp": lax.rem(grp + d, groups), "tp": me}, device_id_type=pl.DeviceIdType.MESH)

    def piece_keep(layer):
        return pltpu.make_async_copy(VG.at[:, pl.ds(layer * piece, piece)], wof_hbm.at[layer, grp],
                                     wx_send.at[layer, 0])

    def pieces_out(which):
        for layer in which:
            piece_keep(layer).start()

            def one(d, _, layer=layer):
                piece_send(layer, d).start()
                return 0
            lax.fori_loop(1, groups, one, 0)

    def pieces_sent():
        for layer in range(layers):
            def one(d, _):
                piece_send(layer, d).wait_send()
                return 0
            lax.fori_loop(1, groups, one, 0)

    def pieces_in(layer):
        def one(d, _):
            pltpu.make_async_remote_copy(
                src_ref=wof_hbm.at[layer, grp], dst_ref=wof_hbm.at[layer, lax.rem(grp + groups - d, groups)],
                send_sem=wx_send.at[layer, d], recv_sem=wx_recv.at[layer, d],
                device_id={"dp": grp, "tp": me}, device_id_type=pl.DeviceIdType.MESH).wait_recv()
            return 0
        piece_keep(layer).wait()
        lax.fori_loop(1, groups, one, 0)

    def wov_copies(layer):
        if piece >= head:
            n = piece // head
            return [pltpu.make_async_copy(wof_hbm.at[layer, g, :, pl.ds(b * head, head)],
                                          WoV.at[:, :, pl.ds((g * n + b) * lanes, lanes)], wl_sem.at[g * n + b])
                    for g in range(groups) for b in range(n)]
        n = head // piece
        return [pltpu.make_async_copy(wof_hbm.at[layer, g],
                                      WoV.at[:, pl.ds((g % n) * piece, piece), pl.ds((g // n) * lanes, lanes)],
                                      wl_sem.at[g]) for g in range(groups)]

    def weight_copies(layer, slot):
        pairs = [(src.at[layer], dst.at[slot]) for src, dst in ((wo_hbm, Wo), (wu_hbm, Wu), (wd_hbm, Wd))]
        pairs += [(wqkv_hbm.at[layer, j], Wqkv.at[slot, :, pl.ds(j * head, head)]) for j in range(3)]
        return [pltpu.make_async_copy(src, dst, w_sem.at[slot, i]) for i, (src, dst) in enumerate(pairs)]

    tile = width // 4

    def grad_copy(layer, i, t):
        at = pl.ds(pl.multiple_of(t * tile, tile), tile)
        if i == 0:
            size = 3 * width
            dst = gqkv_out.at[pl.ds(pl.multiple_of(layer * size + t * 3 * tile, 3 * tile), 3 * tile)]
        else:
            dst = (gout_out.at[layer, :, at], gup_out.at[layer, at], gdown_out.at[layer, :, at])[i - 1]
        return pltpu.make_async_copy((SQ, SO, SU, SD)[i].at[lax.rem(t, 2)], dst, g_sem.at[i, lax.rem(t, 2)])

    def wgrad_tiles(layer, i, fill):
        def body(t, _):
            pl.when(t >= 2)(lambda: grad_copy(layer, i, t - 2).wait())
            fill(t, lax.rem(t, 2), pl.ds(pl.multiple_of(t * tile, tile), tile))
            grad_copy(layer, i, t).start()
            return 0
        lax.fori_loop(0, 4, body, 0)

    def wgrad_wait(layer, i):
        for t in (2, 3):
            grad_copy(layer, i, t).wait()

    def mlp_fwd(chip, par):
        hid = mm(N1[par, chip], Wu[par])
        H[chip] = hid
        act = hid * (0.5 * (1.0 + jnp.tanh(GELU_C * (hid + GELU_A * (hid * hid * hid)))))
        act = act.astype(BF16)
        ACT[par, chip] = act
        PF[chip] = mm(act, Wd[par])

    def mlp_bwd(chip, par):
        grad_act = mm_t(D2[chip], Wd[par])
        hid = H[chip]
        sq = hid * hid
        t = jnp.tanh(GELU_C * (hid + GELU_A * (sq * hid)))
        slope = 0.5 * (1.0 + t) + (0.5 * hid) * ((1.0 - t * t) * (GELU_C * (1.0 + (3.0 * GELU_A) * sq)))
        grad_hid = (grad_act * slope).astype(BF16)
        GH[chip] = grad_hid
        PB[chip] = mm_t(grad_hid, Wu[par]).astype(BF16)

    def attn_fwd(chip, par):
        qkv = mm(N2[par, chip], Wqkv[par]).astype(BF16)
        QKV[chip] = qkv
        parts = [[qkv[s * rows:(s + 1) * rows, j * head:(j + 1) * head] for j in range(3)] for s in range(2)]
        scores = [mm_t(q, kk) * scale for q, kk, _ in parts]
        exps = [jnp.exp(sc - jnp.max(sc, axis=-1, keepdims=True)) for sc in scores]
        probs = [e / jnp.sum(e, axis=-1, keepdims=True) for e in exps]
        for s in range(2):
            PROB[chip, s * rows:(s + 1) * rows] = probs[s]
        outs = [mm(probs[s].astype(BF16), parts[s][2]).astype(BF16) for s in range(2)]
        for s in range(2):
            OG[chip, s * rows:(s + 1) * rows, heads_of(c, k)] = outs[s]

    def attn_bwd(chip, par):
        go = mm_t(D1[chip], Wo[par]).astype(BF16)
        grad_o = [go[s * rows:(s + 1) * rows] for s in range(2)]
        parts = [[QKV[chip, s * rows:(s + 1) * rows, j * head:(j + 1) * head] for j in range(3)] for s in range(2)]
        probs = [PROB[chip, s * rows:(s + 1) * rows] for s in range(2)]
        grad_p = [mm_t(grad_o[s], parts[s][2]) for s in range(2)]
        dots = [jnp.sum(grad_p[s] * probs[s], axis=-1, keepdims=True) for s in range(2)]
        grad_s = [(probs[s] * (grad_p[s] - dots[s]) * scale).astype(BF16) for s in range(2)]
        grads = [[mm(grad_s[s], parts[s][1]), tmm(grad_s[s], parts[s][0]), tmm(probs[s].astype(BF16), grad_o[s])]
                 for s in range(2)]
        for s in range(2):
            for j in range(3):
                GQ[chip, s * rows:(s + 1) * rows, j * head:(j + 1) * head] = grads[s][j].astype(BF16)
        PB[chip] = mm_t(GQ[chip], Wqkv[par]).astype(BF16)

    def flat(x):
        return x.reshape((x.shape[0] * x.shape[1],) + x.shape[2:])

    def mlp_wgrad(layer, par):
        def up(t, slot, at):
            SU[slot] = tmm(flat(N1[par, :, :, at]), flat(GH[...]))

        def down(t, slot, at):
            SD[slot] = tmm(flat(ACT[par]), flat(D2[:, :, at]))
        wgrad_tiles(layer, 2, up)
        wgrad_tiles(layer, 3, down)
        wgrad_wait(layer, 2)
        wgrad_wait(layer, 3)

    def attn_wgrad(layer, par):
        def qkv(t, slot, at):
            res = tmm(flat(N2[par, :, :, at]), flat(GQ[...]))
            for j in range(3):
                SQ[slot, pl.ds(j, tile, stride=3), :] = res[:, j * head:(j + 1) * head]

        def out(t, slot, at):
            SO[slot] = tmm(flat(OG[:, :, heads_of(c, k)]), flat(D1[:, :, at]))
        wgrad_tiles(layer, 0, qkv)
        wgrad_tiles(layer, 1, out)
        wgrad_wait(layer, 0)
        wgrad_wait(layer, 1)

    def own_rows(step):
        def body(r, _):
            step(r, pl.ds(pl.multiple_of(r * CHUNK, CHUNK), CHUNK),
                 pl.ds(pl.multiple_of(k * rows + r * CHUNK, CHUNK), CHUNK))
            return 0
        lax.fori_loop(0, rows // CHUNK, body, 0)

    def inv_rms(x):
        return lax.rsqrt(jnp.mean(x * x, axis=-1, keepdims=True) + NORM_EPS)

    def finish_state(rs, old, new, norm_to):
        rs.land()

        def step(r, loc, at):
            x = old[loc] - rs.total(r)
            new[loc] = x
            if norm_to is not None:
                norm_to[c, at] = (x * inv_rms(x)).astype(BF16)
        own_rows(step)
        rs.drain()

    def finish_cot(rs, cot, x_ref, cast_to):
        rs.land()

        def step(r, loc, at):
            x = x_ref[loc]
            inv = inv_rms(x)
            normed = x * inv
            grad_n = rs.total(r)
            new = cot[loc] + inv * (grad_n - normed * jnp.mean(normed * grad_n, axis=-1, keepdims=True))
            cot[loc] = new
            if cast_to is not None:
                cast_to[c, at] = new.astype(BF16)
        own_rows(step)
        rs.drain()

    def finish_sum(rs, to):
        rs.land()

        def step(r, loc, at):
            to[c, at] = rs.total(r).astype(BF16)
        own_rows(step)
        rs.drain()

    def chip_rows(step):
        def body(i, _):
            step(pl.ds(pl.multiple_of(i * CHUNK, CHUNK), CHUNK))
            return 0
        lax.fori_loop(0, 2 * rows // CHUNK, body, 0)

    def attn_apply(chip, par):
        q = 1 - par
        PF[chip] = mm(OG[chip], flat(WoV[...]))

        def step(at):
            x = Y1[par, chip, at] - PF[chip, at]
            Y1[q, chip, at] = x
            N1[q, chip, at] = (x * inv_rms(x)).astype(BF16)
        chip_rows(step)

    def cot_apply(chip, par):
        def step(at):
            x = Y1[par, chip, at]
            inv = inv_rms(x)
            normed = x * inv
            grad_n = D1[chip, at].astype(F32)
            new = C1[chip, at] + inv * (grad_n - normed * jnp.mean(normed * grad_n, axis=-1, keepdims=True))
            C1[chip, at] = new
            D1[chip, at] = new.astype(BF16)
        chip_rows(step)

    def when(cond, fn):
        if cond is True:
            fn()
        elif cond is not False:
            pl.when(cond)(fn)

    def partials(rs, stages, extra):
        def body(j, _):
            chip = order(j)
            for i, compute in enumerate(stages):
                compute(chip)
                if i == len(stages) - 1:
                    rs.pair(chip).start()
                for step, stage, fn in extra:
                    if stage == i:
                        pl.when(j == step)(fn)
            return 0
        lax.fori_loop(0, NCHIP, body, 0)

    def top_half(layer, par, not_first, last):
        q = 1 - par
        ag_d = gather_rows(D2, 1)
        ag_o = gather_o()
        ag_n = gather_rows(N2.at[par], 0)
        finish_state(rs_f, Y2.at[q], Y2.at[par], N2.at[par])
        ag_n.start()
        first = False if last else jnp.logical_not(not_first)
        ag_w = None if last else gather_pieces(1, 0, layers - 1)
        if last:
            keep_out(x2_out, 0, Y2.at[par]).start()
        else:
            when(first, ag_w.start)
            for cp in weight_copies(layer - 1, q):
                cp.start()
        when(not_first, rs_b.send_relay)
        ag_n.near()

        def d_start():
            attn_wgrad(layer + 1, q)
            finish_cot(rs_b, C2, Y2.at[q], D2)
            ag_d.start()
        when(not_first, d_start)
        ag_n.far()
        ag_n.finish()
        if not last:
            when(first, ag_w.near)
        pieces_in(layer)
        for cp in wov_copies(layer):
            cp.start()

        def fwd(chip, _):
            attn_fwd(chip, par)

            @pl.when(chip == NCHIP // 2 - 1)
            def _():
                ag_o.start_half(0)
                when(not_first, ag_d.near)
            return 0
        lax.fori_loop(0, NCHIP, fwd, 0)
        ag_o.start_half(1)

        def rest_out():
            ag_w.far()
            ag_w.finish()
            pieces_out(range(layers - 2, -1, -1))
        if not last:
            when(first, rest_out)
        ag_o.near0()

        def d_end():
            ag_d.far()
            ag_d.finish()
        when(not_first, d_end)
        partials(rs_b, (lambda chip: mlp_bwd(chip, par),),
                 ((0, 0, ag_o.near1), (1, 0, rs_b.send_opp), (2, 0, rs_b.send_left)))
        rs_b.send_right()
        for cp in wov_copies(layer):
            cp.wait()
        ag_o.far()
        ag_o.finish()

    def low_half(layer, par):
        q = 1 - par
        ag_d = gather_rows(D1, 2)
        for cp in weight_copies(layer - 1, q):
            cp.wait()

        partials(rs_f, (lambda chip: attn_apply(chip, par), lambda chip: mlp_fwd(chip, q)),
                 ((0, 1, rs_b.send_relay), (1, 1, rs_f.send_opp)))
        finish_sum(rs_b, D1)
        ag_d.start()
        rs_f.send_direct()
        mlp_wgrad(layer, par)
        ag_d.near()
        rs_f.send_relay()
        ag_d.far()
        ag_d.finish()
        attn_back(par)

    def attn_back(par):
        partials(rs_b, (lambda chip: cot_apply(chip, par), lambda chip: attn_bwd(chip, par)),
                 ((1, 0, rs_b.send_opp), (2, 1, rs_b.send_left), (3, 0, rs_b.send_right)))

    top = layers - 1
    tp = top % 2
    for layer in range(layers):
        for cp in own_piece_copies(layer):
            cp.start()
    for cp in weight_copies(top, tp):
        cp.start()
    loads = [pltpu.make_async_copy(src.at[me], dst, own_sem.at[i]) for i, (src, dst) in enumerate(
        ((y2_hbm, Y2.at[1 - tp]), (c2_hbm, C2)))]
    for cp in loads:
        cp.start()

    def load_rows(src, dst, i, chip, s):
        return pltpu.make_async_copy(src.at[2 * chip + s], dst.at[chip, pl.ds(s * rows, rows)], io_sem.at[i, chip, s])

    def each_pair(fn):
        def body(j, _):
            for s in range(2):
                fn(order(j), s)
            return 0
        lax.fori_loop(0, NCHIP, body, 0)

    def top_fwd(chip):
        for s in range(2):
            load_rows(y1_hbm, Y1.at[tp], 0, chip, s).wait()

        def step(at):
            x = Y1[tp, chip, at]
            N1[tp, chip, at] = (x * inv_rms(x)).astype(BF16)
        chip_rows(step)
        mlp_fwd(chip, tp)

    def cast_c2():
        each_pair(lambda chip, s: load_rows(c2_hbm, C1, 1, chip, s).wait())

        def body(chip, _):
            def step(at):
                D2[chip, at] = C1[chip, at].astype(BF16)
            chip_rows(step)
            return 0
        lax.fori_loop(0, NCHIP, body, 0)
        each_pair(lambda chip, s: load_rows(c1_hbm, C1, 1, chip, s).start())

    each_pair(lambda chip, s: load_rows(y1_hbm, Y1.at[tp], 0, chip, s).start())
    each_pair(lambda chip, s: load_rows(c2_hbm, C1, 1, chip, s).start())
    ag_w = gather_pieces(0, top, 1)
    for layer in range(layers):
        for cp in own_piece_copies(layer):
            cp.wait()
    ag_w.start()
    for cp in weight_copies(top, tp):
        cp.wait()
    partials(rs_f, (top_fwd,), ((1, 0, rs_f.send_opp),))
    ag_w.near()
    rs_f.send_direct()
    ag_w.far()
    ag_w.finish()
    pieces_out((top,))
    rs_f.send_relay()
    cast_c2()
    for cp in loads:
        cp.wait()
    each_pair(lambda chip, s: load_rows(c1_hbm, C1, 1, chip, s).wait())

    def layer_body(i, _):
        layer = top - i
        par = lax.rem(layer, 2)
        top_half(layer, par, layer < top, False)
        low_half(layer, par)
        return 0
    lax.fori_loop(0, top, layer_body, 0)

    top_half(0, 0, True, True)
    def put_x1(chip):
        return pltpu.make_async_copy(Y1.at[1, chip], x1_out.at[pl.ds(pl.multiple_of(chip * 2 * rows, rows), 2 * rows)],
                                     io_sem.at[0, chip, 0])

    def put_g1(chip):
        return pltpu.make_async_copy(C1.at[chip], g1_out.at[pl.ds(pl.multiple_of(chip * 2 * rows, rows), 2 * rows)],
                                     io_sem.at[0, chip, 1])

    def x1_rows(chip, _):
        attn_apply(chip, 0)
        put_x1(chip).start()
        return 0

    def each_chip(fn):
        def body(chip, _):
            fn(chip)
            return 0
        lax.fori_loop(0, NCHIP, body, 0)

    ag_d1 = gather_rows(D1, 2)
    rs_b.send_relay()
    finish_sum(rs_b, D1)
    ag_d1.start()
    lax.fori_loop(0, NCHIP, x1_rows, 0)
    ag_d1.near()
    ag_x = gather_out(x2_out, 0, Y2.at[0])
    ag_x.start()
    mlp_wgrad(0, 0)
    ag_d1.far()
    ag_d1.finish()
    attn_back(0)
    each_chip(lambda chip: put_g1(chip).start())
    rs_b.send_relay()
    ag_x.near()
    attn_wgrad(0, 0)
    finish_cot(rs_b, C2, Y2.at[0], None)
    last = gather_out(g2_out, 1, C2)
    last.start()
    keep_out(g2_out, 1, C2).start()
    ag_x.far()
    last.near()
    last.far()
    each_chip(lambda chip: put_x1(chip).wait())
    each_chip(lambda chip: put_g1(chip).wait())
    pieces_sent()
    keep_out(x2_out, 0, Y2.at[0]).wait()
    keep_out(g2_out, 1, C2).wait()
    ag_x.finish()
    last.finish()


def solution(mesh):
    act_spec = P("dp", None, None)
    weight_specs = (P(None, None, "tp", None, None), P(None, "tp", None, None), P(None, None, "tp"), P(None, "tp", None))
    grad_specs = (P("dp", None, "tp", None, None), P("dp", "tp", None, None), P("dp", None, "tp"), P("dp", "tp", None))

    groups = mesh.shape["dp"]

    def local_backward(out_y1, out_y2, cot_y1, cot_y2, w_qkv, w_out, w_up, w_down):
        seqs, rows, width = out_y1.shape
        layers, _, heads, three, head = w_qkv.shape
        hidden = w_up.shape[2]
        wq = jnp.transpose(w_qkv.reshape(layers, width, three, head), (0, 2, 1, 3))
        wo = w_out.reshape(layers, heads * head, width)
        pair = 2 * rows
        qkv_w = three * head
        piece = width * head // (128 * groups)
        act = jax.ShapeDtypeStruct((seqs * rows, width), F32)
        dma = pltpu.SemaphoreType.DMA
        outs = pl.pallas_call(
            functools.partial(kernel, groups),
            out_shape=(act, act, act, act,
                       jax.ShapeDtypeStruct((layers * width * three, head), F32),
                       jax.ShapeDtypeStruct((layers, head, width), F32),
                       jax.ShapeDtypeStruct((layers, width, hidden), F32),
                       jax.ShapeDtypeStruct((layers, hidden, width), F32),
                       jax.ShapeDtypeStruct((layers, groups, seqs, piece, 128), BF16)),
            in_specs=[pl.BlockSpec(memory_space=pl.ANY)] * 8,
            out_specs=[pl.BlockSpec(memory_space=pl.ANY)] * 9,
            scratch_shapes=[
                pltpu.VMEM((2, NCHIP, pair, width), BF16),
                pltpu.VMEM((2, NCHIP, pair, width), BF16),
                pltpu.VMEM((NCHIP, pair, width), BF16),
                pltpu.VMEM((NCHIP, pair, width), BF16),
                pltpu.VMEM((2, width, qkv_w), BF16),
                pltpu.VMEM((2, head, width), BF16),
                pltpu.VMEM((2, width, hidden), BF16),
                pltpu.VMEM((2, hidden, width), BF16),
                pltpu.VMEM((2, width // 4 * three, head), F32),
                pltpu.VMEM((2, head, width // 4), F32),
                pltpu.VMEM((2, width // 4, hidden), F32),
                pltpu.VMEM((2, hidden, width // 4), F32),
                pltpu.VMEM((NCHIP, pair, hidden), F32),
                pltpu.VMEM((2, NCHIP, pair, hidden), BF16),
                pltpu.VMEM((NCHIP, pair, hidden), BF16),
                pltpu.VMEM((NCHIP, pair, qkv_w), BF16),
                pltpu.VMEM((NCHIP, pair, rows), F32),
                pltpu.VMEM((NCHIP, pair, seqs * head), BF16),
                pltpu.VMEM((NCHIP, pair, qkv_w), BF16),
                pltpu.VMEM((2, NCHIP, pair, width), F32),
                pltpu.VMEM((2, rows, width), F32),
                pltpu.VMEM((NCHIP, pair, width), F32),
                pltpu.VMEM((rows, width), F32),
                pltpu.VMEM((NCHIP, pair, width), F32),
                pltpu.VMEM((NCHIP, pair, width), BF16),
                pltpu.VMEM((NCHIP, rows, width), F32),
                pltpu.VMEM((NCHIP, rows, width), BF16),
                pltpu.VMEM((3, rows, width), F32),
                pltpu.VMEM((3, rows, width), BF16),
                pltpu.VMEM((seqs, layers * piece, 128), BF16),
                pltpu.VMEM((seqs, head, width), BF16),
                dma((4, 14)), dma((4, 14)), dma((2, 10)), dma((2, 10)), dma((2, 14)), dma((2, 14)),
                dma((2, 6)), dma((4, 2)), dma((2, NCHIP, 2)), dma((2,)),
                dma((2, 14)), dma((2, 14)), dma((layers, groups)), dma((layers, groups)),
                dma((max(layers * max(1, piece // head), groups, width // 128),)),
            ],
            compiler_params=pltpu.CompilerParams(collective_id=0, has_side_effects=True,
                                                 vmem_limit_bytes=67043328),
        )(out_y1, out_y2, cot_y1, cot_y2, wq, wo, w_up, w_down)
        x1, x2, g1, g2 = (o.reshape(seqs, rows, width) for o in outs[:4])
        return (x1, x2, g1, g2, outs[4].reshape(w_qkv.shape), outs[5].reshape(w_out.shape), outs[6], outs[7])

    return jax.shard_map(local_backward, mesh=mesh, in_specs=(act_spec, act_spec, act_spec, act_spec) + weight_specs, out_specs=(act_spec, act_spec, act_spec, act_spec) + grad_specs, check_vma=False)
```

```python
import functools
import math
import jax
import jax.numpy as jnp
from jax import lax
from jax.experimental import pallas as pl
from jax.experimental.pallas import tpu as pltpu
from jax.sharding import PartitionSpec as P

NORM_EPS = 1e-6
F32, BF16 = jnp.float32, jnp.bfloat16
GELU_C = math.sqrt(2.0 / math.pi)
GELU_A = 0.044715
CHUNK = 64
NCHIP = 4


def mm(a, b):
    return lax.dot_general(a, b, (((1,), (0,)), ((), ())), preferred_element_type=F32)


def mm_t(a, b):
    return lax.dot_general(a, b, (((1,), (1,)), ((), ())), preferred_element_type=F32)


def tmm(a, b):
    return lax.dot_general(a, b, (((0,), (0,)), ((), ())), preferred_element_type=F32)


def kernel(groups, y1_hbm, y2_hbm, c1_hbm, c2_hbm, wqkv_hbm, wo_hbm, wu_hbm, wd_hbm,
           x1_out, x2_out, g1_out, g2_out, gqkv_out, gout_out, gup_out, gdown_out, wof_hbm,
           N1, N2, D1, D2, Wqkv, Wo, Wu, Wd, SQ, SO, SU, SD, H, ACT, GH, QKV, PROB, OG, GQ,
           Y1, Y2, C1, C2, PF, PB, XF, XB, RF, RB, VG, WoV,
           ag_send, ag_recv, rs_send, rs_recv, fg_send, fg_recv, w_sem, g_sem, io_sem, own_sem,
           wg_send, wg_recv, wx_send, wx_recv, wl_sem):
    layers = wqkv_hbm.shape[0]
    rows = y1_hbm.shape[1]
    half = rows // 2
    width = y1_hbm.shape[2]
    head = wo_hbm.shape[1]
    scale = 1.0 / math.sqrt(head)
    ndev = 2 * NCHIP
    me = lax.axis_index("tp")
    c = me // 2
    k = lax.rem(me, 2)
    sib = me + 1 - 2 * k
    left = lax.rem(me + ndev - 2, ndev)
    right = lax.rem(me + 2, ndev)
    cl = lax.rem(c + NCHIP - 1, NCHIP)
    cr = lax.rem(c + 1, NCHIP)
    co = lax.rem(c + 2, NCHIP)
    mine = pl.ds(pl.multiple_of(k * rows, rows), rows)
    other = pl.ds(pl.multiple_of((1 - k) * rows, rows), rows)

    def my_half(h):
        return pl.ds(pl.multiple_of(k * rows + h * half, half), half)

    def order(j):
        off = (2 + j) * (1 - j // 2) + (3 - j) * (j // 2)
        return lax.rem(c + off, NCHIP)

    def remote(src, dst, ssem, rsem, dev):
        return pltpu.make_async_remote_copy(src_ref=src, dst_ref=dst, send_sem=ssem, recv_sem=rsem,
                                            device_id={"tp": dev}, device_id_type=pl.DeviceIdType.MESH)

    grp = lax.axis_index("dp")
    barrier = pltpu.get_barrier_semaphore()

    def hello(axis, at, n):
        def one(i, _):
            pl.semaphore_signal(barrier, inc=1, device_id={axis: lax.rem(at + i, n)},
                                device_id_type=pl.DeviceIdType.MESH)
            return 0
        lax.fori_loop(1, n, one, 0)
    hello("tp", me, ndev)
    hello("dp", grp, groups)
    pl.semaphore_wait(barrier, ndev - 1 + groups - 1)

    class Gather:
        def __init__(self, view, ssem, rsem, own=None):
            src = (lambda h: view(c, k, h)) if own is None else own
            moves = [(src(h), view(c, k, h), dev) for h in (0, 1) for dev in (left, right, sib)]
            moves += [(view(chip, k, h), view(chip, k, h), dev) for chip, h, dev in (
                (cr, 0, left), (cl, 1, right), (cr, 0, sib), (cl, 0, sib), (cr, 1, sib), (cl, 1, sib),
                (co, 0, sib), (co, 1, sib))]
            self.send = [remote(a, b, ssem.at[i], rsem.at[i], dev) for i, (a, b, dev) in enumerate(moves)]
            o = 1 - k
            land = [(cr, k, 0), (cl, k, 0), (c, o, 0), (cr, k, 1), (cl, k, 1), (c, o, 1), (co, k, 0), (co, k, 1),
                    (cr, o, 0), (cl, o, 0), (cr, o, 1), (cl, o, 1), (co, o, 0), (co, o, 1)]
            self.recv = [remote(view(*at), view(*at), ssem.at[i], rsem.at[i], sib) for i, at in enumerate(land)]

        def pass_on(self, got, *sends):
            self.recv[got].wait_recv()
            for i in sends:
                self.send[i].start()

        def start_half(self, h):
            for i in range(3 * h, 3 * h + 3):
                self.send[i].start()

        def start(self):
            self.start_half(0)
            self.start_half(1)

        def near0(self):
            self.pass_on(0, 6, 8)
            self.pass_on(1, 9)

        def near1(self):
            self.pass_on(4, 7, 11)
            self.pass_on(3, 10)

        def near(self):
            self.near0()
            self.near1()

        def far(self):
            self.pass_on(6, 12)
            self.pass_on(7, 13)

        def finish(self):
            for i in (2, 5, 8, 9, 10, 11, 12, 13):
                self.recv[i].wait_recv()
            for cp in self.send:
                cp.wait_send()

    class Scatter:
        def __init__(self, part, from_sib, rec, ssem, rsem):
            self.part, self.from_sib = part, from_sib
            self.rel, self.dir, self.fin = rec.at[0], rec.at[1], rec.at[2]
            self.ssem, self.rsem = ssem, rsem

            def hp(chip, h):
                return part.at[chip, my_half(h)]

            def hr(buf, h):
                return buf.at[pl.ds(h * half, half)]

            def mk(i, src, dst, dev):
                return remote(src, dst, ssem.at[i], rsem.at[i], dev)

            self.opp = [mk(4, hp(co, 0), hr(self.rel, 0), left), mk(5, hp(co, 1), hr(self.rel, 1), right)]
            self.direct = [mk(6, hp(cl, 1), hr(self.dir, 1), left), mk(7, hp(cr, 0), hr(self.dir, 0), right)]
            self.relay = [mk(8, hp(cl, 0), hr(self.fin, 0), left), mk(9, hp(cr, 1), hr(self.fin, 1), right)]

        def pair(self, chip):
            return remote(self.part.at[chip, other], self.from_sib.at[chip], self.ssem.at[chip],
                          self.rsem.at[chip], sib)

        def add(self, chip):
            self.pair_recv(chip)
            got = self.part[chip, mine].astype(F32) + self.from_sib[chip].astype(F32)
            self.part[chip, mine] = got.astype(self.part.dtype)

        def pair_recv(self, chip):
            remote(self.from_sib.at[chip], self.from_sib.at[chip], self.ssem.at[chip], self.rsem.at[chip],
                   sib).wait_recv()

        def send_opp(self):
            self.add(co)
            for cp in self.opp:
                cp.start()

        def send_left(self):
            self.add(cl)
            self.direct[0].start()

        def send_right(self):
            self.add(cr)
            self.direct[1].start()

        def send_direct(self):
            self.send_left()
            self.send_right()

        def send_relay(self):
            for h, (chip, cp) in enumerate(((cl, self.relay[0]), (cr, self.relay[1]))):
                self.opp[h].wait_recv()
                got = self.part[chip, my_half(h)].astype(F32) + self.rel[h * half:(h + 1) * half].astype(F32)
                self.part[chip, my_half(h)] = got.astype(self.part.dtype)
                cp.start()

        def land(self):
            self.pair_recv(c)
            for cp in self.direct + self.relay:
                cp.wait_recv()

        def total(self, r):
            at = pl.ds(pl.multiple_of(k * rows + r * CHUNK, CHUNK), CHUNK)
            loc = pl.ds(pl.multiple_of(r * CHUNK, CHUNK), CHUNK)
            return (self.part[c, at].astype(F32) + self.from_sib[c, loc].astype(F32)
                    + self.fin[loc].astype(F32) + self.dir[loc].astype(F32))

        def drain(self):
            for chip in range(NCHIP):
                self.pair(chip).wait_send()
            for cp in self.opp + self.direct + self.relay:
                cp.wait_send()

    rs_f = Scatter(PF, XF, RF, rs_send.at[0], rs_recv.at[0])
    rs_b = Scatter(PB, XB, RB, rs_send.at[1], rs_recv.at[1])

    def span(core, h):
        return pl.ds(pl.multiple_of(core * rows + h * half, half), half)

    def gather_rows(buf, i):
        return Gather(lambda chip, core, h: buf.at[chip, span(core, h)], ag_send.at[i], ag_recv.at[i])

    def heads_of(chip, core):
        return pl.ds(pl.multiple_of((2 * chip + core) * head, head), head)

    def gather_o():
        n = NCHIP // 2
        return Gather(lambda chip, core, h: OG.at[pl.ds(h * n, n), :, heads_of(chip, core)],
                      ag_send.at[3], ag_recv.at[3])

    def gather_out(out, i, src):
        def view(chip, core, h):
            return out.at[pl.ds(pl.multiple_of((2 * chip + core) * rows + h * half, half), half)]
        return Gather(view, fg_send.at[i], fg_recv.at[i], lambda h: src.at[pl.ds(h * half, half)])

    def keep_out(out, i, src):
        return pltpu.make_async_copy(src, out.at[pl.ds(pl.multiple_of(me * rows, rows), rows)], own_sem.at[i])

    lanes = 128
    piece = width * head // (lanes * groups)

    def own_piece_copies(layer):
        if piece >= head:
            n = piece // head
            return [pltpu.make_async_copy(
                wo_hbm.at[layer, :, pl.ds(pl.multiple_of((grp * n + b) * lanes, lanes), lanes)],
                VG.at[me, pl.ds(layer * piece + b * head, head)], wl_sem.at[layer * n + b]) for b in range(n)]
        n = head // piece
        return [pltpu.make_async_copy(
            wo_hbm.at[layer, pl.ds(pl.multiple_of(lax.rem(grp, n) * piece, piece), piece),
                      pl.ds(pl.multiple_of((grp // n) * lanes, lanes), lanes)],
            VG.at[me, pl.ds(layer * piece, piece)], wl_sem.at[layer])]

    def gather_pieces(i, first, n):
        size = n * piece // 2
        return Gather(lambda chip, core, h: VG.at[2 * chip + core, pl.ds(first * piece + h * size, size)],
                      wg_send.at[i], wg_recv.at[i])

    def piece_send(layer, d):
        return pltpu.make_async_remote_copy(
            src_ref=VG.at[:, pl.ds(layer * piece, piece)], dst_ref=wof_hbm.at[layer, grp],
            send_sem=wx_send.at[layer, d], recv_sem=wx_recv.at[layer, d],
            device_id={"dp": lax.rem(grp + d, groups), "tp": me}, device_id_type=pl.DeviceIdType.MESH)

    def piece_keep(layer):
        return pltpu.make_async_copy(VG.at[:, pl.ds(layer * piece, piece)], wof_hbm.at[layer, grp],
                                     wx_send.at[layer, 0])

    def pieces_out(which):
        for layer in which:
            piece_keep(layer).start()

            def one(d, _, layer=layer):
                piece_send(layer, d).start()
                return 0
            lax.fori_loop(1, groups, one, 0)

    def pieces_sent():
        for layer in range(layers):
            def one(d, _):
                piece_send(layer, d).wait_send()
                return 0
            lax.fori_loop(1, groups, one, 0)

    def pieces_in(layer):
        def one(d, _):
            pltpu.make_async_remote_copy(
                src_ref=wof_hbm.at[layer, grp], dst_ref=wof_hbm.at[layer, lax.rem(grp + groups - d, groups)],
                send_sem=wx_send.at[layer, d], recv_sem=wx_recv.at[layer, d],
                device_id={"dp": grp, "tp": me}, device_id_type=pl.DeviceIdType.MESH).wait_recv()
            return 0
        piece_keep(layer).wait()
        lax.fori_loop(1, groups, one, 0)

    def wov_copies(layer):
        if piece >= head:
            n = piece // head
            return [pltpu.make_async_copy(wof_hbm.at[layer, g, :, pl.ds(b * head, head)],
                                          WoV.at[:, :, pl.ds((g * n + b) * lanes, lanes)], wl_sem.at[g * n + b])
                    for g in range(groups) for b in range(n)]
        n = head // piece
        return [pltpu.make_async_copy(wof_hbm.at[layer, g],
                                      WoV.at[:, pl.ds((g % n) * piece, piece), pl.ds((g // n) * lanes, lanes)],
                                      wl_sem.at[g]) for g in range(groups)]

    def weight_copies(layer, slot):
        pairs = [(src.at[layer], dst.at[slot]) for src, dst in ((wo_hbm, Wo), (wu_hbm, Wu), (wd_hbm, Wd))]
        pairs += [(wqkv_hbm.at[layer, j], Wqkv.at[slot, :, pl.ds(j * head, head)]) for j in range(3)]
        return [pltpu.make_async_copy(src, dst, w_sem.at[slot, i]) for i, (src, dst) in enumerate(pairs)]

    tile = width // 4

    def grad_copy(layer, i, t):
        at = pl.ds(pl.multiple_of(t * tile, tile), tile)
        if i == 0:
            size = 3 * width
            dst = gqkv_out.at[pl.ds(pl.multiple_of(layer * size + t * 3 * tile, 3 * tile), 3 * tile)]
        else:
            dst = (gout_out.at[layer, :, at], gup_out.at[layer, at], gdown_out.at[layer, :, at])[i - 1]
        return pltpu.make_async_copy((SQ, SO, SU, SD)[i].at[lax.rem(t, 2)], dst, g_sem.at[i, lax.rem(t, 2)])

    def wgrad_tiles(layer, i, fill):
        def body(t, _):
            pl.when(t >= 2)(lambda: grad_copy(layer, i, t - 2).wait())
            fill(t, lax.rem(t, 2), pl.ds(pl.multiple_of(t * tile, tile), tile))
            grad_copy(layer, i, t).start()
            return 0
        lax.fori_loop(0, 4, body, 0)

    def wgrad_wait(layer, i):
        for t in (2, 3):
            grad_copy(layer, i, t).wait()

    def mlp_fwd(chip, par):
        hid = mm(N1[par, chip], Wu[par])
        H[chip] = hid
        act = hid * (0.5 * (1.0 + jnp.tanh(GELU_C * (hid + GELU_A * (hid * hid * hid)))))
        act = act.astype(BF16)
        ACT[par, chip] = act
        PF[chip] = mm(act, Wd[par])

    def mlp_bwd(chip, par):
        grad_act = mm_t(D2[chip], Wd[par])
        hid = H[chip]
        sq = hid * hid
        t = jnp.tanh(GELU_C * (hid + GELU_A * (sq * hid)))
        slope = 0.5 * (1.0 + t) + (0.5 * hid) * ((1.0 - t * t) * (GELU_C * (1.0 + (3.0 * GELU_A) * sq)))
        grad_hid = (grad_act * slope).astype(BF16)
        GH[chip] = grad_hid
        PB[chip] = mm_t(grad_hid, Wu[par]).astype(BF16)

    def attn_fwd(chip, par):
        qkv = mm(N2[par, chip], Wqkv[par]).astype(BF16)
        QKV[chip] = qkv
        parts = [[qkv[s * rows:(s + 1) * rows, j * head:(j + 1) * head] for j in range(3)] for s in range(2)]
        scores = [mm_t(q, kk) * scale for q, kk, _ in parts]
        exps = [jnp.exp(sc - jnp.max(sc, axis=-1, keepdims=True)) for sc in scores]
        probs = [e / jnp.sum(e, axis=-1, keepdims=True) for e in exps]
        for s in range(2):
            PROB[chip, s * rows:(s + 1) * rows] = probs[s]
        outs = [mm(probs[s].astype(BF16), parts[s][2]).astype(BF16) for s in range(2)]
        for s in range(2):
            OG[chip, s * rows:(s + 1) * rows, heads_of(c, k)] = outs[s]

    def attn_bwd(chip, par):
        go = mm_t(D1[chip], Wo[par]).astype(BF16)
        grad_o = [go[s * rows:(s + 1) * rows] for s in range(2)]
        parts = [[QKV[chip, s * rows:(s + 1) * rows, j * head:(j + 1) * head] for j in range(3)] for s in range(2)]
        probs = [PROB[chip, s * rows:(s + 1) * rows] for s in range(2)]
        grad_p = [mm_t(grad_o[s], parts[s][2]) for s in range(2)]
        dots = [jnp.sum(grad_p[s] * probs[s], axis=-1, keepdims=True) for s in range(2)]
        grad_s = [(probs[s] * (grad_p[s] - dots[s]) * scale).astype(BF16) for s in range(2)]
        grads = [[mm(grad_s[s], parts[s][1]), tmm(grad_s[s], parts[s][0]), tmm(probs[s].astype(BF16), grad_o[s])]
                 for s in range(2)]
        for s in range(2):
            for j in range(3):
                GQ[chip, s * rows:(s + 1) * rows, j * head:(j + 1) * head] = grads[s][j].astype(BF16)
        PB[chip] = mm_t(GQ[chip], Wqkv[par]).astype(BF16)

    def flat(x):
        return x.reshape((x.shape[0] * x.shape[1],) + x.shape[2:])

    def mlp_wgrad(layer, par):
        def up(t, slot, at):
            SU[slot] = tmm(flat(N1[par, :, :, at]), flat(GH[...]))

        def down(t, slot, at):
            SD[slot] = tmm(flat(ACT[par]), flat(D2[:, :, at]))
        wgrad_tiles(layer, 2, up)
        wgrad_tiles(layer, 3, down)
        wgrad_wait(layer, 2)
        wgrad_wait(layer, 3)

    def attn_wgrad(layer, par):
        def qkv(t, slot, at):
            res = tmm(flat(N2[par, :, :, at]), flat(GQ[...]))
            for j in range(3):
                SQ[slot, pl.ds(j, tile, stride=3), :] = res[:, j * head:(j + 1) * head]

        def out(t, slot, at):
            SO[slot] = tmm(flat(OG[:, :, heads_of(c, k)]), flat(D1[:, :, at]))
        wgrad_tiles(layer, 0, qkv)
        wgrad_tiles(layer, 1, out)
        wgrad_wait(layer, 0)
        wgrad_wait(layer, 1)

    def own_rows(step):
        def body(r, _):
            step(r, pl.ds(pl.multiple_of(r * CHUNK, CHUNK), CHUNK),
                 pl.ds(pl.multiple_of(k * rows + r * CHUNK, CHUNK), CHUNK))
            return 0
        lax.fori_loop(0, rows // CHUNK, body, 0)

    def inv_rms(x):
        return lax.rsqrt(jnp.mean(x * x, axis=-1, keepdims=True) + NORM_EPS)

    def finish_state(rs, old, new, norm_to):
        rs.land()

        def step(r, loc, at):
            x = old[loc] - rs.total(r)
            new[loc] = x
            if norm_to is not None:
                norm_to[c, at] = (x * inv_rms(x)).astype(BF16)
        own_rows(step)
        rs.drain()

    def finish_cot(rs, cot, x_ref, cast_to):
        rs.land()

        def step(r, loc, at):
            x = x_ref[loc]
            inv = inv_rms(x)
            normed = x * inv
            grad_n = rs.total(r)
            new = cot[loc] + inv * (grad_n - normed * jnp.mean(normed * grad_n, axis=-1, keepdims=True))
            cot[loc] = new
            if cast_to is not None:
                cast_to[c, at] = new.astype(BF16)
        own_rows(step)
        rs.drain()

    def finish_sum(rs, to):
        rs.land()

        def step(r, loc, at):
            to[c, at] = rs.total(r).astype(BF16)
        own_rows(step)
        rs.drain()

    def chip_rows(step):
        def body(i, _):
            step(pl.ds(pl.multiple_of(i * CHUNK, CHUNK), CHUNK))
            return 0
        lax.fori_loop(0, 2 * rows // CHUNK, body, 0)

    def attn_apply(chip, par):
        q = 1 - par
        PF[chip] = mm(OG[chip], flat(WoV[...]))

        def step(at):
            x = Y1[par, chip, at] - PF[chip, at]
            Y1[q, chip, at] = x
            N1[q, chip, at] = (x * inv_rms(x)).astype(BF16)
        chip_rows(step)

    def cot_apply(chip, par):
        def step(at):
            x = Y1[par, chip, at]
            inv = inv_rms(x)
            normed = x * inv
            grad_n = D1[chip, at].astype(F32)
            new = C1[chip, at] + inv * (grad_n - normed * jnp.mean(normed * grad_n, axis=-1, keepdims=True))
            C1[chip, at] = new
            D1[chip, at] = new.astype(BF16)
        chip_rows(step)

    def when(cond, fn):
        if cond is True:
            fn()
        elif cond is not False:
            pl.when(cond)(fn)

    def partials(rs, stages, extra):
        def body(j, _):
            chip = order(j)
            for i, compute in enumerate(stages):
                compute(chip)
                if i == len(stages) - 1:
                    rs.pair(chip).start()
                for step, stage, fn in extra:
                    if stage == i:
                        pl.when(j == step)(fn)
            return 0
        lax.fori_loop(0, NCHIP, body, 0)

    def top_half(layer, par, not_first, last):
        q = 1 - par
        ag_d = gather_rows(D2, 1)
        ag_o = gather_o()
        ag_n = gather_rows(N2.at[par], 0)
        finish_state(rs_f, Y2.at[q], Y2.at[par], N2.at[par])
        ag_n.start()
        first = False if last else jnp.logical_not(not_first)
        ag_w = None if last else gather_pieces(1, 0, layers - 1)
        if last:
            keep_out(x2_out, 0, Y2.at[par]).start()
        else:
            when(first, ag_w.start)
            for cp in weight_copies(layer - 1, q):
                cp.start()
        when(not_first, rs_b.send_relay)
        ag_n.near()

        def d_start():
            attn_wgrad(layer + 1, q)
            finish_cot(rs_b, C2, Y2.at[q], D2)
            ag_d.start()
        when(not_first, d_start)
        ag_n.far()
        ag_n.finish()
        if not last:
            when(first, ag_w.near)
        pieces_in(layer)
        for cp in wov_copies(layer):
            cp.start()

        def fwd(chip, _):
            attn_fwd(chip, par)

            @pl.when(chip == NCHIP // 2 - 1)
            def _():
                ag_o.start_half(0)
                when(not_first, ag_d.near)
            return 0
        lax.fori_loop(0, NCHIP, fwd, 0)
        ag_o.start_half(1)

        def rest_out():
            ag_w.far()
            ag_w.finish()
            pieces_out(range(layers - 2, -1, -1))
        if not last:
            when(first, rest_out)
        ag_o.near0()

        def d_end():
            ag_d.far()
            ag_d.finish()
        when(not_first, d_end)
        partials(rs_b, (lambda chip: mlp_bwd(chip, par),),
                 ((0, 0, ag_o.near1), (1, 0, rs_b.send_opp), (2, 0, rs_b.send_left)))
        rs_b.send_right()
        for cp in wov_copies(layer):
            cp.wait()
        ag_o.far()
        ag_o.finish()

    def low_half(layer, par):
        q = 1 - par
        ag_d = gather_rows(D1, 2)
        for cp in weight_copies(layer - 1, q):
            cp.wait()

        partials(rs_f, (lambda chip: attn_apply(chip, par), lambda chip: mlp_fwd(chip, q)),
                 ((0, 1, rs_b.send_relay), (1, 1, rs_f.send_opp)))
        finish_sum(rs_b, D1)
        ag_d.start()
        rs_f.send_direct()
        mlp_wgrad(layer, par)
        ag_d.near()
        rs_f.send_relay()
        ag_d.far()
        ag_d.finish()
        attn_back(par)

    def attn_back(par):
        partials(rs_b, (lambda chip: cot_apply(chip, par), lambda chip: attn_bwd(chip, par)),
                 ((1, 0, rs_b.send_opp), (2, 1, rs_b.send_left), (3, 0, rs_b.send_right)))

    top = layers - 1
    tp = top % 2
    for layer in range(layers):
        for cp in own_piece_copies(layer):
            cp.start()
    for cp in weight_copies(top, tp):
        cp.start()
    loads = [pltpu.make_async_copy(src.at[me], dst, own_sem.at[i]) for i, (src, dst) in enumerate(
        ((y2_hbm, Y2.at[1 - tp]), (c2_hbm, C2)))]
    for cp in loads:
        cp.start()

    def load_rows(src, dst, i, chip, s):
        return pltpu.make_async_copy(src.at[2 * chip + s], dst.at[chip, pl.ds(s * rows, rows)], io_sem.at[i, chip, s])

    def each_pair(fn):
        def body(j, _):
            for s in range(2):
                fn(order(j), s)
            return 0
        lax.fori_loop(0, NCHIP, body, 0)

    def top_fwd(chip):
        for s in range(2):
            load_rows(y1_hbm, Y1.at[tp], 0, chip, s).wait()

        def step(at):
            x = Y1[tp, chip, at]
            N1[tp, chip, at] = (x * inv_rms(x)).astype(BF16)
        chip_rows(step)
        mlp_fwd(chip, tp)

    def cast_c2():
        each_pair(lambda chip, s: load_rows(c2_hbm, C1, 1, chip, s).wait())

        def body(chip, _):
            def step(at):
                D2[chip, at] = C1[chip, at].astype(BF16)
            chip_rows(step)
            return 0
        lax.fori_loop(0, NCHIP, body, 0)
        each_pair(lambda chip, s: load_rows(c1_hbm, C1, 1, chip, s).start())

    each_pair(lambda chip, s: load_rows(y1_hbm, Y1.at[tp], 0, chip, s).start())
    each_pair(lambda chip, s: load_rows(c2_hbm, C1, 1, chip, s).start())
    ag_w = gather_pieces(0, top, 1)
    for layer in range(layers):
        for cp in own_piece_copies(layer):
            cp.wait()
    ag_w.start()
    for cp in weight_copies(top, tp):
        cp.wait()
    partials(rs_f, (top_fwd,), ((1, 0, rs_f.send_opp),))
    ag_w.near()
    rs_f.send_direct()
    ag_w.far()
    ag_w.finish()
    pieces_out((top,))
    rs_f.send_relay()
    cast_c2()
    for cp in loads:
        cp.wait()
    each_pair(lambda chip, s: load_rows(c1_hbm, C1, 1, chip, s).wait())

    def layer_body(i, _):
        layer = top - i
        par = lax.rem(layer, 2)
        top_half(layer, par, layer < top, False)
        low_half(layer, par)
        return 0
    lax.fori_loop(0, top, layer_body, 0)

    top_half(0, 0, True, True)
    def put_x1(chip):
        return pltpu.make_async_copy(Y1.at[1, chip], x1_out.at[pl.ds(pl.multiple_of(chip * 2 * rows, rows), 2 * rows)],
                                     io_sem.at[0, chip, 0])

    def put_g1(chip):
        return pltpu.make_async_copy(C1.at[chip], g1_out.at[pl.ds(pl.multiple_of(chip * 2 * rows, rows), 2 * rows)],
                                     io_sem.at[0, chip, 1])

    def x1_rows(chip, _):
        attn_apply(chip, 0)
        put_x1(chip).start()
        return 0

    def each_chip(fn):
        def body(chip, _):
            fn(chip)
            return 0
        lax.fori_loop(0, NCHIP, body, 0)

    ag_d1 = gather_rows(D1, 2)
    rs_b.send_relay()
    finish_sum(rs_b, D1)
    ag_d1.start()
    lax.fori_loop(0, NCHIP, x1_rows, 0)
    ag_d1.near()
    ag_x = gather_out(x2_out, 0, Y2.at[0])
    ag_x.start()
    mlp_wgrad(0, 0)
    ag_d1.far()
    ag_d1.finish()
    attn_back(0)
    each_chip(lambda chip: put_g1(chip).start())
    rs_b.send_relay()
    ag_x.near()
    attn_wgrad(0, 0)
    finish_cot(rs_b, C2, Y2.at[0], None)
    last = gather_out(g2_out, 1, C2)
    last.start()
    keep_out(g2_out, 1, C2).start()
    ag_x.far()
    last.near()
    last.far()
    each_chip(lambda chip: put_x1(chip).wait())
    each_chip(lambda chip: put_g1(chip).wait())
    pieces_sent()
    keep_out(x2_out, 0, Y2.at[0]).wait()
    keep_out(g2_out, 1, C2).wait()
    ag_x.finish()
    last.finish()


PARTS = 8


def copy_kernel(*refs):
    n = (len(refs) - 2) // 3
    ins, outs, bufs, rsem, wsem = refs[:n], refs[n:2 * n], refs[2 * n:3 * n], refs[-2], refs[-1]

    def part(ref, p):
        if len(ref.shape) == 2:
            size = ref.shape[0] // PARTS
            return ref.at[pl.ds(p * size, size)]
        per = PARTS // ref.shape[0]
        size = ref.shape[1] // per
        return ref.at[p // per, pl.ds((p % per) * size, size)]
    todo = [(i, p) for i in range(n) for p in range(PARTS)]
    reads = [pltpu.make_async_copy(part(ins[i], p), part(bufs[i], p), rsem.at[i, p]) for i, p in todo]
    writes = [pltpu.make_async_copy(part(bufs[i], p), part(outs[i], p), wsem.at[i, p]) for i, p in todo]
    for cp in reads:
        cp.start()
    for rd, wr in zip(reads, writes):
        rd.wait()
        wr.start()
    for cp in writes:
        cp.wait()


def copy_out(arrays):
    shapes = [jax.ShapeDtypeStruct(a.shape, a.dtype) for a in arrays]
    sems = pltpu.SemaphoreType.DMA((len(arrays), PARTS))
    return pl.pallas_call(
        copy_kernel,
        out_shape=shapes,
        in_specs=[pl.BlockSpec(memory_space=pl.ANY)] * len(arrays),
        out_specs=[pl.BlockSpec(memory_space=pl.ANY)] * len(arrays),
        scratch_shapes=[pltpu.VMEM(a.shape, a.dtype) for a in arrays] + [sems, sems],
        compiler_params=pltpu.CompilerParams(vmem_limit_bytes=67043328),
    )(*arrays)


def solution(mesh):
    act_spec = P("dp", None, None)
    weight_specs = (P(None, None, "tp", None, None), P(None, "tp", None, None), P(None, None, "tp"), P(None, "tp", None))
    grad_specs = (P("dp", None, "tp", None, None), P("dp", "tp", None, None), P("dp", None, "tp"), P("dp", "tp", None))

    groups = mesh.shape["dp"]

    def local_backward(out_y1, out_y2, cot_y1, cot_y2, w_qkv, w_out, w_up, w_down):
        seqs, rows, width = out_y1.shape
        layers, _, heads, three, head = w_qkv.shape
        hidden = w_up.shape[2]
        wq = jnp.transpose(w_qkv.reshape(layers, width, three, head), (0, 2, 1, 3))
        wo = w_out.reshape(layers, heads * head, width)
        pair = 2 * rows
        qkv_w = three * head
        piece = width * head // (128 * groups)
        act = jax.ShapeDtypeStruct((seqs * rows, width), F32)
        dma = pltpu.SemaphoreType.DMA
        outs = pl.pallas_call(
            functools.partial(kernel, groups),
            out_shape=(act, act, act, act,
                       jax.ShapeDtypeStruct((layers * width * three, head), F32),
                       jax.ShapeDtypeStruct((layers, head, width), F32),
                       jax.ShapeDtypeStruct((layers, width, hidden), F32),
                       jax.ShapeDtypeStruct((layers, hidden, width), F32),
                       jax.ShapeDtypeStruct((layers, groups, seqs, piece, 128), BF16)),
            in_specs=[pl.BlockSpec(memory_space=pl.ANY)] * 8,
            out_specs=[pl.BlockSpec(memory_space=pl.ANY)] * 9,
            scratch_shapes=[
                pltpu.VMEM((2, NCHIP, pair, width), BF16),
                pltpu.VMEM((2, NCHIP, pair, width), BF16),
                pltpu.VMEM((NCHIP, pair, width), BF16),
                pltpu.VMEM((NCHIP, pair, width), BF16),
                pltpu.VMEM((2, width, qkv_w), BF16),
                pltpu.VMEM((2, head, width), BF16),
                pltpu.VMEM((2, width, hidden), BF16),
                pltpu.VMEM((2, hidden, width), BF16),
                pltpu.VMEM((2, width // 4 * three, head), F32),
                pltpu.VMEM((2, head, width // 4), F32),
                pltpu.VMEM((2, width // 4, hidden), F32),
                pltpu.VMEM((2, hidden, width // 4), F32),
                pltpu.VMEM((NCHIP, pair, hidden), F32),
                pltpu.VMEM((2, NCHIP, pair, hidden), BF16),
                pltpu.VMEM((NCHIP, pair, hidden), BF16),
                pltpu.VMEM((NCHIP, pair, qkv_w), BF16),
                pltpu.VMEM((NCHIP, pair, rows), F32),
                pltpu.VMEM((NCHIP, pair, seqs * head), BF16),
                pltpu.VMEM((NCHIP, pair, qkv_w), BF16),
                pltpu.VMEM((2, NCHIP, pair, width), F32),
                pltpu.VMEM((2, rows, width), F32),
                pltpu.VMEM((NCHIP, pair, width), F32),
                pltpu.VMEM((rows, width), F32),
                pltpu.VMEM((NCHIP, pair, width), F32),
                pltpu.VMEM((NCHIP, pair, width), BF16),
                pltpu.VMEM((NCHIP, rows, width), F32),
                pltpu.VMEM((NCHIP, rows, width), BF16),
                pltpu.VMEM((3, rows, width), F32),
                pltpu.VMEM((3, rows, width), BF16),
                pltpu.VMEM((seqs, layers * piece, 128), BF16),
                pltpu.VMEM((seqs, head, width), BF16),
                dma((4, 14)), dma((4, 14)), dma((2, 10)), dma((2, 10)), dma((2, 14)), dma((2, 14)),
                dma((2, 6)), dma((4, 2)), dma((2, NCHIP, 2)), dma((2,)),
                dma((2, 14)), dma((2, 14)), dma((layers, groups)), dma((layers, groups)),
                dma((max(layers * max(1, piece // head), groups, width // 128),)),
            ],
            compiler_params=pltpu.CompilerParams(collective_id=0, has_side_effects=True,
                                                 vmem_limit_bytes=67043328),
        )(out_y1, out_y2, cot_y1, cot_y2, wq, wo, w_up, w_down)
        outs = copy_out(outs[:8])
        x1, x2, g1, g2 = (o.reshape(seqs, rows, width) for o in outs[:4])
        return (x1, x2, g1, g2, outs[4].reshape(w_qkv.shape), outs[5].reshape(w_out.shape), outs[6], outs[7])

    return jax.shard_map(local_backward, mesh=mesh, in_specs=(act_spec, act_spec, act_spec, act_spec) + weight_specs, out_specs=(act_spec, act_spec, act_spec, act_spec) + grad_specs, check_vma=False)
```

```python
import functools
import math
import jax
import jax.numpy as jnp
from jax import lax
from jax.experimental import pallas as pl
from jax.experimental.pallas import tpu as pltpu
from jax.sharding import PartitionSpec as P

NORM_EPS = 1e-6
F32, BF16 = jnp.float32, jnp.bfloat16
GELU_C = math.sqrt(2.0 / math.pi)
GELU_A = 0.044715
CHUNK = 128
NCHIP = 4


def mm(a, b):
    return lax.dot_general(a, b, (((1,), (0,)), ((), ())), preferred_element_type=F32)


def mm_t(a, b):
    return lax.dot_general(a, b, (((1,), (1,)), ((), ())), preferred_element_type=F32)


def tmm(a, b):
    return lax.dot_general(a, b, (((0,), (0,)), ((), ())), preferred_element_type=F32)


def kernel(groups, y1_hbm, y2_hbm, c1_hbm, c2_hbm, wqkv_hbm, wo_hbm, wu_hbm, wd_hbm,
           x1_out, x2_out, g1_out, g2_out, gqkv_out, gout_out, gup_out, gdown_out, wof_hbm,
           N1, N2, D1, D2, Wqkv, Wo, Wu, Wd, SQ, SO, SU, SD, H, ACT, GH, QKV, PROB, OG, GQ,
           Y1, Y2, C1, C2, PF, PB, XF, XB, RF, RB, VG, WoV,
           ag_send, ag_recv, rs_send, rs_recv, fg_send, fg_recv, w_sem, g_sem, io_sem, own_sem,
           wg_send, wg_recv, wx_send, wx_recv, wl_sem):
    layers = wqkv_hbm.shape[0]
    rows = y1_hbm.shape[1]
    half = rows // 2
    width = y1_hbm.shape[2]
    head = wo_hbm.shape[1]
    scale = 1.0 / math.sqrt(head)
    ndev = 2 * NCHIP
    me = lax.axis_index("tp")
    c = me // 2
    k = lax.rem(me, 2)
    sib = me + 1 - 2 * k
    left = lax.rem(me + ndev - 2, ndev)
    right = lax.rem(me + 2, ndev)
    cl = lax.rem(c + NCHIP - 1, NCHIP)
    cr = lax.rem(c + 1, NCHIP)
    co = lax.rem(c + 2, NCHIP)
    mine = pl.ds(pl.multiple_of(k * rows, rows), rows)
    other = pl.ds(pl.multiple_of((1 - k) * rows, rows), rows)

    def my_half(h):
        return pl.ds(pl.multiple_of(k * rows + h * half, half), half)

    def order(j):
        off = (2 + j) * (1 - j // 2) + (3 - j) * (j // 2)
        return lax.rem(c + off, NCHIP)

    def remote(src, dst, ssem, rsem, dev):
        return pltpu.make_async_remote_copy(src_ref=src, dst_ref=dst, send_sem=ssem, recv_sem=rsem,
                                            device_id={"tp": dev}, device_id_type=pl.DeviceIdType.MESH)

    grp = lax.axis_index("dp")
    barrier = pltpu.get_barrier_semaphore()

    def hello(axis, at, n):
        def one(i, _):
            pl.semaphore_signal(barrier, inc=1, device_id={axis: lax.rem(at + i, n)},
                                device_id_type=pl.DeviceIdType.MESH)
            return 0
        lax.fori_loop(1, n, one, 0)
    hello("tp", me, ndev)
    hello("dp", grp, groups)
    pl.semaphore_wait(barrier, ndev - 1 + groups - 1)

    class Gather:
        def __init__(self, view, ssem, rsem, own=None):
            src = (lambda h: view(c, k, h)) if own is None else own
            moves = [(src(h), view(c, k, h), dev) for h in (0, 1) for dev in (left, right, sib)]
            moves += [(view(chip, k, h), view(chip, k, h), dev) for chip, h, dev in (
                (cr, 0, left), (cl, 1, right), (cr, 0, sib), (cl, 0, sib), (cr, 1, sib), (cl, 1, sib),
                (co, 0, sib), (co, 1, sib))]
            self.send = [remote(a, b, ssem.at[i], rsem.at[i], dev) for i, (a, b, dev) in enumerate(moves)]
            o = 1 - k
            land = [(cr, k, 0), (cl, k, 0), (c, o, 0), (cr, k, 1), (cl, k, 1), (c, o, 1), (co, k, 0), (co, k, 1),
                    (cr, o, 0), (cl, o, 0), (cr, o, 1), (cl, o, 1), (co, o, 0), (co, o, 1)]
            self.recv = [remote(view(*at), view(*at), ssem.at[i], rsem.at[i], sib) for i, at in enumerate(land)]

        def pass_on(self, got, *sends):
            self.recv[got].wait_recv()
            for i in sends:
                self.send[i].start()

        def start_half(self, h):
            for i in range(3 * h, 3 * h + 3):
                self.send[i].start()

        def start(self):
            self.start_half(0)
            self.start_half(1)

        def near0(self):
            self.pass_on(0, 6, 8)
            self.pass_on(1, 9)

        def near1(self):
            self.pass_on(4, 7, 11)
            self.pass_on(3, 10)

        def near(self):
            self.near0()
            self.near1()

        def far(self):
            self.pass_on(6, 12)
            self.pass_on(7, 13)

        def finish(self):
            for i in (2, 5, 8, 9, 10, 11, 12, 13):
                self.recv[i].wait_recv()
            for cp in self.send:
                cp.wait_send()

    class Scatter:
        def __init__(self, part, from_sib, rec, ssem, rsem):
            self.part, self.from_sib = part, from_sib
            self.rel, self.dir, self.fin = rec.at[0], rec.at[1], rec.at[2]
            self.ssem, self.rsem = ssem, rsem

            def hp(chip, h):
                return part.at[chip, my_half(h)]

            def hr(buf, h):
                return buf.at[pl.ds(h * half, half)]

            def mk(i, src, dst, dev):
                return remote(src, dst, ssem.at[i], rsem.at[i], dev)

            self.opp = [mk(4, hp(co, 0), hr(self.rel, 0), left), mk(5, hp(co, 1), hr(self.rel, 1), right)]
            self.direct = [mk(6, hp(cl, 1), hr(self.dir, 1), left), mk(7, hp(cr, 0), hr(self.dir, 0), right)]
            self.relay = [mk(8, hp(cl, 0), hr(self.fin, 0), left), mk(9, hp(cr, 1), hr(self.fin, 1), right)]

        def pair(self, chip):
            return remote(self.part.at[chip, other], self.from_sib.at[chip], self.ssem.at[chip],
                          self.rsem.at[chip], sib)

        def add(self, chip):
            self.pair_recv(chip)
            got = self.part[chip, mine].astype(F32) + self.from_sib[chip].astype(F32)
            self.part[chip, mine] = got.astype(self.part.dtype)

        def pair_recv(self, chip):
            remote(self.from_sib.at[chip], self.from_sib.at[chip], self.ssem.at[chip], self.rsem.at[chip],
                   sib).wait_recv()

        def send_opp(self):
            self.add(co)
            for cp in self.opp:
                cp.start()

        def send_left(self):
            self.add(cl)
            self.direct[0].start()

        def send_right(self):
            self.add(cr)
            self.direct[1].start()

        def send_direct(self):
            self.send_left()
            self.send_right()

        def send_relay(self):
            for h, (chip, cp) in enumerate(((cl, self.relay[0]), (cr, self.relay[1]))):
                self.opp[h].wait_recv()
                got = self.part[chip, my_half(h)].astype(F32) + self.rel[h * half:(h + 1) * half].astype(F32)
                self.part[chip, my_half(h)] = got.astype(self.part.dtype)
                cp.start()

        def land(self):
            self.pair_recv(c)
            for cp in self.direct + self.relay:
                cp.wait_recv()

        def total(self, r):
            at = pl.ds(pl.multiple_of(k * rows + r * CHUNK, CHUNK), CHUNK)
            loc = pl.ds(pl.multiple_of(r * CHUNK, CHUNK), CHUNK)
            return (self.part[c, at].astype(F32) + self.from_sib[c, loc].astype(F32)
                    + self.fin[loc].astype(F32) + self.dir[loc].astype(F32))

        def drain(self):
            for chip in range(NCHIP):
                self.pair(chip).wait_send()
            for cp in self.opp + self.direct + self.relay:
                cp.wait_send()

    rs_f = Scatter(PF, XF, RF, rs_send.at[0], rs_recv.at[0])
    rs_b = Scatter(PB, XB, RB, rs_send.at[1], rs_recv.at[1])

    def span(core, h):
        return pl.ds(pl.multiple_of(core * rows + h * half, half), half)

    def gather_rows(buf, i):
        return Gather(lambda chip, core, h: buf.at[chip, span(core, h)], ag_send.at[i], ag_recv.at[i])

    def heads_of(chip, core):
        return pl.ds(pl.multiple_of((2 * chip + core) * head, head), head)

    def gather_o():
        n = NCHIP // 2
        return Gather(lambda chip, core, h: OG.at[pl.ds(h * n, n), :, heads_of(chip, core)],
                      ag_send.at[3], ag_recv.at[3])

    def gather_out(out, i, src):
        def view(chip, core, h):
            return out.at[pl.ds(pl.multiple_of((2 * chip + core) * rows + h * half, half), half)]
        return Gather(view, fg_send.at[i], fg_recv.at[i], lambda h: src.at[pl.ds(h * half, half)])

    def keep_out(out, i, src):
        return pltpu.make_async_copy(src, out.at[pl.ds(pl.multiple_of(me * rows, rows), rows)], own_sem.at[i])

    lanes = 128
    piece = width * head // (lanes * groups)

    def own_piece_copies(layer):
        if piece >= head:
            n = piece // head
            return [pltpu.make_async_copy(
                wo_hbm.at[layer, :, pl.ds(pl.multiple_of((grp * n + b) * lanes, lanes), lanes)],
                VG.at[me, pl.ds(layer * piece + b * head, head)], wl_sem.at[layer * n + b]) for b in range(n)]
        n = head // piece
        return [pltpu.make_async_copy(
            wo_hbm.at[layer, pl.ds(pl.multiple_of(lax.rem(grp, n) * piece, piece), piece),
                      pl.ds(pl.multiple_of((grp // n) * lanes, lanes), lanes)],
            VG.at[me, pl.ds(layer * piece, piece)], wl_sem.at[layer])]

    def gather_pieces(i, first, n):
        size = n * piece // 2
        return Gather(lambda chip, core, h: VG.at[2 * chip + core, pl.ds(first * piece + h * size, size)],
                      wg_send.at[i], wg_recv.at[i])

    def piece_send(layer, d):
        return pltpu.make_async_remote_copy(
            src_ref=VG.at[:, pl.ds(layer * piece, piece)], dst_ref=wof_hbm.at[layer, grp],
            send_sem=wx_send.at[layer, d], recv_sem=wx_recv.at[layer, d],
            device_id={"dp": lax.rem(grp + d, groups), "tp": me}, device_id_type=pl.DeviceIdType.MESH)

    def piece_keep(layer):
        return pltpu.make_async_copy(VG.at[:, pl.ds(layer * piece, piece)], wof_hbm.at[layer, grp],
                                     wx_send.at[layer, 0])

    def pieces_out(which):
        for layer in which:
            piece_keep(layer).start()

            def one(d, _, layer=layer):
                piece_send(layer, d).start()
                return 0
            lax.fori_loop(1, groups, one, 0)

    def pieces_sent():
        for layer in range(layers):
            def one(d, _):
                piece_send(layer, d).wait_send()
                return 0
            lax.fori_loop(1, groups, one, 0)

    def pieces_in(layer):
        def one(d, _):
            pltpu.make_async_remote_copy(
                src_ref=wof_hbm.at[layer, grp], dst_ref=wof_hbm.at[layer, lax.rem(grp + groups - d, groups)],
                send_sem=wx_send.at[layer, d], recv_sem=wx_recv.at[layer, d],
                device_id={"dp": grp, "tp": me}, device_id_type=pl.DeviceIdType.MESH).wait_recv()
            return 0
        piece_keep(layer).wait()
        lax.fori_loop(1, groups, one, 0)

    def wov_copies(layer):
        if piece >= head:
            n = piece // head
            return [pltpu.make_async_copy(wof_hbm.at[layer, g, :, pl.ds(b * head, head)],
                                          WoV.at[:, :, pl.ds((g * n + b) * lanes, lanes)], wl_sem.at[g * n + b])
                    for g in range(groups) for b in range(n)]
        n = head // piece
        return [pltpu.make_async_copy(wof_hbm.at[layer, g],
                                      WoV.at[:, pl.ds((g % n) * piece, piece), pl.ds((g // n) * lanes, lanes)],
                                      wl_sem.at[g]) for g in range(groups)]

    def weight_copies(layer, slot):
        pairs = [(src.at[layer], dst.at[slot]) for src, dst in ((wo_hbm, Wo), (wu_hbm, Wu), (wd_hbm, Wd))]
        pairs += [(wqkv_hbm.at[layer, j], Wqkv.at[slot, :, pl.ds(j * head, head)]) for j in range(3)]
        return [pltpu.make_async_copy(src, dst, w_sem.at[slot, i]) for i, (src, dst) in enumerate(pairs)]

    tile = width // 4

    def grad_copy(layer, i, t):
        at = pl.ds(pl.multiple_of(t * tile, tile), tile)
        if i == 0:
            size = 3 * width
            dst = gqkv_out.at[pl.ds(pl.multiple_of(layer * size + t * 3 * tile, 3 * tile), 3 * tile)]
        else:
            dst = (gout_out.at[layer, :, at], gup_out.at[layer, at], gdown_out.at[layer, :, at])[i - 1]
        return pltpu.make_async_copy((SQ, SO, SU, SD)[i].at[lax.rem(t, 2)], dst, g_sem.at[i, lax.rem(t, 2)])

    def wgrad_tiles(layer, i, fill):
        def body(t, _):
            pl.when(t >= 2)(lambda: grad_copy(layer, i, t - 2).wait())
            fill(t, lax.rem(t, 2), pl.ds(pl.multiple_of(t * tile, tile), tile))
            grad_copy(layer, i, t).start()
            return 0
        lax.fori_loop(0, 4, body, 0)

    def wgrad_wait(layer, i):
        for t in (2, 3):
            grad_copy(layer, i, t).wait()

    def mlp_fwd(chip, par):
        hid = mm(N1[par, chip], Wu[par])
        H[chip] = hid
        act = hid * (0.5 * (1.0 + jnp.tanh(GELU_C * (hid + GELU_A * (hid * hid * hid)))))
        act = act.astype(BF16)
        ACT[par, chip] = act
        PF[chip] = mm(act, Wd[par])

    def mlp_bwd(chip, par):
        grad_act = mm_t(D2[chip], Wd[par])
        hid = H[chip]
        sq = hid * hid
        t = jnp.tanh(GELU_C * (hid + GELU_A * (sq * hid)))
        slope = 0.5 * (1.0 + t) + (0.5 * hid) * ((1.0 - t * t) * (GELU_C * (1.0 + (3.0 * GELU_A) * sq)))
        grad_hid = (grad_act * slope).astype(BF16)
        GH[chip] = grad_hid
        PB[chip] = mm_t(grad_hid, Wu[par]).astype(BF16)

    def attn_fwd(chip, par):
        qkv = mm(N2[par, chip], Wqkv[par]).astype(BF16)
        QKV[chip] = qkv
        parts = [[qkv[s * rows:(s + 1) * rows, j * head:(j + 1) * head] for j in range(3)] for s in range(2)]
        scores = [mm_t(q, kk) * scale for q, kk, _ in parts]
        exps = [jnp.exp(sc - jnp.max(sc, axis=-1, keepdims=True)) for sc in scores]
        probs = [e / jnp.sum(e, axis=-1, keepdims=True) for e in exps]
        for s in range(2):
            PROB[chip, s * rows:(s + 1) * rows] = probs[s]
        outs = [mm(probs[s].astype(BF16), parts[s][2]).astype(BF16) for s in range(2)]
        for s in range(2):
            OG[chip, s * rows:(s + 1) * rows, heads_of(c, k)] = outs[s]

    def attn_bwd(chip, par):
        go = mm_t(D1[chip], Wo[par]).astype(BF16)
        grad_o = [go[s * rows:(s + 1) * rows] for s in range(2)]
        parts = [[QKV[chip, s * rows:(s + 1) * rows, j * head:(j + 1) * head] for j in range(3)] for s in range(2)]
        probs = [PROB[chip, s * rows:(s + 1) * rows] for s in range(2)]
        grad_p = [mm_t(grad_o[s], parts[s][2]) for s in range(2)]
        dots = [jnp.sum(grad_p[s] * probs[s], axis=-1, keepdims=True) for s in range(2)]
        grad_s = [(probs[s] * (grad_p[s] - dots[s]) * scale).astype(BF16) for s in range(2)]
        grads = [[mm(grad_s[s], parts[s][1]), tmm(grad_s[s], parts[s][0]), tmm(probs[s].astype(BF16), grad_o[s])]
                 for s in range(2)]
        for s in range(2):
            for j in range(3):
                GQ[chip, s * rows:(s + 1) * rows, j * head:(j + 1) * head] = grads[s][j].astype(BF16)
        PB[chip] = mm_t(GQ[chip], Wqkv[par]).astype(BF16)

    def flat(x):
        return x.reshape((x.shape[0] * x.shape[1],) + x.shape[2:])

    def mlp_wgrad(layer, par):
        def up(t, slot, at):
            SU[slot] = tmm(flat(N1[par, :, :, at]), flat(GH[...]))

        def down(t, slot, at):
            SD[slot] = tmm(flat(ACT[par]), flat(D2[:, :, at]))
        wgrad_tiles(layer, 2, up)
        wgrad_tiles(layer, 3, down)
        wgrad_wait(layer, 2)
        wgrad_wait(layer, 3)

    def attn_wgrad(layer, par):
        def qkv(t, slot, at):
            res = tmm(flat(N2[par, :, :, at]), flat(GQ[...]))
            for j in range(3):
                SQ[slot, pl.ds(j, tile, stride=3), :] = res[:, j * head:(j + 1) * head]

        def out(t, slot, at):
            SO[slot] = tmm(flat(OG[:, :, heads_of(c, k)]), flat(D1[:, :, at]))
        wgrad_tiles(layer, 0, qkv)
        wgrad_tiles(layer, 1, out)
        wgrad_wait(layer, 0)
        wgrad_wait(layer, 1)

    def own_rows(step):
        def body(r, _):
            step(r, pl.ds(pl.multiple_of(r * CHUNK, CHUNK), CHUNK),
                 pl.ds(pl.multiple_of(k * rows + r * CHUNK, CHUNK), CHUNK))
            return 0
        lax.fori_loop(0, rows // CHUNK, body, 0)

    def inv_rms(x):
        return lax.rsqrt(jnp.mean(x * x, axis=-1, keepdims=True) + NORM_EPS)

    def finish_state(rs, old, new, norm_to):
        rs.land()

        def step(r, loc, at):
            x = old[loc] - rs.total(r)
            new[loc] = x
            if norm_to is not None:
                norm_to[c, at] = (x * inv_rms(x)).astype(BF16)
        own_rows(step)
        rs.drain()

    def finish_cot(rs, cot, x_ref, cast_to):
        rs.land()

        def step(r, loc, at):
            x = x_ref[loc]
            inv = inv_rms(x)
            normed = x * inv
            grad_n = rs.total(r)
            new = cot[loc] + inv * (grad_n - normed * jnp.mean(normed * grad_n, axis=-1, keepdims=True))
            cot[loc] = new
            if cast_to is not None:
                cast_to[c, at] = new.astype(BF16)
        own_rows(step)
        rs.drain()

    def finish_sum(rs, to):
        rs.land()

        def step(r, loc, at):
            to[c, at] = rs.total(r).astype(BF16)
        own_rows(step)
        rs.drain()

    def chip_rows(step):
        def body(i, _):
            step(pl.ds(pl.multiple_of(i * CHUNK, CHUNK), CHUNK))
            return 0
        lax.fori_loop(0, 2 * rows // CHUNK, body, 0)

    def attn_apply(chip, par):
        q = 1 - par
        PF[chip] = mm(OG[chip], flat(WoV[...]))

        def step(at):
            x = Y1[par, chip, at] - PF[chip, at]
            Y1[q, chip, at] = x
            N1[q, chip, at] = (x * inv_rms(x)).astype(BF16)
        chip_rows(step)

    def cot_apply(chip, par):
        def step(at):
            x = Y1[par, chip, at]
            inv = inv_rms(x)
            normed = x * inv
            grad_n = D1[chip, at].astype(F32)
            new = C1[chip, at] + inv * (grad_n - normed * jnp.mean(normed * grad_n, axis=-1, keepdims=True))
            C1[chip, at] = new
            D1[chip, at] = new.astype(BF16)
        chip_rows(step)

    def when(cond, fn):
        if cond is True:
            fn()
        elif cond is not False:
            pl.when(cond)(fn)

    def partials(rs, stages, extra):
        def body(j, _):
            chip = order(j)
            for i, compute in enumerate(stages):
                compute(chip)
                if i == len(stages) - 1:
                    rs.pair(chip).start()
                for step, stage, fn in extra:
                    if stage == i:
                        pl.when(j == step)(fn)
            return 0
        lax.fori_loop(0, NCHIP, body, 0)

    def top_half(layer, par, not_first, last):
        q = 1 - par
        ag_d = gather_rows(D2, 1)
        ag_o = gather_o()
        ag_n = gather_rows(N2.at[par], 0)
        finish_state(rs_f, Y2.at[q], Y2.at[par], N2.at[par])
        ag_n.start()
        first = False if last else jnp.logical_not(not_first)
        ag_w = None if last else gather_pieces(1, 0, layers - 1)
        if last:
            keep_out(x2_out, 0, Y2.at[par]).start()
        else:
            when(first, ag_w.start)
            for cp in weight_copies(layer - 1, q):
                cp.start()
        when(not_first, rs_b.send_relay)
        ag_n.near()

        def d_start():
            attn_wgrad(layer + 1, q)
            finish_cot(rs_b, C2, Y2.at[q], D2)
            ag_d.start()
        when(not_first, d_start)
        ag_n.far()
        ag_n.finish()
        if not last:
            when(first, ag_w.near)
        pieces_in(layer)
        for cp in wov_copies(layer):
            cp.start()

        def fwd(chip, _):
            attn_fwd(chip, par)

            @pl.when(chip == NCHIP // 2 - 1)
            def _():
                ag_o.start_half(0)
                when(not_first, ag_d.near)
            return 0
        lax.fori_loop(0, NCHIP, fwd, 0)
        ag_o.start_half(1)

        def rest_out():
            ag_w.far()
            ag_w.finish()
            pieces_out(range(layers - 2, -1, -1))
        if not last:
            when(first, rest_out)
        ag_o.near0()

        def d_end():
            ag_d.far()
            ag_d.finish()
        when(not_first, d_end)
        partials(rs_b, (lambda chip: mlp_bwd(chip, par),),
                 ((0, 0, ag_o.near1), (1, 0, rs_b.send_opp), (2, 0, rs_b.send_left)))
        rs_b.send_right()
        for cp in wov_copies(layer):
            cp.wait()
        ag_o.far()
        ag_o.finish()

    def low_half(layer, par):
        q = 1 - par
        ag_d = gather_rows(D1, 2)
        for cp in weight_copies(layer - 1, q):
            cp.wait()

        partials(rs_f, (lambda chip: attn_apply(chip, par), lambda chip: mlp_fwd(chip, q)),
                 ((0, 1, rs_b.send_relay), (1, 1, rs_f.send_opp)))
        finish_sum(rs_b, D1)
        ag_d.start()
        rs_f.send_direct()
        mlp_wgrad(layer, par)
        ag_d.near()
        rs_f.send_relay()
        ag_d.far()
        ag_d.finish()
        attn_back(par)

    def attn_back(par):
        partials(rs_b, (lambda chip: cot_apply(chip, par), lambda chip: attn_bwd(chip, par)),
                 ((1, 0, rs_b.send_opp), (2, 1, rs_b.send_left), (3, 0, rs_b.send_right)))

    top = layers - 1
    tp = top % 2
    for layer in range(layers):
        for cp in own_piece_copies(layer):
            cp.start()
    for cp in weight_copies(top, tp):
        cp.start()
    loads = [pltpu.make_async_copy(src.at[me], dst, own_sem.at[i]) for i, (src, dst) in enumerate(
        ((y2_hbm, Y2.at[1 - tp]), (c2_hbm, C2)))]
    for cp in loads:
        cp.start()

    def load_rows(src, dst, i, chip, s):
        return pltpu.make_async_copy(src.at[2 * chip + s], dst.at[chip, pl.ds(s * rows, rows)], io_sem.at[i, chip, s])

    def each_pair(fn):
        def body(j, _):
            for s in range(2):
                fn(order(j), s)
            return 0
        lax.fori_loop(0, NCHIP, body, 0)

    def top_fwd(chip):
        for s in range(2):
            load_rows(y1_hbm, Y1.at[tp], 0, chip, s).wait()

        def step(at):
            x = Y1[tp, chip, at]
            N1[tp, chip, at] = (x * inv_rms(x)).astype(BF16)
        chip_rows(step)
        mlp_fwd(chip, tp)

    def cast_c2():
        each_pair(lambda chip, s: load_rows(c2_hbm, C1, 1, chip, s).wait())

        def body(chip, _):
            def step(at):
                D2[chip, at] = C1[chip, at].astype(BF16)
            chip_rows(step)
            return 0
        lax.fori_loop(0, NCHIP, body, 0)
        each_pair(lambda chip, s: load_rows(c1_hbm, C1, 1, chip, s).start())

    each_pair(lambda chip, s: load_rows(y1_hbm, Y1.at[tp], 0, chip, s).start())
    each_pair(lambda chip, s: load_rows(c2_hbm, C1, 1, chip, s).start())
    ag_w = gather_pieces(0, top, 1)
    for layer in range(layers):
        for cp in own_piece_copies(layer):
            cp.wait()
    ag_w.start()
    for cp in weight_copies(top, tp):
        cp.wait()
    partials(rs_f, (top_fwd,), ((1, 0, rs_f.send_opp),))
    ag_w.near()
    rs_f.send_direct()
    ag_w.far()
    ag_w.finish()
    pieces_out((top,))
    rs_f.send_relay()
    cast_c2()
    for cp in loads:
        cp.wait()
    each_pair(lambda chip, s: load_rows(c1_hbm, C1, 1, chip, s).wait())

    def layer_body(i, _):
        layer = top - i
        par = lax.rem(layer, 2)
        top_half(layer, par, layer < top, False)
        low_half(layer, par)
        return 0
    lax.fori_loop(0, top, layer_body, 0)

    top_half(0, 0, True, True)
    def put_x1(chip):
        return pltpu.make_async_copy(Y1.at[1, chip], x1_out.at[pl.ds(pl.multiple_of(chip * 2 * rows, rows), 2 * rows)],
                                     io_sem.at[0, chip, 0])

    def put_g1(chip):
        return pltpu.make_async_copy(C1.at[chip], g1_out.at[pl.ds(pl.multiple_of(chip * 2 * rows, rows), 2 * rows)],
                                     io_sem.at[0, chip, 1])

    def x1_rows(chip, _):
        attn_apply(chip, 0)
        put_x1(chip).start()
        return 0

    def each_chip(fn):
        def body(chip, _):
            fn(chip)
            return 0
        lax.fori_loop(0, NCHIP, body, 0)

    ag_d1 = gather_rows(D1, 2)
    rs_b.send_relay()
    finish_sum(rs_b, D1)
    ag_d1.start()
    lax.fori_loop(0, NCHIP, x1_rows, 0)
    ag_d1.near()
    ag_x = gather_out(x2_out, 0, Y2.at[0])
    ag_x.start()
    mlp_wgrad(0, 0)
    ag_d1.far()
    ag_d1.finish()
    attn_back(0)
    each_chip(lambda chip: put_g1(chip).start())
    rs_b.send_relay()
    ag_x.near()
    attn_wgrad(0, 0)
    finish_cot(rs_b, C2, Y2.at[0], None)
    last = gather_out(g2_out, 1, C2)
    last.start()
    keep_out(g2_out, 1, C2).start()
    ag_x.far()
    last.near()
    last.far()
    each_chip(lambda chip: put_x1(chip).wait())
    each_chip(lambda chip: put_g1(chip).wait())
    pieces_sent()
    keep_out(x2_out, 0, Y2.at[0]).wait()
    keep_out(g2_out, 1, C2).wait()
    ag_x.finish()
    last.finish()


PARTS = 8


def copy_kernel(*refs):
    n = (len(refs) - 2) // 3
    ins, outs, bufs, rsem, wsem = refs[:n], refs[n:2 * n], refs[2 * n:3 * n], refs[-2], refs[-1]

    def part(ref, p):
        if len(ref.shape) == 2:
            size = ref.shape[0] // PARTS
            return ref.at[pl.ds(p * size, size)]
        per = PARTS // ref.shape[0]
        size = ref.shape[1] // per
        return ref.at[p // per, pl.ds((p % per) * size, size)]
    todo = [(i, p) for i in range(n) for p in range(PARTS)]
    reads = [pltpu.make_async_copy(part(ins[i], p), part(bufs[i], p), rsem.at[i, p]) for i, p in todo]
    writes = [pltpu.make_async_copy(part(bufs[i], p), part(outs[i], p), wsem.at[i, p]) for i, p in todo]
    for cp in reads:
        cp.start()
    for rd, wr in zip(reads, writes):
        rd.wait()
        wr.start()
    for cp in writes:
        cp.wait()


def copy_out(arrays):
    shapes = [jax.ShapeDtypeStruct(a.shape, a.dtype) for a in arrays]
    sems = pltpu.SemaphoreType.DMA((len(arrays), PARTS))
    return pl.pallas_call(
        copy_kernel,
        out_shape=shapes,
        in_specs=[pl.BlockSpec(memory_space=pl.ANY)] * len(arrays),
        out_specs=[pl.BlockSpec(memory_space=pl.ANY)] * len(arrays),
        scratch_shapes=[pltpu.VMEM(a.shape, a.dtype) for a in arrays] + [sems, sems],
        compiler_params=pltpu.CompilerParams(vmem_limit_bytes=67043328),
    )(*arrays)


def solution(mesh):
    act_spec = P("dp", None, None)
    weight_specs = (P(None, None, "tp", None, None), P(None, "tp", None, None), P(None, None, "tp"), P(None, "tp", None))
    grad_specs = (P("dp", None, "tp", None, None), P("dp", "tp", None, None), P("dp", None, "tp"), P("dp", "tp", None))

    groups = mesh.shape["dp"]

    def local_backward(out_y1, out_y2, cot_y1, cot_y2, w_qkv, w_out, w_up, w_down):
        seqs, rows, width = out_y1.shape
        layers, _, heads, three, head = w_qkv.shape
        hidden = w_up.shape[2]
        wq = jnp.transpose(w_qkv.reshape(layers, width, three, head), (0, 2, 1, 3))
        wo = w_out.reshape(layers, heads * head, width)
        pair = 2 * rows
        qkv_w = three * head
        piece = width * head // (128 * groups)
        act = jax.ShapeDtypeStruct((seqs * rows, width), F32)
        dma = pltpu.SemaphoreType.DMA
        outs = pl.pallas_call(
            functools.partial(kernel, groups),
            out_shape=(act, act, act, act,
                       jax.ShapeDtypeStruct((layers * width * three, head), F32),
                       jax.ShapeDtypeStruct((layers, head, width), F32),
                       jax.ShapeDtypeStruct((layers, width, hidden), F32),
                       jax.ShapeDtypeStruct((layers, hidden, width), F32),
                       jax.ShapeDtypeStruct((layers, groups, seqs, piece, 128), BF16)),
            in_specs=[pl.BlockSpec(memory_space=pl.ANY)] * 8,
            out_specs=[pl.BlockSpec(memory_space=pl.ANY)] * 9,
            scratch_shapes=[
                pltpu.VMEM((2, NCHIP, pair, width), BF16),
                pltpu.VMEM((2, NCHIP, pair, width), BF16),
                pltpu.VMEM((NCHIP, pair, width), BF16),
                pltpu.VMEM((NCHIP, pair, width), BF16),
                pltpu.VMEM((2, width, qkv_w), BF16),
                pltpu.VMEM((2, head, width), BF16),
                pltpu.VMEM((2, width, hidden), BF16),
                pltpu.VMEM((2, hidden, width), BF16),
                pltpu.VMEM((2, width // 4 * three, head), F32),
                pltpu.VMEM((2, head, width // 4), F32),
                pltpu.VMEM((2, width // 4, hidden), F32),
                pltpu.VMEM((2, hidden, width // 4), F32),
                pltpu.VMEM((NCHIP, pair, hidden), F32),
                pltpu.VMEM((2, NCHIP, pair, hidden), BF16),
                pltpu.VMEM((NCHIP, pair, hidden), BF16),
                pltpu.VMEM((NCHIP, pair, qkv_w), BF16),
                pltpu.VMEM((NCHIP, pair, rows), F32),
                pltpu.VMEM((NCHIP, pair, seqs * head), BF16),
                pltpu.VMEM((NCHIP, pair, qkv_w), BF16),
                pltpu.VMEM((2, NCHIP, pair, width), F32),
                pltpu.VMEM((2, rows, width), F32),
                pltpu.VMEM((NCHIP, pair, width), F32),
                pltpu.VMEM((rows, width), F32),
                pltpu.VMEM((NCHIP, pair, width), F32),
                pltpu.VMEM((NCHIP, pair, width), BF16),
                pltpu.VMEM((NCHIP, rows, width), F32),
                pltpu.VMEM((NCHIP, rows, width), BF16),
                pltpu.VMEM((3, rows, width), F32),
                pltpu.VMEM((3, rows, width), BF16),
                pltpu.VMEM((seqs, layers * piece, 128), BF16),
                pltpu.VMEM((seqs, head, width), BF16),
                dma((4, 14)), dma((4, 14)), dma((2, 10)), dma((2, 10)), dma((2, 14)), dma((2, 14)),
                dma((2, 6)), dma((4, 2)), dma((2, NCHIP, 2)), dma((2,)),
                dma((2, 14)), dma((2, 14)), dma((layers, groups)), dma((layers, groups)),
                dma((max(layers * max(1, piece // head), groups, width // 128),)),
            ],
            compiler_params=pltpu.CompilerParams(collective_id=0, has_side_effects=True,
                                                 vmem_limit_bytes=67043328),
        )(out_y1, out_y2, cot_y1, cot_y2, wq, wo, w_up, w_down)
        outs = copy_out(outs[:8])
        x1, x2, g1, g2 = (o.reshape(seqs, rows, width) for o in outs[:4])
        return (x1, x2, g1, g2, outs[4].reshape(w_qkv.shape), outs[5].reshape(w_out.shape), outs[6], outs[7])

    return jax.shard_map(local_backward, mesh=mesh, in_specs=(act_spec, act_spec, act_spec, act_spec) + weight_specs, out_specs=(act_spec, act_spec, act_spec, act_spec) + grad_specs, check_vma=False)
```
